128 devices in a mesh: view: 4 (over z_hi, core), gz: 32 (over z_lo, y, x).
Axes of the slice: x: 4, y: 4, z: 4 (z_hi: 2, z_lo: 2; z = z_hi * 2 + z_lo), core: 2. Of those that a mesh axis runs over, the one named last changes fastest.
Arguments:
- views_data: float32 [4, 512, 128, 384], P('view', 'gz'), may hold values from 0.25 to 4
- start: float32 [512, 128, 384], P('gz'), may hold values from 0.5 to 2
- psf_table: float32 [8, 3, 17], replicated, may hold values from 0.05 to 1
- psf_index: int32 [4], P('view'), may hold values from 0 to 7
Outputs:
- estimate: float32 [512, 128, 384], P('gz')
The draws below stay inside these ranges and needn't reach their ends.
All inputs are finite; a program needn't handle non-finite values.
Results may differ from the reference program's by a relative error of at most 0.0001.
Values sent between devices are 32-bit elements; how exact they have to be, the bound alone decides.
A program may use at most 128 MiB of HBM per device.

```python
import math
import jax
import jax.numpy as jnp
from jax import lax

NX = 128
NY = 384
RAD = 8
ITERS = 2
NPSF = 8
VIEWS = 4
TAPS = 17
NZ = 512


def plant(result, rng, least, high):
    extent = result.shape
    place = [jax.random.randint(jax.random.fold_in(rng, axis), (), 0, extent[axis]) for axis in range(len(extent))]
    result = result.at[tuple(place)].set(least)
    longest = extent.index(max(extent))
    place[longest] = (place[longest] + 1) % extent[longest]
    return result.at[tuple(place)].set(high)


def level_of(stream_key, shape, shards, smallest, high):
    def one(position, shards_of):
        steps = jax.random.uniform(jax.random.fold_in(jax.random.fold_in(stream_key, 6), position), (shards_of,), jnp.float32, smallest / len(shards), high / len(shards))
        return jnp.repeat(jnp.exp(steps), shape[position] // shards_of).reshape((-1,) + (1,) * (len(shape) - position - 1))

    gain = one(*shards[0])
    for cut in shards[1:]:
        gain = gain * one(*cut)
    return gain


def setup_inputs(seed: int = 0) -> dict:
    arg_keys = jax.random.split(jax.random.key(seed), 5)
    return {
        "views_data": jnp.clip(jnp.exp(math.log(4.0) - 2.7725887 * jax.random.uniform(arg_keys[0], (VIEWS, NZ, NX, NY), jnp.float32) ** level_of(arg_keys[0], (VIEWS, NZ, NX, NY), ((0, 4), (1, 32)), -0.2, 0.2)), 0.25, 4.0),
        "start": jnp.clip(jnp.exp(math.log(2.0) - 1.3862944 * jax.random.uniform(arg_keys[1], (NZ, NX, NY), jnp.float32) ** level_of(arg_keys[1], (NZ, NX, NY), ((0, 32),), -0.2, 0.2)), 0.5, 2.0),
        "psf_table": jnp.clip(jnp.exp(jax.random.uniform(arg_keys[2], (NPSF, 3, TAPS), jnp.float32, math.log(0.05), math.log(1.0))), 0.05, 1.0),
        "psf_index": plant(jax.random.randint(arg_keys[3], (VIEWS,), 0, NPSF), jax.random.fold_in(arg_keys[3], 1), 0, NPSF - 1).astype(jnp.int32),
    }


def band_matrix(kern_row, length):
    places = jnp.arange(length)
    offsets = places[None, :] - places[:, None]
    tap_shift = jnp.arange(2 * RAD + 1) - RAD
    matches = (offsets[None, :, :] == tap_shift[:, None, None]).astype(jnp.float32)
    return jnp.sum(kern_row[:, None, None] * matches, axis=0)


def blur_planes(volume, mat_x, mat_y):
    along_x = jnp.einsum("ij,zjy->ziy", mat_x, volume, precision=lax.Precision.HIGHEST)
    return jnp.einsum("zxj,ij->zxi", along_x, mat_y, precision=lax.Precision.HIGHEST)


def back_planes(volume, mat_x, mat_y):
    along_x = jnp.einsum("ij,ziy->zjy", mat_x, volume, precision=lax.Precision.HIGHEST)
    return jnp.einsum("zxi,ij->zxj", along_x, mat_y, precision=lax.Precision.HIGHEST)


def forward_z(padded, kern_z, rows):
    total = kern_z[0] * padded[0:rows]
    for tap in range(1, 2 * RAD + 1):
        total = total + kern_z[tap] * padded[tap:tap + rows]
    return total


def backward_z(padded, kern_z, rows):
    total = kern_z[0] * padded[2 * RAD:2 * RAD + rows]
    for tap in range(1, 2 * RAD + 1):
        total = total + kern_z[tap] * padded[2 * RAD - tap:2 * RAD - tap + rows]
    return total


def reference(views_data, start, psf_table, psf_index):
    estimate = start
    widths = ((RAD, RAD), (0, 0), (0, 0))
    for step in range(ITERS):
        total = None
        for which in range(VIEWS):
            kern = psf_table[psf_index[which]]
            kern = kern / jnp.sum(kern, axis=-1, keepdims=True)
            mat_x = band_matrix(kern[1], NX)
            mat_y = band_matrix(kern[2], NY)
            planes = blur_planes(estimate, mat_x, mat_y)
            blurred = forward_z(jnp.pad(planes, widths), kern[0], NZ)
            ratio = views_data[which] / blurred
            smeared = backward_z(jnp.pad(ratio, widths), kern[0], NZ)
            correction = back_planes(smeared, mat_x, mat_y)
            total = correction if total is None else total * correction
        estimate = estimate * jnp.power(total, 1.0 / VIEWS)
    return estimate
```

```python
import functools

import jax
import jax.numpy as jnp
from jax import lax
from jax.experimental import pallas as pl
from jax.experimental.pallas import tpu as pltpu
from jax.sharding import PartitionSpec as P

ITERS = 2
GROUP = 4
CHUNK = 32


def toeplitz(row, length):
    taps = row.shape[0]
    radius = (taps - 1) // 2
    places = jnp.arange(length)
    shift = places[None, :] - places[:, None] + radius
    hits = (shift[None] == jnp.arange(taps)[:, None, None]).astype(jnp.float32)
    return jnp.sum(row[:, None, None] * hits, axis=0)


def halves(value):
    high = value.astype(jnp.bfloat16)
    return high, (value - high.astype(jnp.float32)).astype(jnp.bfloat16)


def lane_matrix(matrix):
    high, low = halves(matrix)
    top = jnp.concatenate([high, low], axis=1)
    return jnp.concatenate([top, top], axis=0)


def row_matrix(matrix):
    high, low = halves(matrix)
    return jnp.concatenate([high, low, high], axis=1)


def convolve(taps, coef, read, matrix_x, matrix_y, mixed, finish):
    rows = mixed.shape[1]
    wide = mixed.shape[2]
    for r0 in range(0, rows, CHUNK):
        total = [None] * GROUP
        for i in range(taps + GROUP - 1):
            value = read(i, r0)
            for o in range(GROUP):
                if 0 <= i - o < taps:
                    term = coef[i - o] * value
                    total[o] = term if total[o] is None else total[o] + term
        for o in range(GROUP):
            mixed[o, pl.ds(r0, CHUNK), :] = total[o]
    for pair in range(GROUP // 2):
        both = []
        for o in (2 * pair, 2 * pair + 1):
            high, low = halves(mixed[o])
            out = jnp.dot(jnp.concatenate([high, low], axis=1), matrix_x, preferred_element_type=jnp.float32)
            both.append(halves(out[:, :wide] + out[:, wide:]))
        high = jnp.concatenate([both[0][0], both[1][0]], axis=1)
        low = jnp.concatenate([both[0][1], both[1][1]], axis=1)
        out = jnp.dot(matrix_y, jnp.concatenate([high, high, low], axis=0), preferred_element_type=jnp.float32)
        finish(2 * pair, out[:, :wide])
        finish(2 * pair + 1, out[:, wide:])


def step_kernel(taps, kz, xf, xb, yf, yb, est, views, prod, ratio, mixed):
    own, outer = prod.shape[0], ratio.shape[0]
    for v in range(2):
        ahead = [kz[v, d] for d in range(taps)]
        behind = ahead[::-1]

        @pl.loop(0, outer // GROUP)
        def _(step):
            base = step * GROUP

            def finish(o, out):
                ratio[base + o] = views[v, base + o] / out

            convolve(taps, ahead, lambda i, r0: est[base + i, pl.ds(r0, CHUNK), :], xf[v], yf[v], mixed, finish)

        @pl.loop(0, own // GROUP)
        def _(step):
            base = step * GROUP

            def finish(o, out):
                prod[base + o] = out if v == 0 else prod[base + o] * out

            convolve(taps, behind, lambda i, r0: ratio[base + i, pl.ds(r0, CHUNK), :], xb[v], yb[v], mixed, finish)


def one_step(kz, xf, xb, yf, yb, est, views):
    taps = kz.shape[1]
    outer, rows, wide = views.shape[1:]
    own = outer - taps + 1
    vmem = pl.BlockSpec(memory_space=pltpu.VMEM)
    return pl.pallas_call(
        functools.partial(step_kernel, taps),
        name="rl_step",
        out_shape=jax.ShapeDtypeStruct((own, rows, wide), jnp.float32),
        in_specs=[pl.BlockSpec(memory_space=pltpu.SMEM)] + [vmem] * 6,
        out_specs=vmem,
        scratch_shapes=[
            pltpu.VMEM((outer, rows, wide), jnp.float32),
            pltpu.VMEM((GROUP, rows, wide), jnp.float32),
        ],
        compiler_params=pltpu.CompilerParams(vmem_limit_bytes=50 * 2**20),
    )(kz, xf, xb, yf, yb, est, views)


def on_device(views_data, start, psf_table, psf_index):
    planes, width_x, width_y = start.shape
    radius = (psf_table.shape[2] - 1) // 2
    members, count = lax.axis_size("view"), lax.axis_size("gz")
    half = width_y // 2
    window = half + 4 * radius
    member = lax.axis_index("view")
    upper, core = member // 2, member % 2
    first = upper * (width_y - window)

    across = [(i, (i + 2) % members) for i in range(members)]
    beside = [(i, i ^ 1) for i in range(members)]
    forward = [(i, i + 1) for i in range(count - 1)]
    backward = [(i + 1, i) for i in range(count - 1)]

    picked = (jnp.arange(psf_table.shape[0]) == psf_index[0]).astype(jnp.float32)
    kern = jnp.sum(picked[:, None, None] * psf_table, axis=0)
    kern = kern / jnp.sum(kern, axis=-1, keepdims=True)
    kerns = [kern, lax.ppermute(kern, "view", across)]
    kz = jnp.stack([k[0] for k in kerns])
    mx = [toeplitz(k[1], width_x) for k in kerns]
    my = [toeplitz(k[2], window) for k in kerns]
    xf = jnp.stack([lane_matrix(m.T) for m in mx])
    xb = jnp.stack([lane_matrix(m) for m in mx])
    yf = jnp.stack([row_matrix(m) for m in my])
    yb = jnp.stack([row_matrix(m.T) for m in my])

    slab = jnp.swapaxes(views_data[0], 1, 2)
    mine = lax.dynamic_slice_in_dim(slab, first, window, 1)
    theirs = lax.dynamic_slice_in_dim(slab, width_y - window - first, window, 1)
    both = jnp.stack([mine, lax.ppermute(theirs, "view", across)])
    low = lax.ppermute(both[:, planes - radius :], "gz", forward)
    high = lax.ppermute(both[:, :radius], "gz", backward)
    views = jnp.concatenate([low, both, high], axis=1)

    def widen(own):
        part = lax.dynamic_slice_in_dim(own, core * (planes // 2), planes // 2, 0)
        sides = []
        for way in (forward, backward):
            got = lax.ppermute(part, "gz", way)
            other = lax.ppermute(got, "view", beside)
            sides.append(
                jnp.concatenate([jnp.where(core == 0, got, other), jnp.where(core == 0, other, got)], axis=0)
            )
        return jnp.concatenate([sides[0], own, sides[1]], axis=0)

    est = lax.dynamic_slice_in_dim(jnp.swapaxes(start, 1, 2), first, window, 1)
    for step in range(ITERS):
        prod = one_step(kz, xf, xb, yf, yb, widen(est), views)
        prod = prod * lax.ppermute(prod, "view", beside)
        est = est * jnp.sqrt(jnp.sqrt(prod))
    own = lax.dynamic_slice_in_dim(est, upper * (window - half), half, 1)
    part = lax.dynamic_slice_in_dim(own, core * (planes // 2), planes // 2, 0)
    got = lax.ppermute(part, "view", across)
    other = lax.ppermute(got, "view", beside)
    rest = jnp.concatenate([jnp.where(core == 0, got, other), jnp.where(core == 0, other, got)], axis=0)
    result = jnp.concatenate([jnp.where(upper == 0, own, rest), jnp.where(upper == 0, rest, own)], axis=1)
    return jnp.swapaxes(result, 1, 2)


def solution(mesh):
    return jax.shard_map(
        on_device,
        mesh=mesh,
        in_specs=(P("view", "gz", None, None), P("gz", None, None), P(), P("view")),
        out_specs=P("gz", None, None),
        check_vma=False,
    )
```

```python
import functools

import jax
import jax.numpy as jnp
from jax import lax
from jax.experimental import pallas as pl
from jax.experimental.pallas import tpu as pltpu
from jax.sharding import PartitionSpec as P

MESH = pl.DeviceIdType.MESH
GROUP = 4
CHUNK = 32


def halves(value):
    high = value.astype(jnp.bfloat16)
    return high, (value - high.astype(jnp.float32)).astype(jnp.bfloat16)


def fill_bands(kern, taps, first_tap, ahead, behind, period, low_block):
    rows, cols = ahead.shape
    step = 32
    radius = (taps - 1) // 2

    @pl.loop(0, rows // step)
    def _(block):
        top = pl.multiple_of(block * step, step)
        row = lax.broadcasted_iota(jnp.int32, (step, cols), 0) + top
        col = lax.broadcasted_iota(jnp.int32, (step, cols), 1)
        is_low = (col >= low_block * period) & (col < (low_block + 1) * period)
        for wrap in range(cols // period - 1):
            col = jnp.where(col >= period, col - period, col)
        for wrap in range(rows // period - 1):
            row = jnp.where(row >= period, row - period, row)
        shift = col - row
        first = jnp.zeros((step, cols), jnp.float32)
        second = first
        for tap in range(taps):
            value = jnp.broadcast_to(kern[pl.ds(first_tap + tap, 1), pl.ds(0, 1)], (step, cols))
            first = jnp.where(shift == tap - radius, value, first)
            second = jnp.where(shift == radius - tap, value, second)
        for target, matrix in ((ahead, first), (behind, second)):
            high = matrix.astype(jnp.bfloat16).astype(jnp.float32)
            target[pl.ds(top, step), :] = jnp.where(is_low, matrix - high, high).astype(jnp.bfloat16)


def convolve(taps, coef, read, matrix_x, matrix_y, mixed, finish):
    rows = mixed.shape[1]
    wide = mixed.shape[2]
    for r0 in range(0, rows, CHUNK):
        total = [None] * GROUP
        for i in range(taps + GROUP - 1):
            value = read(i, r0)
            for o in range(GROUP):
                if 0 <= i - o < taps:
                    term = coef[i - o] * value
                    total[o] = term if total[o] is None else total[o] + term
        for o in range(GROUP):
            mixed[o, pl.ds(r0, CHUNK), :] = total[o]
    for pair in range(GROUP // 2):
        both = []
        for o in (2 * pair, 2 * pair + 1):
            high, low = halves(mixed[o])
            out = jnp.dot(jnp.concatenate([high, low], axis=1), matrix_x, preferred_element_type=jnp.float32)
            both.append(halves(out[:, :wide] + out[:, wide:]))
        high = jnp.concatenate([both[0][0], both[1][0]], axis=1)
        low = jnp.concatenate([both[0][1], both[1][1]], axis=1)
        out = jnp.dot(matrix_y, jnp.concatenate([high, high, low], axis=0), preferred_element_type=jnp.float32)
        finish(2 * pair, out[:, :wide])
        finish(2 * pair + 1, out[:, wide:])


def whole_kernel(
    taps, views_in, start_in, kern_in, out,
    vin, sin, kern, xf, xb, yf, yb, est1, est2, spare, views, theirs, ratio, mixed, prod, prod_in, result,
    load_sem, out_sem, kern_sem, z_sem, start_sem, extra_sem, pass_sem, view_sem, est_sem, prod_sem, last_sem,
):
    planes, full, wide = result.shape
    rows = views.shape[2]
    half = full // 2
    radius = (taps - 1) // 2
    valid = rows - radius
    known = rows - 2 * radius
    v = lax.axis_index("view")
    g = lax.axis_index("gz")
    last = lax.axis_size("gz") - 1
    upper, core = v // 2, v % 2
    lower = 1 - upper
    seam = (last + 1) // 2
    partner = {"view": (v + 2) % 4, "gz": g}
    sibling = {"view": v + 1 - 2 * core, "gz": g}
    beside = ({"view": v, "gz": g + 1}, {"view": v, "gz": g - 1})
    opposite = ({"view": (v + 2) % 4, "gz": g + 1}, {"view": (v + 2) % 4, "gz": g - 1})
    sends = (g < last, g > 0)
    receives = (g > 0, g < last)
    at_seam = (g == seam - 1, g == seam)

    loads = []
    for q in range(planes // GROUP):
        part = pl.ds(q * GROUP, GROUP)
        loads.append(
            (
                pltpu.make_async_copy(start_in.at[part], sin.at[part], load_sem.at[0, q]),
                pltpu.make_async_copy(views_in.at[part], vin.at[part], load_sem.at[1, q]),
            )
        )
        for copy in loads[-1]:
            copy.start()

    ones = jnp.ones((8, wide), jnp.float32)
    view_pad = pl.multiple_of(lower * valid, 8)
    est_pad = pl.multiple_of(lower * known, 8)

    @pl.loop(0, views.shape[1])
    def _(f):
        for which in range(2):
            views[which, f, pl.ds(view_pad, 8), :] = ones
        est2[f + jnp.where(f >= planes, planes, 0), pl.ds(est_pad, 8), :] = ones
        est2[f + jnp.where(f >= planes, planes, 0), pl.ds(est_pad + 8, 8), :] = ones

    for side in range(2):

        @pl.when(jnp.logical_not(receives[side]))
        def _():
            zero = jnp.zeros((rows, wide), jnp.float32)

            @pl.loop(0, planes)
            def _(p):
                est1[2 * planes * side + p] = zero
                est2[2 * planes * side + p] = zero

            @pl.loop(0, radius)
            def _(p):
                for which in range(2):
                    views[which, (planes + radius) * side + p] = zero

    barrier = pltpu.get_barrier_semaphore()
    for there in (partner, sibling):
        pl.semaphore_signal(barrier, inc=1, device_id=there, device_id_type=MESH)
    count = 2
    for side in range(2):

        @pl.when(sends[side])
        def _():
            pl.semaphore_signal(barrier, inc=1, device_id=beside[side], device_id_type=MESH)

        @pl.when(at_seam[side])
        def _():
            pl.semaphore_signal(barrier, inc=1, device_id=opposite[side], device_id_type=MESH)

        count = count + jnp.where(sends[side], 1, 0) + jnp.where(at_seam[side], 1, 0)
    pl.semaphore_wait(barrier, count)

    def remote(src, dst, sem, there):
        return pltpu.make_async_remote_copy(
            src_ref=src, dst_ref=dst, send_sem=sem.at[0], recv_sem=sem.at[1], device_id=there, device_id_type=MESH
        )

    def est_place(side, k, who):
        return 12 - 4 * who - 8 * k if side == 0 else 4 * who + 8 * k

    def est_copy(est, sem, side, k):
        high = rows if est is est1 else known
        offset = 0 if est is est1 else pl.multiple_of(upper * 2 * radius, 8)
        place = est_place(side, k, core)
        src = est.at[pl.ds(planes + place, GROUP), pl.ds(offset, high), :]
        dst = est.at[pl.ds(2 * planes * side + place, GROUP), pl.ds(offset, high), :]
        return remote(src, dst, sem.at[side, k], beside[side])

    def extra_copy(side, k):
        place = est_place(side, k, core)
        return pltpu.make_async_remote_copy(
            src_ref=spare.at[pl.ds(place, GROUP)],
            dst_ref=est1.at[pl.ds(2 * planes * side + place, GROUP)],
            send_sem=extra_sem.at[side, k],
            recv_sem=start_sem.at[side, k, 1],
            device_id=opposite[side],
            device_id_type=MESH,
        )

    def pass_copy(est, sem, side, k, who):
        high = rows if est is est1 else known
        offset = 0 if est is est1 else pl.multiple_of(upper * 2 * radius, 8)
        place = est.at[pl.ds(2 * planes * side + est_place(side, k, who), GROUP), pl.ds(offset, high), :]
        return remote(place, place, sem.at[side, k], sibling)

    my_rows = pl.ds(pl.multiple_of(upper * radius, 8), valid)
    other_rows = pl.ds(pl.multiple_of(lower * radius, 8), valid)
    z_planes = (12, 0, 8, 4)

    def z_copy(k):
        return remote(
            theirs.at[pl.ds(z_planes[k], GROUP), other_rows, :],
            views.at[1, pl.ds(radius + z_planes[k], GROUP), other_rows, :],
            z_sem.at[k],
            partner,
        )

    def z_arrival(k):
        here = views.at[1, pl.ds(radius + z_planes[k], GROUP), my_rows, :]
        return remote(here, here, z_sem.at[k], partner)

    def view_copy(which, side, k):
        src = (12 - 4 * k if side == 0 else 4 * k) + radius
        dst = 4 - 4 * k if side == 0 else planes + radius + 4 * k
        return remote(
            views.at[which, pl.ds(src, GROUP), my_rows, :],
            views.at[which, pl.ds(dst, GROUP), my_rows, :],
            view_sem.at[which, side, k],
            beside[side],
        )

    def direct_copy(side, k):
        src = 12 - 4 * k if side == 0 else 4 * k
        dst = 4 - 4 * k if side == 0 else planes + radius + 4 * k
        return remote(
            theirs.at[pl.ds(src, GROUP), other_rows, :],
            views.at[1, pl.ds(dst, GROUP), other_rows, :],
            view_sem.at[1, side, k],
            opposite[side],
        )

    def prod_copy(i, q):
        part = pl.ds(q * GROUP, GROUP)
        return remote(prod.at[i, part], prod_in.at[i, part], prod_sem.at[i, q], sibling)

    kern_copy = remote(kern_in, kern.at[1], kern_sem, partner)
    kern_copy.start()
    kern[0] = kern_in[...]

    def turn(source, p, own, other):
        @pl.when(upper == 0)
        def _():
            own[...] = source[p, :, pl.ds(0, 256)].T[:rows]
            other[...] = source[p, :, pl.ds(128, 256)].T[256 - rows :]

        @pl.when(upper == 1)
        def _():
            own[...] = source[p, :, pl.ds(128, 256)].T[256 - rows :]
            other[...] = source[p, :, pl.ds(0, 256)].T[:rows]

    for q in range(planes // GROUP):
        loads[q][0].wait()

    @pl.loop(0, planes)
    def _(p):
        turn(sin, p, est1.at[planes + p], spare.at[p])

    plain = [jnp.logical_not(at_seam[side]) for side in range(2)]
    for k in range(2):
        for side in range(2):

            @pl.when(sends[side] & (plain[side] | (upper == core)))
            def _():
                est_copy(est1, start_sem, side, k).start()

            @pl.when(at_seam[side] & (upper == core))
            def _():
                extra_copy(side, k).start()

    for q in range(planes // GROUP):
        loads[q][1].wait()

    @pl.loop(0, planes)
    def _(p):
        turn(vin, p, views.at[0, radius + p], theirs.at[p])

    for k in range(4):
        z_copy(k).start()
    for k in range(2):
        for side in range(2):

            @pl.when(sends[side])
            def _():
                view_copy(0, side, k).start()

    def bands(which):
        fill_bands(kern.at[which], taps, taps, xb.at[which], xf.at[which], wide, 1)
        fill_bands(kern.at[which], taps, 2 * taps, yf.at[which], yb.at[which], rows, 1)

    bands(0)
    kern_copy.wait_recv()
    bands(1)

    def ahead_group(est, which, group, divide):
        base = group * GROUP
        coef = [kern[which, pl.ds(d, 1), :] for d in range(taps)]

        def finish(o, value):
            ratio[which, base + o] = views[which, base + o] / value if divide else value

        convolve(taps, coef, lambda i, r0: est[base + i, pl.ds(r0, CHUNK), :], xf[which], yf[which], mixed, finish)

    def back_group(i, which, group):
        base = group * GROUP
        coef = [kern[which, pl.ds(taps - 1 - d, 1), :] for d in range(taps)]

        def finish(o, value):
            prod[i, base + o] = value if which == 0 else prod[i, base + o] * value

        convolve(
            taps, coef, lambda j, r0: ratio[which, base + j, pl.ds(r0, CHUNK), :], xb[which], yb[which], mixed, finish
        )

    def arrive(est, sem, side_sem, k):
        for side in range(2):

            @pl.when(receives[side])
            def _():
                est_copy(est, sem, side, k).wait_recv()
                pass_copy(est, side_sem, side, k, core).start()

        for side in range(2):

            @pl.when(receives[side])
            def _():
                pass_copy(est, side_sem, side, k, 1 - core).wait_recv()

    def ahead(est, groups, divide):
        first, number, stride = groups

        @pl.loop(0, 2)
        def _(which):
            @pl.loop(0, number)
            def _(n):
                ahead_group(est, which, first + stride * n, divide)

    arrive(est1, start_sem, pass_sem.at[0], 0)
    ahead(est1, (2, 4, 1), False)
    arrive(est1, start_sem, pass_sem.at[0], 1)

    @pl.loop(0, 2)
    def _(which):
        @pl.loop(0, 4)
        def _(n):
            ahead_group(est1, which, n + 4 * (n // 2), False)

    for k in range(4):
        side, piece = k % 2, k // 2
        z_arrival(k).wait_recv()

        @pl.when(sends[side] & plain[side])
        def _():
            view_copy(1, side, piece).start()

        @pl.when(at_seam[side])
        def _():
            direct_copy(side, piece).start()

    def divide(which, first, number):
        @pl.loop(first, first + number)
        def _(f):
            ratio[which, f] = views[which, f] / ratio[which, f]

    for k in range(2):
        for side in range(2):

            @pl.when(receives[side])
            def _():
                view_copy(0, side, k).wait_recv()

    divide(0, 0, planes + 2 * radius)

    @pl.loop(0, planes // GROUP)
    def _(group):
        back_group(0, 0, group)

    def update(i, est, q, store):
        prod_copy(i, q).wait_recv()
        for o in range(GROUP):
            p = q * GROUP + o
            both = prod[i, p] * prod_in[i, p]
            store(p, est[planes + p] * jnp.sqrt(jnp.sqrt(both)))

    def keep(p, value):
        est2[planes + p] = value

    for k in range(2):
        for side in range(2):

            @pl.when(receives[side])
            def _():
                view_copy(1, side, k).wait_recv()

        if k == 0:
            divide(1, 4, planes + 2 * radius - 8)
        else:
            divide(1, 0, 4)
            divide(1, planes + 2 * radius - 4, 4)
        groups = (1, 2) if k == 0 else (0, 3)

        @pl.loop(0, 2)
        def _(n):
            back_group(0, 1, n + 1 if k == 0 else 3 * n)

        for q in groups:
            prod_copy(0, q).start()
        for q in groups:
            update(0, est1, q, keep)
        for side in range(2):
            if k == 0:

                @pl.when(sends[side] & (core == 1))
                def _():
                    est_copy(est2, est_sem, side, 0).start()
            else:

                @pl.when(sends[side] & (core == 0))
                def _():
                    est_copy(est2, est_sem, side, 0).start()
    for side in range(2):

        @pl.when(sends[side])
        def _():
            est_copy(est2, est_sem, side, 1).start()

    arrive(est2, est_sem, pass_sem.at[1], 0)
    ahead(est2, (2, 4, 1), True)
    arrive(est2, est_sem, pass_sem.at[1], 1)

    @pl.loop(0, 2)
    def _(which):
        @pl.loop(0, 4)
        def _(n):
            ahead_group(est2, which, n + 4 * (n // 2), True)

    own_rows = pl.ds(pl.multiple_of(upper * half, 8), half)
    rest_rows = pl.ds(pl.multiple_of(lower * half, 8), half)
    inner = pl.multiple_of(upper * (rows - half), 8)

    def last_copy(q):
        part = result.at[pl.ds(q * GROUP, GROUP), own_rows, :]
        return remote(part, part, last_sem.at[0, q], partner)

    def last_arrival(q):
        part = result.at[pl.ds(q * GROUP, GROUP), rest_rows, :]
        return remote(part, part, last_sem.at[0, q], partner)

    def last_pass(q):
        part = result.at[pl.ds(q * GROUP, GROUP), rest_rows, :]
        return remote(part, part, last_sem.at[1, q], sibling)

    def out_copy(q):
        part = pl.ds(q * GROUP, GROUP)
        return pltpu.make_async_copy(result.at[part], out.at[part], out_sem.at[q])

    for q in range(planes // GROUP):
        back_group(1, 0, q)
        back_group(1, 1, q)
        prod_copy(1, q).start()
        prod_copy(1, q).wait_recv()
        for o in range(GROUP):
            p = q * GROUP + o
            both = prod[1, p] * prod_in[1, p]
            prod_in[0, p] = est2[planes + p] * jnp.sqrt(jnp.sqrt(both))
            result[p, own_rows, :] = prod_in[0, p, pl.ds(inner, half), :]

        @pl.when(core == q % 2)
        def _():
            last_copy(q).start()

    for q in range(planes // GROUP):

        @pl.when(core == q % 2)
        def _():
            last_arrival(q).wait_recv()
            last_pass(q).start()

    for q in range(planes // GROUP):

        @pl.when(core != q % 2)
        def _():
            last_pass(q).wait_recv()

        out_copy(q).start()

    kern_copy.wait_send()
    for k in range(4):
        z_copy(k).wait_send()
        prod_copy(0, k).wait_send()
        prod_copy(1, k).wait_send()
    for q in range(planes // GROUP):

        @pl.when(core == q % 2)
        def _():
            last_copy(q).wait_send()
            last_pass(q).wait_send()

        out_copy(q).wait()
    for side in range(2):
        for k in range(2):

            @pl.when(sends[side])
            def _():
                view_copy(0, side, k).wait_send()
                view_copy(1, side, k).wait_send()
                est_copy(est2, est_sem, side, k).wait_send()

            @pl.when(sends[side] & (plain[side] | (upper == core)))
            def _():
                est_copy(est1, start_sem, side, k).wait_send()

            @pl.when(at_seam[side] & (upper == core))
            def _():
                extra_copy(side, k).wait_send()

            @pl.when(receives[side])
            def _():
                pass_copy(est1, pass_sem.at[0], side, k, core).wait_send()
                pass_copy(est2, pass_sem.at[1], side, k, core).wait_send()


def turn_back(source, target):
    for p in range(source.shape[0]):
        target[p] = source[p].T


def on_device(views_data, start, psf_table, psf_index):
    planes, width_x, width_y = start.shape
    taps = psf_table.shape[2]
    radius = (taps - 1) // 2
    rows = width_y // 2 + 4 * radius
    outer = planes + 2 * radius

    picked = (jnp.arange(psf_table.shape[0]) == psf_index[0]).astype(jnp.float32)
    kern = jnp.sum(picked[:, None, None] * psf_table, axis=0)
    kern = kern / jnp.sum(kern, axis=-1, keepdims=True)
    kern = jnp.broadcast_to(jnp.pad(kern.reshape(-1), (0, -kern.size % 8))[:, None], (kern.size + -kern.size % 8, 128))

    f32, bf16 = jnp.float32, jnp.bfloat16
    plane = (rows, width_x)
    dma = pltpu.SemaphoreType.DMA
    anywhere = pl.BlockSpec(memory_space=pl.ANY)
    turned = pl.pallas_call(
        functools.partial(whole_kernel, taps),
        name="deconvolve",
        out_shape=jax.ShapeDtypeStruct((planes, width_y, width_x), f32),
        in_specs=[anywhere, anywhere, pl.BlockSpec(memory_space=pltpu.VMEM)],
        out_specs=anywhere,
        scratch_shapes=[
            pltpu.VMEM((planes, width_x, width_y), f32),
            pltpu.VMEM((planes, width_x, width_y), f32),
            pltpu.VMEM((2,) + kern.shape, f32),
            pltpu.VMEM((2, 2 * width_x, 2 * width_x), bf16),
            pltpu.VMEM((2, 2 * width_x, 2 * width_x), bf16),
            pltpu.VMEM((2, rows, 3 * rows), bf16),
            pltpu.VMEM((2, rows, 3 * rows), bf16),
            pltpu.VMEM((3 * planes,) + plane, f32),
            pltpu.VMEM((3 * planes,) + plane, f32),
            pltpu.VMEM((planes,) + plane, f32),
            pltpu.VMEM((2, outer) + plane, f32),
            pltpu.VMEM((planes,) + plane, f32),
            pltpu.VMEM((2, outer) + plane, f32),
            pltpu.VMEM((GROUP,) + plane, f32),
            pltpu.VMEM((2, planes) + plane, f32),
            pltpu.VMEM((2, planes) + plane, f32),
            pltpu.VMEM((planes, width_y, width_x), f32),
            dma((2, 4)),
            dma((4,)),
            dma((2,)),
            dma((4, 2)),
            dma((2, 2, 2)),
            dma((2, 2)),
            dma((2, 2, 2, 2)),
            dma((2, 2, 2, 2)),
            dma((2, 2, 2)),
            dma((2, 4, 2)),
            dma((2, 4, 2)),
        ],
        compiler_params=pltpu.CompilerParams(
            collective_id=0, has_side_effects=True, vmem_limit_bytes=60 * 2**20
        ),
    )(views_data[0], start, kern)
    return pl.pallas_call(
        turn_back,
        name="turn_back",
        grid=(planes // GROUP,),
        out_shape=jax.ShapeDtypeStruct(start.shape, f32),
        in_specs=[pl.BlockSpec((GROUP, width_y, width_x), lambda q: (q, 0, 0))],
        out_specs=pl.BlockSpec((GROUP, width_x, width_y), lambda q: (q, 0, 0)),
    )(turned)


def solution(mesh):
    return jax.shard_map(
        on_device,
        mesh=mesh,
        in_specs=(P("view", "gz", None, None), P("gz", None, None), P(), P("view")),
        out_specs=P("gz", None, None),
        check_vma=False,
    )
```

```python
import functools

import jax
import jax.numpy as jnp
from jax import lax
from jax.experimental import pallas as pl
from jax.experimental.pallas import tpu as pltpu
from jax.sharding import PartitionSpec as P

MESH = pl.DeviceIdType.MESH
GROUP = 4
CHUNK = 32


def halves(value):
    high = value.astype(jnp.bfloat16)
    return high, (value - high.astype(jnp.float32)).astype(jnp.bfloat16)


def fill_bands(kern, taps, first_tap, ahead, behind, period, low_block):
    rows, cols = ahead.shape
    step = 32
    radius = (taps - 1) // 2

    @pl.loop(0, rows // step)
    def _(block):
        top = pl.multiple_of(block * step, step)
        row = lax.broadcasted_iota(jnp.int32, (step, cols), 0) + top
        col = lax.broadcasted_iota(jnp.int32, (step, cols), 1)
        is_low = (col >= low_block * period) & (col < (low_block + 1) * period)
        for wrap in range(cols // period - 1):
            col = jnp.where(col >= period, col - period, col)
        for wrap in range(rows // period - 1):
            row = jnp.where(row >= period, row - period, row)
        shift = col - row
        first = jnp.zeros((step, cols), jnp.float32)
        second = first
        for tap in range(taps):
            value = jnp.broadcast_to(kern[pl.ds(first_tap + tap, 1), pl.ds(0, 1)], (step, cols))
            first = jnp.where(shift == tap - radius, value, first)
            second = jnp.where(shift == radius - tap, value, second)
        for target, matrix in ((ahead, first), (behind, second)):
            high = matrix.astype(jnp.bfloat16).astype(jnp.float32)
            target[pl.ds(top, step), :] = jnp.where(is_low, matrix - high, high).astype(jnp.bfloat16)


def convolve(taps, coef, read, matrix_x, matrix_y, mixed, finish):
    rows = mixed.shape[1]
    wide = mixed.shape[2]
    for r0 in range(0, rows, CHUNK):
        total = [None] * GROUP
        for i in range(taps + GROUP - 1):
            value = read(i, r0)
            for o in range(GROUP):
                if 0 <= i - o < taps:
                    term = coef[i - o] * value
                    total[o] = term if total[o] is None else total[o] + term
        for o in range(GROUP):
            mixed[o, pl.ds(r0, CHUNK), :] = total[o]
    for pair in range(GROUP // 2):
        both = []
        for o in (2 * pair, 2 * pair + 1):
            high, low = halves(mixed[o])
            out = jnp.dot(jnp.concatenate([high, low], axis=1), matrix_x, preferred_element_type=jnp.float32)
            both.append(halves(out[:, :wide] + out[:, wide:]))
        high = jnp.concatenate([both[0][0], both[1][0]], axis=1)
        low = jnp.concatenate([both[0][1], both[1][1]], axis=1)
        out = jnp.dot(matrix_y, jnp.concatenate([high, high, low], axis=0), preferred_element_type=jnp.float32)
        finish(2 * pair, out[:, :wide])
        finish(2 * pair + 1, out[:, wide:])


def whole_kernel(
    taps, views_in, start_in, kern_in, out,
    vin, sin, kern, xf, xb, yf, yb, est1, est2, spare, views, theirs, ratio, mixed, prod, prod_in, result, hop,
    load_sem, out_sem, kern_sem, z_sem, start_sem, extra_sem, pass_sem, view_sem, est_sem, prod_sem, last_sem,
    hop_sem, onward_sem,
):
    planes, full, wide = result.shape
    rows = views.shape[2]
    half = full // 2
    radius = (taps - 1) // 2
    valid = rows - radius
    known = rows - 2 * radius
    v = lax.axis_index("view")
    g = lax.axis_index("gz")
    last = lax.axis_size("gz") - 1
    upper, core = v // 2, v % 2
    lower = 1 - upper
    seam = (last + 1) // 2
    partner = {"view": (v + 2) % 4, "gz": g}
    sibling = {"view": v + 1 - 2 * core, "gz": g}
    beside = ({"view": v, "gz": g + 1}, {"view": v, "gz": g - 1})
    opposite = ({"view": (v + 2) % 4, "gz": g + 1}, {"view": (v + 2) % 4, "gz": g - 1})
    sends = (g < last, g > 0)
    receives = (g > 0, g < last)
    at_seam = (g == seam - 1, g == seam)

    loads = []
    for q in range(planes // GROUP):
        part = pl.ds(q * GROUP, GROUP)
        loads.append(
            (
                pltpu.make_async_copy(start_in.at[part], sin.at[part], load_sem.at[0, q]),
                pltpu.make_async_copy(views_in.at[part], vin.at[part], load_sem.at[1, q]),
            )
        )
        for copy in loads[-1]:
            copy.start()

    relays = ({"view": v, "gz": last}, {"view": v, "gz": 0})
    relays_across = ({"view": (v + 2) % 4, "gz": last}, {"view": (v + 2) % 4, "gz": 0})
    at_relay = (g == last, g == 0)
    sources = ({"view": v, "gz": seam - 1}, {"view": v, "gz": seam})
    sources_across = ({"view": (v + 2) % 4, "gz": seam - 1}, {"view": (v + 2) % 4, "gz": seam})

    barrier = pltpu.get_barrier_semaphore()

    def greet(there):
        pl.semaphore_signal(barrier, inc=1, device_id=there, device_id_type=MESH)

    greet(partner)
    greet(sibling)
    count = 2
    for side in range(2):

        @pl.when(sends[side])
        def _():
            greet(beside[side])

        @pl.when(at_seam[side])
        def _():
            greet(opposite[side])
            greet(relays[side])
            greet(relays_across[side])
            greet(relays[1 - side])

        @pl.when(at_relay[side])
        def _():
            greet(sources[side])
            greet(sources_across[side])
            greet(sources[1 - side])

        count = count + jnp.where(sends[side], 1, 0) + jnp.where(at_seam[side], 4, 0) + jnp.where(at_relay[side], 3, 0)

    def remote(src, dst, sem, there):
        return pltpu.make_async_remote_copy(
            src_ref=src, dst_ref=dst, send_sem=sem.at[0], recv_sem=sem.at[1], device_id=there, device_id_type=MESH
        )

    def est_place(side, k, who):
        return 14 - 2 * who - 4 * k if side == 0 else 2 * who + 4 * k

    def est_copy(est, sem, side, k):
        high = rows if est is est1 else known
        offset = 0 if est is est1 else pl.multiple_of(upper * 2 * radius, 8)
        place = est_place(side, k, core)
        src = est.at[pl.ds(planes + place, 2), pl.ds(offset, high), :]
        dst = est.at[pl.ds(2 * planes * side + place, 2), pl.ds(offset, high), :]
        return remote(src, dst, sem.at[side, k], beside[side])

    def extra_copy(side, k):
        place = est_place(side, k, core)
        return pltpu.make_async_remote_copy(
            src_ref=spare.at[pl.ds(place, 2)],
            dst_ref=est1.at[pl.ds(2 * planes * side + place, 2)],
            send_sem=extra_sem.at[side, k],
            recv_sem=start_sem.at[side, k, 1],
            device_id=opposite[side],
            device_id_type=MESH,
        )

    def pass_copy(est, sem, side, k, who):
        high = rows if est is est1 else known
        offset = 0 if est is est1 else pl.multiple_of(upper * 2 * radius, 8)
        place = est.at[pl.ds(2 * planes * side + est_place(side, k, who), 2), pl.ds(offset, high), :]
        return remote(place, place, sem.at[side, k], sibling)

    my_rows = pl.ds(pl.multiple_of(upper * radius, 8), valid)
    other_rows = pl.ds(pl.multiple_of(lower * radius, 8), valid)
    z_planes = (12, 0, 8, 4)

    def z_copy(k):
        return remote(
            theirs.at[pl.ds(z_planes[k], GROUP), other_rows, :],
            views.at[1, pl.ds(radius + z_planes[k], GROUP), other_rows, :],
            z_sem.at[k],
            partner,
        )

    def z_arrival(k):
        here = views.at[1, pl.ds(radius + z_planes[k], GROUP), my_rows, :]
        return remote(here, here, z_sem.at[k], partner)

    def view_copy(which, side, k):
        src = (12 - 4 * k if side == 0 else 4 * k) + radius
        dst = 4 - 4 * k if side == 0 else planes + radius + 4 * k
        return remote(
            views.at[which, pl.ds(src, GROUP), my_rows, :],
            views.at[which, pl.ds(dst, GROUP), my_rows, :],
            view_sem.at[which, side, k],
            beside[side],
        )

    def direct_copy(side, k):
        src = 12 - 4 * k if side == 0 else 4 * k
        dst = 4 - 4 * k if side == 0 else planes + radius + 4 * k
        return remote(
            theirs.at[pl.ds(src, GROUP), other_rows, :],
            views.at[1, pl.ds(dst, GROUP), other_rows, :],
            view_sem.at[1, side, k],
            opposite[side],
        )

    def hop_copy(slot, src, high, send, there):
        return pltpu.make_async_remote_copy(
            src_ref=src,
            dst_ref=hop.at[slot, pl.ds(0, src.shape[0]), high, :],
            send_sem=hop_sem.at[0, send],
            recv_sem=hop_sem.at[1, slot],
            device_id=there,
            device_id_type=MESH,
        )

    def hop_start(side, k, across):
        place = est_place(side, k, core)
        src = spare.at[pl.ds(place, 2)] if across else est1.at[pl.ds(planes + place, 2)]
        there = relays_across[side] if across else relays[side]
        return hop_copy(k, src, pl.ds(0, rows), k + 2 * across, there)

    def hop_view(side, across):
        src = 8 if side == 0 else 4
        part = pl.ds(src, GROUP)
        if across:
            return hop_copy(1, theirs.at[part, other_rows, :], other_rows, 1, relays_across[side])
        return hop_copy(0, views.at[0, pl.ds(radius + src, GROUP), my_rows, :], my_rows, 0, relays[side])

    def onward(slot, side):
        target = sources[1 - side]
        if slot >= 2:
            src = hop.at[slot, pl.ds(0, 2)]
            dst = est1.at[pl.ds(2 * planes * side + est_place(side, slot, core), 2)]
            recv = start_sem.at[side, slot, 1]
        else:
            src = hop.at[slot, pl.ds(0, GROUP), my_rows, :]
            dst = views.at[slot, pl.ds(0 if side == 0 else planes + radius + 4, GROUP), my_rows, :]
            recv = view_sem.at[slot, side, 1, 1]
        return pltpu.make_async_remote_copy(
            src_ref=src,
            dst_ref=dst,
            send_sem=onward_sem.at[0, slot],
            recv_sem=recv,
            device_id=target,
            device_id_type=MESH,
        )

    def hop_arrival(slot):
        here = hop.at[slot, pl.ds(0, 2)] if slot >= 2 else hop.at[slot, pl.ds(0, GROUP), my_rows, :]
        return pltpu.make_async_remote_copy(
            src_ref=here,
            dst_ref=here,
            send_sem=onward_sem.at[1, slot],
            recv_sem=hop_sem.at[1, slot],
            device_id=partner,
            device_id_type=MESH,
        )

    def serve(slots):
        for side in range(2):

            @pl.when(at_relay[side])
            def _():
                for slot in slots:
                    hop_arrival(slot).wait_recv()
                    onward(slot, side).start()

    def prod_copy(i, q):
        part = pl.ds(q * GROUP, GROUP)
        return remote(prod.at[i, part], prod_in.at[i, part], prod_sem.at[i, q], sibling)

    def turn(source, p, own, other):
        @pl.when(upper == 0)
        def _():
            own[...] = source[p, :, pl.ds(0, 256)].T[:rows]
            other[...] = source[p, :, pl.ds(128, 256)].T[256 - rows :]

        @pl.when(upper == 1)
        def _():
            own[...] = source[p, :, pl.ds(128, 256)].T[256 - rows :]
            other[...] = source[p, :, pl.ds(0, 256)].T[:rows]

    plain = [jnp.logical_not(at_seam[side]) for side in range(2)]

    def turn_start(q):
        loads[q][0].wait()

        @pl.loop(q * GROUP, (q + 1) * GROUP)
        def _(p):
            turn(sin, p, est1.at[planes + p], spare.at[p])

    def send_start(k):
        for side in range(2):

            @pl.when(sends[side] & plain[side])
            def _():
                est_copy(est1, start_sem, side, k).start()

            @pl.when(at_seam[side] & (upper == core))
            def _():
                if k < 2:
                    est_copy(est1, start_sem, side, k).start()
                    extra_copy(side, k).start()
                else:
                    hop_start(side, k, 0).start()
                    hop_start(side, k, 1).start()

    with jax.named_scope("turn_start"):
        turn_start(3)
        turn_start(0)
    with jax.named_scope("barrier"):
        pl.semaphore_wait(barrier, count)
    with jax.named_scope("turn_rest"):
        send_start(0)
        kern_copy = remote(kern_in, kern.at[1], kern_sem, partner)
        kern_copy.start()
        turn_start(2)
        turn_start(1)
        for k in range(1, 4):
            send_start(k)
    with jax.named_scope("turn_views"):
        for k in range(4):
            q = z_planes[k] // GROUP
            loads[q][1].wait()

            @pl.loop(q * GROUP, (q + 1) * GROUP)
            def _(p):
                turn(vin, p, views.at[0, radius + p], theirs.at[p])

            z_copy(k).start()
        for k in range(2):
            for side in range(2):

                @pl.when(sends[side] & plain[side])
                def _():
                    view_copy(0, side, k).start()

    kern[0] = kern_in[...]
    ones = jnp.ones((8, wide), jnp.float32)
    view_pad = pl.multiple_of(lower * valid, 8)
    est_pad = pl.multiple_of(lower * known, 8)

    @pl.loop(0, views.shape[1])
    def _(f):
        for which in range(2):
            views[which, f, pl.ds(view_pad, 8), :] = ones
        est2[f + jnp.where(f >= planes, planes, 0), pl.ds(est_pad, 8), :] = ones
        est2[f + jnp.where(f >= planes, planes, 0), pl.ds(est_pad + 8, 8), :] = ones

    for side in range(2):

        @pl.when(jnp.logical_not(receives[side]))
        def _():
            zero = jnp.zeros((rows, wide), jnp.float32)

            @pl.loop(0, planes)
            def _(p):
                est1[2 * planes * side + p] = zero
                est2[2 * planes * side + p] = zero

            @pl.loop(0, radius)
            def _(p):
                for which in range(2):
                    views[which, (planes + radius) * side + p] = zero

    def bands(which):
        fill_bands(kern.at[which], taps, taps, xb.at[which], xf.at[which], wide, 1)
        fill_bands(kern.at[which], taps, 2 * taps, yf.at[which], yb.at[which], rows, 1)

    with jax.named_scope("bands"):
        bands(0)
        kern_copy.wait_recv()
        bands(1)

    def ahead_group(est, which, group, divide):
        base = group * GROUP
        coef = [kern[which, pl.ds(d, 1), :] for d in range(taps)]

        def finish(o, value):
            ratio[which, base + o] = views[which, base + o] / value if divide else value

        convolve(taps, coef, lambda i, r0: est[base + i, pl.ds(r0, CHUNK), :], xf[which], yf[which], mixed, finish)

    def back_group(i, which, group):
        base = group * GROUP
        coef = [kern[which, pl.ds(taps - 1 - d, 1), :] for d in range(taps)]

        def finish(o, value):
            prod[i, base + o] = value if which == 0 else prod[i, base + o] * value

        convolve(
            taps, coef, lambda j, r0: ratio[which, base + j, pl.ds(r0, CHUNK), :], xb[which], yb[which], mixed, finish
        )

    def arrive(est, sem, side_sem, k):
        for side in range(2):

            @pl.when(receives[side])
            def _():
                est_copy(est, sem, side, k).wait_recv()
                pass_copy(est, side_sem, side, k, core).start()

        for side in range(2):

            @pl.when(receives[side])
            def _():
                pass_copy(est, side_sem, side, k, 1 - core).wait_recv()

    def ahead(est, k, divide):
        @pl.loop(0, 2)
        def _(which):
            @pl.loop(0, 2)
            def _(n):
                ahead_group(est, which, 3 - k + n * (2 * k + 1), divide)

    with jax.named_scope("ahead1"):

        @pl.loop(0, 4)
        def _(k):
            with jax.named_scope("arrive1"):
                arrive(est1, start_sem, pass_sem.at[0], k)

                @pl.when(k == 1)
                def _():
                    serve((2, 3))

            ahead(est1, k, False)

    for side in range(2):

        @pl.when(at_seam[side])
        def _():
            view_copy(0, side, 0).start()
            hop_view(side, 0).start()
            direct_copy(side, 0).start()
            hop_view(side, 1).start()

    for k in range(4):
        side, piece = k % 2, k // 2
        with jax.named_scope("wait_z"):
            z_arrival(k).wait_recv()

        @pl.when(sends[side] & plain[side])
        def _():
            view_copy(1, side, piece).start()

    serve((0, 1))

    def divide(which, first, number):
        @pl.loop(first, first + number)
        def _(f):
            ratio[which, f] = views[which, f] / ratio[which, f]

    with jax.named_scope("wait_own"):
        for k in range(2):
            for side in range(2):

                @pl.when(receives[side])
                def _():
                    view_copy(0, side, k).wait_recv()

    with jax.named_scope("back1own"):
        divide(0, 0, planes + 2 * radius)

        @pl.loop(0, planes // GROUP)
        def _(group):
            back_group(0, 0, group)

    def update(i, est, q, store):
        prod_copy(i, q).wait_recv()
        for o in range(GROUP):
            p = q * GROUP + o
            both = prod[i, p] * prod_in[i, p]
            store(p, est[planes + p] * jnp.sqrt(jnp.sqrt(both)))

    def keep(p, value):
        est2[planes + p] = value

    for k in range(2):
        with jax.named_scope("wait_other"):
            for side in range(2):

                @pl.when(receives[side])
                def _():
                    view_copy(1, side, k).wait_recv()

        with jax.named_scope("back1other"):
            if k == 0:
                divide(1, 4, planes + 2 * radius - 8)
            else:
                divide(1, 0, 4)
                divide(1, planes + 2 * radius - 4, 4)
            groups = (1, 2) if k == 0 else (0, 3)

            @pl.loop(0, 2)
            def _(n):
                back_group(0, 1, n + 1 if k == 0 else 3 * n)

        with jax.named_scope("update1"):
            for q in groups:
                prod_copy(0, q).start()
            for q in groups:
                update(0, est1, q, keep)
        for piece in (1,) if k == 0 else (0, 2, 3):
            for side in range(2):

                @pl.when(sends[side])
                def _():
                    est_copy(est2, est_sem, side, piece).start()

    @pl.loop(0, 4)
    def _(k):
        with jax.named_scope("arrive2"):
            arrive(est2, est_sem, pass_sem.at[1], k)
        with jax.named_scope("ahead2"):
            ahead(est2, k, True)

    own_rows = pl.ds(pl.multiple_of(upper * half, 8), half)
    rest_rows = pl.ds(pl.multiple_of(lower * half, 8), half)
    inner = pl.multiple_of(upper * (rows - half), 8)

    def last_copy(q):
        part = result.at[pl.ds(q * GROUP, GROUP), own_rows, :]
        return remote(part, part, last_sem.at[0, q], partner)

    def last_arrival(q):
        part = result.at[pl.ds(q * GROUP, GROUP), rest_rows, :]
        return remote(part, part, last_sem.at[0, q], partner)

    def last_pass(q):
        part = result.at[pl.ds(q * GROUP, GROUP), rest_rows, :]
        return remote(part, part, last_sem.at[1, q], sibling)

    def out_copy(q):
        part = pl.ds(q * GROUP, GROUP)
        return pltpu.make_async_copy(result.at[part], out.at[part], out_sem.at[q])

    def finish_group(q):
        prod_copy(1, q).wait_recv()
        for o in range(GROUP):
            p = q * GROUP + o
            both = prod[1, p] * prod_in[1, p]
            prod_in[0, p] = est2[planes + p] * jnp.sqrt(jnp.sqrt(both))
            result[p, own_rows, :] = prod_in[0, p, pl.ds(inner, half), :]

        @pl.when(core == q % 2)
        def _():
            last_copy(q).start()

    @pl.loop(0, planes // GROUP)
    def _(q):
        with jax.named_scope("back2"):
            back_group(1, 0, q)
            back_group(1, 1, q)
            prod_copy(1, q).start()
        with jax.named_scope("update2"):

            @pl.when(q > 0)
            def _():
                finish_group(q - 1)

    with jax.named_scope("update2"):
        finish_group(planes // GROUP - 1)

    with jax.named_scope("wait_last"):
        for q in range(planes // GROUP):

            @pl.when(core == q % 2)
            def _():
                last_arrival(q).wait_recv()
                last_pass(q).start()

    for q in range(planes // GROUP):

        @pl.when(core != q % 2)
        def _():
            last_pass(q).wait_recv()

        out_copy(q).start()

    kern_copy.wait_send()
    for k in range(4):
        z_copy(k).wait_send()
        prod_copy(0, k).wait_send()
        prod_copy(1, k).wait_send()
    for q in range(planes // GROUP):

        @pl.when(core == q % 2)
        def _():
            last_copy(q).wait_send()
            last_pass(q).wait_send()

        out_copy(q).wait()
    for side in range(2):
        for k in range(4):

            @pl.when(sends[side])
            def _():
                est_copy(est2, est_sem, side, k).wait_send()

            @pl.when(sends[side] & plain[side])
            def _():
                est_copy(est1, start_sem, side, k).wait_send()

            @pl.when(at_seam[side] & (upper == core))
            def _():
                if k < 2:
                    est_copy(est1, start_sem, side, k).wait_send()
                    extra_copy(side, k).wait_send()
                else:
                    hop_start(side, k, 0).wait_send()
                    hop_start(side, k, 1).wait_send()

            @pl.when(receives[side])
            def _():
                pass_copy(est1, pass_sem.at[0], side, k, core).wait_send()
                pass_copy(est2, pass_sem.at[1], side, k, core).wait_send()

        for k in range(2):

            @pl.when(sends[side] & plain[side])
            def _():
                view_copy(0, side, k).wait_send()
                view_copy(1, side, k).wait_send()

        @pl.when(at_seam[side])
        def _():
            view_copy(0, side, 0).wait_send()
            hop_view(side, 0).wait_send()
            direct_copy(side, 0).wait_send()
            hop_view(side, 1).wait_send()

        @pl.when(at_relay[side])
        def _():
            for slot in range(4):
                onward(slot, side).wait_send()


def turn_back(source, target):
    for p in range(source.shape[0]):
        target[p] = source[p].T


def on_device(views_data, start, psf_table, psf_index):
    planes, width_x, width_y = start.shape
    taps = psf_table.shape[2]
    radius = (taps - 1) // 2
    rows = width_y // 2 + 4 * radius
    outer = planes + 2 * radius

    picked = (jnp.arange(psf_table.shape[0]) == psf_index[0]).astype(jnp.float32)
    kern = jnp.sum(picked[:, None, None] * psf_table, axis=0)
    kern = kern / jnp.sum(kern, axis=-1, keepdims=True)
    kern = jnp.broadcast_to(jnp.pad(kern.reshape(-1), (0, -kern.size % 8))[:, None], (kern.size + -kern.size % 8, 128))

    f32, bf16 = jnp.float32, jnp.bfloat16
    plane = (rows, width_x)
    dma = pltpu.SemaphoreType.DMA
    anywhere = pl.BlockSpec(memory_space=pl.ANY)
    turned = pl.pallas_call(
        functools.partial(whole_kernel, taps),
        name="deconvolve",
        out_shape=jax.ShapeDtypeStruct((planes, width_y, width_x), f32),
        in_specs=[anywhere, anywhere, pl.BlockSpec(memory_space=pltpu.VMEM)],
        out_specs=anywhere,
        scratch_shapes=[
            pltpu.VMEM((planes, width_x, width_y), f32),
            pltpu.VMEM((planes, width_x, width_y), f32),
            pltpu.VMEM((2,) + kern.shape, f32),
            pltpu.VMEM((2, 2 * width_x, 2 * width_x), bf16),
            pltpu.VMEM((2, 2 * width_x, 2 * width_x), bf16),
            pltpu.VMEM((2, rows, 3 * rows), bf16),
            pltpu.VMEM((2, rows, 3 * rows), bf16),
            pltpu.VMEM((3 * planes,) + plane, f32),
            pltpu.VMEM((3 * planes,) + plane, f32),
            pltpu.VMEM((planes,) + plane, f32),
            pltpu.VMEM((2, outer) + plane, f32),
            pltpu.VMEM((planes,) + plane, f32),
            pltpu.VMEM((2, outer) + plane, f32),
            pltpu.VMEM((GROUP,) + plane, f32),
            pltpu.VMEM((2, planes) + plane, f32),
            pltpu.VMEM((2, planes) + plane, f32),
            pltpu.VMEM((planes, width_y, width_x), f32),
            pltpu.VMEM((4, GROUP) + plane, f32),
            dma((2, 4)),
            dma((4,)),
            dma((2,)),
            dma((4, 2)),
            dma((2, 4, 2)),
            dma((2, 2)),
            dma((2, 2, 4, 2)),
            dma((2, 2, 2, 2)),
            dma((2, 4, 2)),
            dma((2, 4, 2)),
            dma((2, 4, 2)),
            dma((2, 6)),
            dma((2, 4)),
        ],
        compiler_params=pltpu.CompilerParams(
            collective_id=0, has_side_effects=True, vmem_limit_bytes=60 * 2**20
        ),
    )(views_data[0], start, kern)
    return pl.pallas_call(
        turn_back,
        name="turn_back",
        grid=(planes // GROUP,),
        out_shape=jax.ShapeDtypeStruct(start.shape, f32),
        in_specs=[pl.BlockSpec((GROUP, width_y, width_x), lambda q: (q, 0, 0))],
        out_specs=pl.BlockSpec((GROUP, width_x, width_y), lambda q: (q, 0, 0)),
    )(turned)


def solution(mesh):
    return jax.shard_map(
        on_device,
        mesh=mesh,
        in_specs=(P("view", "gz", None, None), P("gz", None, None), P(), P("view")),
        out_specs=P("gz", None, None),
        check_vma=False,
    )
```

```python
import functools

import jax
import jax.numpy as jnp
from jax import lax
from jax.experimental import pallas as pl
from jax.experimental.pallas import tpu as pltpu
from jax.sharding import PartitionSpec as P

MESH = pl.DeviceIdType.MESH
GROUP = 4
CHUNK = 32


def halves(value):
    high = value.astype(jnp.bfloat16)
    return high, (value - high.astype(jnp.float32)).astype(jnp.bfloat16)


def fill_bands(kern, taps, first_tap, ahead, behind, period, low_block):
    rows, cols = ahead.shape
    step = 32
    radius = (taps - 1) // 2

    @pl.loop(0, rows // step)
    def _(block):
        top = pl.multiple_of(block * step, step)
        row = lax.broadcasted_iota(jnp.int32, (step, cols), 0) + top
        col = lax.broadcasted_iota(jnp.int32, (step, cols), 1)
        is_low = (col >= low_block * period) & (col < (low_block + 1) * period)
        for wrap in range(cols // period - 1):
            col = jnp.where(col >= period, col - period, col)
        for wrap in range(rows // period - 1):
            row = jnp.where(row >= period, row - period, row)
        shift = col - row
        first = jnp.zeros((step, cols), jnp.float32)
        second = first
        for tap in range(taps):
            value = jnp.broadcast_to(kern[pl.ds(first_tap + tap, 1), pl.ds(0, 1)], (step, cols))
            first = jnp.where(shift == tap - radius, value, first)
            second = jnp.where(shift == radius - tap, value, second)
        for target, matrix in ((ahead, first), (behind, second)):
            high = matrix.astype(jnp.bfloat16).astype(jnp.float32)
            target[pl.ds(top, step), :] = jnp.where(is_low, matrix - high, high).astype(jnp.bfloat16)


def convolve(taps, coef, read, matrix_x, matrix_y, mixed, finish):
    rows = mixed.shape[1]
    wide = mixed.shape[2]
    for r0 in range(0, rows, CHUNK):
        total = [None] * GROUP
        for i in range(taps + GROUP - 1):
            value = read(i, r0)
            for o in range(GROUP):
                if 0 <= i - o < taps:
                    term = coef[i - o] * value
                    total[o] = term if total[o] is None else total[o] + term
        for o in range(GROUP):
            mixed[o, pl.ds(r0, CHUNK), :] = total[o]
    for pair in range(GROUP // 2):
        both = []
        for o in (2 * pair, 2 * pair + 1):
            high, low = halves(mixed[o])
            out = jnp.dot(jnp.concatenate([high, low], axis=1), matrix_x, preferred_element_type=jnp.float32)
            both.append(halves(out[:, :wide] + out[:, wide:]))
        high = jnp.concatenate([both[0][0], both[1][0]], axis=1)
        low = jnp.concatenate([both[0][1], both[1][1]], axis=1)
        out = jnp.dot(matrix_y, jnp.concatenate([high, high, low], axis=0), preferred_element_type=jnp.float32)
        finish(2 * pair, out[:, :wide])
        finish(2 * pair + 1, out[:, wide:])


def whole_kernel(
    taps, views_in, start_in, kern_in, out,
    vin, sin, kern, xf, xb, yf, yb, est1, est2, spare, views, theirs, ratio, mixed, prod, prod_in, result, hop,
    load_sem, out_sem, kern_sem, z_sem, start_sem, extra_sem, pass_sem, view_sem, est_sem, prod_sem, last_sem,
    hop_sem, onward_sem,
):
    planes, full, wide = result.shape
    rows = views.shape[2]
    half = full // 2
    radius = (taps - 1) // 2
    valid = rows - radius
    known = rows - 2 * radius
    v = lax.axis_index("view")
    g = lax.axis_index("gz")
    last = lax.axis_size("gz") - 1
    upper, core = v // 2, v % 2
    lower = 1 - upper
    seam = (last + 1) // 2
    partner = {"view": (v + 2) % 4, "gz": g}
    sibling = {"view": v + 1 - 2 * core, "gz": g}
    beside = ({"view": v, "gz": g + 1}, {"view": v, "gz": g - 1})
    opposite = ({"view": (v + 2) % 4, "gz": g + 1}, {"view": (v + 2) % 4, "gz": g - 1})
    sends = (g < last, g > 0)
    receives = (g > 0, g < last)
    at_seam = (g == seam - 1, g == seam)

    loads = []
    for q in range(planes // GROUP):
        part = pl.ds(q * GROUP, GROUP)
        loads.append(
            (
                pltpu.make_async_copy(start_in.at[part], sin.at[part], load_sem.at[0, q]),
                pltpu.make_async_copy(views_in.at[part], vin.at[part], load_sem.at[1, q]),
            )
        )
    for q in (3, 0, 2, 1):
        loads[q][0].start()

    relays = ({"view": v, "gz": last}, {"view": v, "gz": 0})
    relays_across = ({"view": (v + 2) % 4, "gz": last}, {"view": (v + 2) % 4, "gz": 0})
    at_relay = (g == last, g == 0)
    sources = ({"view": v, "gz": seam - 1}, {"view": v, "gz": seam})
    sources_across = ({"view": (v + 2) % 4, "gz": seam - 1}, {"view": (v + 2) % 4, "gz": seam})

    barrier = pltpu.get_barrier_semaphore()

    def greet(there):
        pl.semaphore_signal(barrier, inc=1, device_id=there, device_id_type=MESH)

    greet(partner)
    greet(sibling)
    count = 2
    for side in range(2):

        @pl.when(sends[side])
        def _():
            greet(beside[side])

        @pl.when(at_seam[side])
        def _():
            greet(opposite[side])
            greet(relays[side])
            greet(relays_across[side])
            greet(relays[1 - side])

        @pl.when(at_relay[side])
        def _():
            greet(sources[side])
            greet(sources_across[side])
            greet(sources[1 - side])

        count = count + jnp.where(sends[side], 1, 0) + jnp.where(at_seam[side], 4, 0) + jnp.where(at_relay[side], 3, 0)

    def remote(src, dst, sem, there):
        return pltpu.make_async_remote_copy(
            src_ref=src, dst_ref=dst, send_sem=sem.at[0], recv_sem=sem.at[1], device_id=there, device_id_type=MESH
        )

    def est_place(side, k, who):
        return 14 - 2 * who - 4 * k if side == 0 else 2 * who + 4 * k

    def est_copy(est, sem, side, k):
        high = rows if est is est1 else known
        offset = 0 if est is est1 else pl.multiple_of(upper * 2 * radius, 8)
        place = est_place(side, k, core)
        src = est.at[pl.ds(planes + place, 2), pl.ds(offset, high), :]
        dst = est.at[pl.ds(2 * planes * side + place, 2), pl.ds(offset, high), :]
        return remote(src, dst, sem.at[side, k], beside[side])

    def extra_copy(side, k):
        place = est_place(side, k, core)
        return pltpu.make_async_remote_copy(
            src_ref=spare.at[pl.ds(place, 2)],
            dst_ref=est1.at[pl.ds(2 * planes * side + place, 2)],
            send_sem=extra_sem.at[side, k],
            recv_sem=start_sem.at[side, k, 1],
            device_id=opposite[side],
            device_id_type=MESH,
        )

    def pass_copy(est, sem, side, k, who):
        high = rows if est is est1 else known
        offset = 0 if est is est1 else pl.multiple_of(upper * 2 * radius, 8)
        place = est.at[pl.ds(2 * planes * side + est_place(side, k, who), 2), pl.ds(offset, high), :]
        return remote(place, place, sem.at[side, k], sibling)

    my_rows = pl.ds(pl.multiple_of(upper * radius, 8), valid)
    other_rows = pl.ds(pl.multiple_of(lower * radius, 8), valid)
    z_planes = [jnp.where(g == last, b, a) for a, b in zip((12, 0, 8, 4), (0, 12, 4, 8))]

    def z_copy(k):
        return remote(
            theirs.at[pl.ds(z_planes[k], GROUP), other_rows, :],
            views.at[1, pl.ds(radius + z_planes[k], GROUP), other_rows, :],
            z_sem.at[k],
            partner,
        )

    def z_arrival(k):
        here = views.at[1, pl.ds(radius + z_planes[k], GROUP), my_rows, :]
        return remote(here, here, z_sem.at[k], partner)

    def view_copy(which, side, k):
        src = (12 - 4 * k if side == 0 else 4 * k) + radius
        dst = 4 - 4 * k if side == 0 else planes + radius + 4 * k
        return remote(
            views.at[which, pl.ds(src, GROUP), my_rows, :],
            views.at[which, pl.ds(dst, GROUP), my_rows, :],
            view_sem.at[which, side, k],
            beside[side],
        )

    def direct_copy(side, k):
        src = 12 - 4 * k if side == 0 else 4 * k
        dst = 4 - 4 * k if side == 0 else planes + radius + 4 * k
        return remote(
            theirs.at[pl.ds(src, GROUP), other_rows, :],
            views.at[1, pl.ds(dst, GROUP), other_rows, :],
            view_sem.at[1, side, k],
            opposite[side],
        )

    def hop_copy(slot, src, high, send, there):
        return pltpu.make_async_remote_copy(
            src_ref=src,
            dst_ref=hop.at[slot, pl.ds(0, src.shape[0]), high, :],
            send_sem=hop_sem.at[0, send],
            recv_sem=hop_sem.at[1, slot],
            device_id=there,
            device_id_type=MESH,
        )

    def hop_start(side, k, across):
        place = est_place(side, k, core)
        src = spare.at[pl.ds(place, 2)] if across else est1.at[pl.ds(planes + place, 2)]
        there = relays_across[side] if across else relays[side]
        return hop_copy(k, src, pl.ds(0, rows), k + 2 * across, there)

    def hop_view(side, across):
        src = 8 if side == 0 else 4
        part = pl.ds(src, GROUP)
        if across:
            return hop_copy(1, theirs.at[part, other_rows, :], other_rows, 1, relays_across[side])
        return hop_copy(0, views.at[0, pl.ds(radius + src, GROUP), my_rows, :], my_rows, 0, relays[side])

    def onward(slot, side):
        target = sources[1 - side]
        if slot >= 2:
            src = hop.at[slot, pl.ds(0, 2)]
            dst = est1.at[pl.ds(2 * planes * side + est_place(side, slot, core), 2)]
            recv = start_sem.at[side, slot, 1]
        else:
            src = hop.at[slot, pl.ds(0, GROUP), my_rows, :]
            dst = views.at[slot, pl.ds(0 if side == 0 else planes + radius + 4, GROUP), my_rows, :]
            recv = view_sem.at[slot, side, 1, 1]
        return pltpu.make_async_remote_copy(
            src_ref=src,
            dst_ref=dst,
            send_sem=onward_sem.at[0, slot],
            recv_sem=recv,
            device_id=target,
            device_id_type=MESH,
        )

    def hop_arrival(slot):
        here = hop.at[slot, pl.ds(0, 2)] if slot >= 2 else hop.at[slot, pl.ds(0, GROUP), my_rows, :]
        return pltpu.make_async_remote_copy(
            src_ref=here,
            dst_ref=here,
            send_sem=onward_sem.at[1, slot],
            recv_sem=hop_sem.at[1, slot],
            device_id=partner,
            device_id_type=MESH,
        )

    def serve(slots):
        for side in range(2):

            @pl.when(at_relay[side])
            def _():
                for slot in slots:
                    hop_arrival(slot).wait_recv()
                    onward(slot, side).start()

    def prod_copy(i, q):
        part = pl.ds(q * GROUP, GROUP)
        return remote(prod.at[i, part], prod_in.at[i, part], prod_sem.at[i, q], sibling)

    def turn(source, p, own, other):
        @pl.when(upper == 0)
        def _():
            own[...] = source[p, :, pl.ds(0, 256)].T[:rows]
            other[...] = source[p, :, pl.ds(128, 256)].T[256 - rows :]

        @pl.when(upper == 1)
        def _():
            own[...] = source[p, :, pl.ds(128, 256)].T[256 - rows :]
            other[...] = source[p, :, pl.ds(0, 256)].T[:rows]

    plain = [jnp.logical_not(at_seam[side]) for side in range(2)]

    def turn_start(q):
        loads[q][0].wait()

        @pl.loop(q * GROUP, (q + 1) * GROUP)
        def _(p):
            turn(sin, p, est1.at[planes + p], spare.at[p])

    def send_start(k):
        for side in range(2):

            @pl.when(sends[side] & plain[side])
            def _():
                est_copy(est1, start_sem, side, k).start()

            @pl.when(at_seam[side] & (upper == core))
            def _():
                if k < 2:
                    est_copy(est1, start_sem, side, k).start()
                    extra_copy(side, k).start()
                else:
                    hop_start(side, k, 0).start()
                    hop_start(side, k, 1).start()

    with jax.named_scope("turn_start"):
        turn_start(3)
        turn_start(0)
        for q in (3, 0, 2, 1):
            loads[q][1].start()
    with jax.named_scope("barrier"):
        pl.semaphore_wait(barrier, count)
    with jax.named_scope("turn_rest"):
        send_start(0)
        kern_copy = remote(kern_in, kern.at[1], kern_sem, partner)
        kern_copy.start()
        turn_start(2)
        turn_start(1)
        for k in range(1, 4):
            send_start(k)
    with jax.named_scope("turn_views"):
        for k in range(4):
            q = z_planes[k] // GROUP
            part = pl.ds(q * GROUP, GROUP)
            pltpu.make_async_copy(views_in.at[part], vin.at[part], load_sem.at[1, q]).wait()

            @pl.loop(q * GROUP, (q + 1) * GROUP)
            def _(p):
                turn(vin, p, views.at[0, radius + p], theirs.at[p])

            @pl.when(jnp.logical_not(at_seam[0] | at_seam[1]))
            def _():
                z_copy(k).start()

        for side in range(2):

            @pl.when(at_seam[side])
            def _():
                hop_view(side, 0).start()
                hop_view(side, 1).start()
                for k in range(4):
                    z_copy(k).start()

        for k in range(2):
            for side in range(2):

                @pl.when(sends[side] & plain[side])
                def _():
                    view_copy(0, side, k).start()

    kern[0] = kern_in[...]
    ones = jnp.ones((8, wide), jnp.float32)
    view_pad = pl.multiple_of(lower * valid, 8)
    est_pad = pl.multiple_of(lower * known, 8)

    @pl.loop(0, views.shape[1])
    def _(f):
        for which in range(2):
            views[which, f, pl.ds(view_pad, 8), :] = ones
        est2[f + jnp.where(f >= planes, planes, 0), pl.ds(est_pad, 8), :] = ones
        est2[f + jnp.where(f >= planes, planes, 0), pl.ds(est_pad + 8, 8), :] = ones

    for side in range(2):

        @pl.when(jnp.logical_not(receives[side]))
        def _():
            zero = jnp.zeros((rows, wide), jnp.float32)

            @pl.loop(0, planes)
            def _(p):
                est1[2 * planes * side + p] = zero
                est2[2 * planes * side + p] = zero

            @pl.loop(0, radius)
            def _(p):
                for which in range(2):
                    views[which, (planes + radius) * side + p] = zero

    def bands(which):
        fill_bands(kern.at[which], taps, taps, xb.at[which], xf.at[which], wide, 1)
        fill_bands(kern.at[which], taps, 2 * taps, yf.at[which], yb.at[which], rows, 1)

    with jax.named_scope("bands"):
        bands(0)
        kern_copy.wait_recv()
        bands(1)

    def ahead_group(est, which, group, divide):
        base = group * GROUP
        coef = [kern[which, pl.ds(d, 1), :] for d in range(taps)]

        def finish(o, value):
            ratio[which, base + o] = views[which, base + o] / value if divide else value

        convolve(taps, coef, lambda i, r0: est[base + i, pl.ds(r0, CHUNK), :], xf[which], yf[which], mixed, finish)

    def back_group(i, which, group):
        base = group * GROUP
        coef = [kern[which, pl.ds(taps - 1 - d, 1), :] for d in range(taps)]

        def finish(o, value):
            prod[i, base + o] = value if which == 0 else prod[i, base + o] * value

        convolve(
            taps, coef, lambda j, r0: ratio[which, base + j, pl.ds(r0, CHUNK), :], xb[which], yb[which], mixed, finish
        )

    def hand_over(est, sem, side_sem, k):
        for side in range(2):

            @pl.when(receives[side])
            def _():
                est_copy(est, sem, side, k).wait_recv()
                pass_copy(est, side_sem, side, k, core).start()

    def arrive(est, side_sem, k):
        for side in range(2):

            @pl.when(receives[side])
            def _():
                pass_copy(est, side_sem, side, k, 1 - core).wait_recv()

    def ahead(est, k, divide, between):
        @pl.loop(0, 2)
        def _(which):
            @pl.loop(0, 2)
            def _(n):
                ahead_group(est, which, 3 - k + n * (2 * k + 1), divide)

            @pl.when(which == 0)
            def _():
                between()

    def ahead1(k, more):
        with jax.named_scope("arrive1"):
            arrive(est1, pass_sem.at[0], k)
        with jax.named_scope("ahead1"):

            def between():
                if more:
                    hand_over(est1, start_sem, pass_sem.at[0], k + 1)

                    @pl.when(k == 0)
                    def _():
                        serve((2, 3))

            ahead(est1, k, False, between)

    with jax.named_scope("arrive1"):
        hand_over(est1, start_sem, pass_sem.at[0], 0)

    @pl.loop(0, 3)
    def _(k):
        ahead1(k, True)

    ahead1(3, False)

    for side in range(2):

        @pl.when(at_seam[side])
        def _():
            view_copy(0, side, 0).start()
            direct_copy(side, 0).start()

    def forward(k):
        with jax.named_scope("wait_z"):
            z_arrival(k).wait_recv()
        side, piece = k % 2, k // 2

        @pl.when(sends[side] & plain[side] & (g < last))
        def _():
            view_copy(1, side, piece).start()

        if side == 0:

            @pl.when(g == last)
            def _():
                view_copy(1, 1, piece).start()

    with jax.named_scope("serve"):
        serve((0, 1))
    for k in range(3):
        forward(k)

    def divide(which, first, number):
        @pl.loop(first, first + number)
        def _(f):
            ratio[which, f] = views[which, f] / ratio[which, f]

    with jax.named_scope("wait_own"):
        for k in range(2):
            for side in range(2):

                @pl.when(receives[side])
                def _():
                    view_copy(0, side, k).wait_recv()

    with jax.named_scope("back1own"):
        divide(0, 0, planes + 2 * radius)

        @pl.loop(0, planes // GROUP)
        def _(group):
            back_group(0, 0, group)

    forward(3)

    def update(i, est, q, store):
        prod_copy(i, q).wait_recv()
        for o in range(GROUP):
            p = q * GROUP + o
            both = prod[i, p] * prod_in[i, p]
            store(p, est[planes + p] * jnp.sqrt(jnp.sqrt(both)))

    def keep(p, value):
        est2[planes + p] = value

    for k in range(2):
        with jax.named_scope("wait_other"):
            for side in range(2):

                @pl.when(receives[side])
                def _():
                    view_copy(1, side, k).wait_recv()

        with jax.named_scope("back1other"):
            if k == 0:
                divide(1, 4, planes + 2 * radius - 8)
            else:
                divide(1, 0, 4)
                divide(1, planes + 2 * radius - 4, 4)
            groups = (1, 2) if k == 0 else (0, 3)

            @pl.loop(0, 2)
            def _(n):
                q = n + 1 if k == 0 else 3 * n
                back_group(0, 1, q)
                prod_copy(0, q).start()

        with jax.named_scope("update1"):
            for q in groups:
                update(0, est1, q, keep)
        for piece in (1,) if k == 0 else (0, 2, 3):
            for side in range(2):

                @pl.when(sends[side])
                def _():
                    est_copy(est2, est_sem, side, piece).start()

    def ahead2(k, more):
        with jax.named_scope("arrive2"):
            arrive(est2, pass_sem.at[1], k)
        with jax.named_scope("ahead2"):

            def between():
                if more:
                    hand_over(est2, est_sem, pass_sem.at[1], k + 1)

            ahead(est2, k, True, between)

    with jax.named_scope("arrive2"):
        hand_over(est2, est_sem, pass_sem.at[1], 0)

    @pl.loop(0, 3)
    def _(k):
        ahead2(k, True)

    own_rows = pl.ds(pl.multiple_of(upper * half, 8), half)
    rest_rows = pl.ds(pl.multiple_of(lower * half, 8), half)
    inner = pl.multiple_of(upper * (rows - half), 8)

    def last_part(q, who, high):
        return result.at[pl.ds(q * GROUP + 2 * who, 2), high, :]

    def last_copy(q):
        part = last_part(q, core, own_rows)
        return remote(part, part, last_sem.at[0, q], partner)

    def last_arrival(q):
        part = last_part(q, core, rest_rows)
        return remote(part, part, last_sem.at[0, q], partner)

    def last_pass(q, who):
        part = last_part(q, who, rest_rows)
        return remote(part, part, last_sem.at[1, q], sibling)

    def out_copy(q):
        part = pl.ds(q * GROUP, GROUP)
        return pltpu.make_async_copy(result.at[part], out.at[part], out_sem.at[q])

    def finish_group(q):
        prod_copy(1, q).wait_recv()
        for o in range(GROUP):
            p = q * GROUP + o
            both = prod[1, p] * prod_in[1, p]
            prod_in[0, p] = est2[planes + p] * jnp.sqrt(jnp.sqrt(both))
            result[p, own_rows, :] = prod_in[0, p, pl.ds(inner, half), :]

        last_copy(q).start()

    def back2(first, step):
        @pl.loop(0, 2)
        def _(n):
            q = first + step * n
            with jax.named_scope("back2"):
                back_group(1, 0, q)
                back_group(1, 1, q)
                prod_copy(1, q).start()

            @pl.when(n > 0)
            def _():
                finish_group(first)

    back2(1, 1)
    ahead2(3, False)
    finish_group(2)
    back2(0, 3)
    finish_group(3)

    with jax.named_scope("wait_last"):
        for n, q in enumerate((1, 2, 0, 3)):
            last_arrival(q).wait_recv()
            last_pass(q, core).start()
            if n > 0:
                last_pass(before, 1 - core).wait_recv()
                out_copy(before).start()
            before = q
        last_pass(before, 1 - core).wait_recv()
        out_copy(before).start()

    kern_copy.wait_send()
    for k in range(4):
        z_copy(k).wait_send()
        prod_copy(0, k).wait_send()
        prod_copy(1, k).wait_send()
    for q in range(planes // GROUP):

        last_copy(q).wait_send()
        last_pass(q, core).wait_send()
        out_copy(q).wait()
    for side in range(2):
        for k in range(4):

            @pl.when(sends[side])
            def _():
                est_copy(est2, est_sem, side, k).wait_send()

            @pl.when(sends[side] & plain[side])
            def _():
                est_copy(est1, start_sem, side, k).wait_send()

            @pl.when(at_seam[side] & (upper == core))
            def _():
                if k < 2:
                    est_copy(est1, start_sem, side, k).wait_send()
                    extra_copy(side, k).wait_send()
                else:
                    hop_start(side, k, 0).wait_send()
                    hop_start(side, k, 1).wait_send()

            @pl.when(receives[side])
            def _():
                pass_copy(est1, pass_sem.at[0], side, k, core).wait_send()
                pass_copy(est2, pass_sem.at[1], side, k, core).wait_send()

        for k in range(2):

            @pl.when(sends[side] & plain[side])
            def _():
                view_copy(0, side, k).wait_send()
                view_copy(1, side, k).wait_send()

        @pl.when(at_seam[side])
        def _():
            view_copy(0, side, 0).wait_send()
            hop_view(side, 0).wait_send()
            direct_copy(side, 0).wait_send()
            hop_view(side, 1).wait_send()

        @pl.when(at_relay[side])
        def _():
            for slot in range(4):
                onward(slot, side).wait_send()


def turn_back(source, target):
    for p in range(source.shape[0]):
        target[p] = source[p].T


def on_device(views_data, start, psf_table, psf_index):
    planes, width_x, width_y = start.shape
    taps = psf_table.shape[2]
    radius = (taps - 1) // 2
    rows = width_y // 2 + 4 * radius
    outer = planes + 2 * radius

    picked = (jnp.arange(psf_table.shape[0]) == psf_index[0]).astype(jnp.float32)
    kern = jnp.sum(picked[:, None, None] * psf_table, axis=0)
    kern = kern / jnp.sum(kern, axis=-1, keepdims=True)
    kern = jnp.broadcast_to(jnp.pad(kern.reshape(-1), (0, -kern.size % 8))[:, None], (kern.size + -kern.size % 8, 128))

    f32, bf16 = jnp.float32, jnp.bfloat16
    plane = (rows, width_x)
    dma = pltpu.SemaphoreType.DMA
    anywhere = pl.BlockSpec(memory_space=pl.ANY)
    turned = pl.pallas_call(
        functools.partial(whole_kernel, taps),
        name="deconvolve",
        out_shape=jax.ShapeDtypeStruct((planes, width_y, width_x), f32),
        in_specs=[anywhere, anywhere, pl.BlockSpec(memory_space=pltpu.VMEM)],
        out_specs=anywhere,
        scratch_shapes=[
            pltpu.VMEM((planes, width_x, width_y), f32),
            pltpu.VMEM((planes, width_x, width_y), f32),
            pltpu.VMEM((2,) + kern.shape, f32),
            pltpu.VMEM((2, 2 * width_x, 2 * width_x), bf16),
            pltpu.VMEM((2, 2 * width_x, 2 * width_x), bf16),
            pltpu.VMEM((2, rows, 3 * rows), bf16),
            pltpu.VMEM((2, rows, 3 * rows), bf16),
            pltpu.VMEM((3 * planes,) + plane, f32),
            pltpu.VMEM((3 * planes,) + plane, f32),
            pltpu.VMEM((planes,) + plane, f32),
            pltpu.VMEM((2, outer) + plane, f32),
            pltpu.VMEM((planes,) + plane, f32),
            pltpu.VMEM((2, outer) + plane, f32),
            pltpu.VMEM((GROUP,) + plane, f32),
            pltpu.VMEM((2, planes) + plane, f32),
            pltpu.VMEM((2, planes) + plane, f32),
            pltpu.VMEM((planes, width_y, width_x), f32),
            pltpu.VMEM((4, GROUP) + plane, f32),
            dma((2, 4)),
            dma((4,)),
            dma((2,)),
            dma((4, 2)),
            dma((2, 4, 2)),
            dma((2, 2)),
            dma((2, 2, 4, 2)),
            dma((2, 2, 2, 2)),
            dma((2, 4, 2)),
            dma((2, 4, 2)),
            dma((2, 4, 2)),
            dma((2, 6)),
            dma((2, 4)),
        ],
        compiler_params=pltpu.CompilerParams(
            collective_id=0, has_side_effects=True, vmem_limit_bytes=60 * 2**20
        ),
    )(views_data[0], start, kern)
    return pl.pallas_call(
        turn_back,
        name="turn_back",
        grid=(planes // GROUP,),
        out_shape=jax.ShapeDtypeStruct(start.shape, f32),
        in_specs=[pl.BlockSpec((GROUP, width_y, width_x), lambda q: (q, 0, 0))],
        out_specs=pl.BlockSpec((GROUP, width_x, width_y), lambda q: (q, 0, 0)),
    )(turned)


def solution(mesh):
    return jax.shard_map(
        on_device,
        mesh=mesh,
        in_specs=(P("view", "gz", None, None), P("gz", None, None), P(), P("view")),
        out_specs=P("gz", None, None),
        check_vma=False,
    )
```

```python
import functools

import jax
import jax.numpy as jnp
from jax import lax
from jax.experimental import pallas as pl
from jax.experimental.pallas import tpu as pltpu
from jax.sharding import PartitionSpec as P

MESH = pl.DeviceIdType.MESH
GROUP = 4
CHUNK = 32


def halves(value):
    high = value.astype(jnp.bfloat16)
    return high, (value - high.astype(jnp.float32)).astype(jnp.bfloat16)


def fill_bands(kern, taps, first_tap, ahead, behind, period, low_block):
    rows, cols = ahead.shape
    step = 32
    radius = (taps - 1) // 2

    @pl.loop(0, rows // step)
    def _(block):
        top = pl.multiple_of(block * step, step)
        row = lax.broadcasted_iota(jnp.int32, (step, cols), 0) + top
        col = lax.broadcasted_iota(jnp.int32, (step, cols), 1)
        is_low = (col >= low_block * period) & (col < (low_block + 1) * period)
        for wrap in range(cols // period - 1):
            col = jnp.where(col >= period, col - period, col)
        for wrap in range(rows // period - 1):
            row = jnp.where(row >= period, row - period, row)
        shift = col - row
        first = jnp.zeros((step, cols), jnp.float32)
        second = first
        for tap in range(taps):
            value = jnp.broadcast_to(kern[pl.ds(first_tap + tap, 1), pl.ds(0, 1)], (step, cols))
            first = jnp.where(shift == tap - radius, value, first)
            second = jnp.where(shift == radius - tap, value, second)
        for target, matrix in ((ahead, first), (behind, second)):
            high = matrix.astype(jnp.bfloat16).astype(jnp.float32)
            target[pl.ds(top, step), :] = jnp.where(is_low, matrix - high, high).astype(jnp.bfloat16)


def convolve(taps, coef, read, matrix_x, matrix_y, mixed, finish):
    rows = mixed.shape[1]
    wide = mixed.shape[2]
    for r0 in range(0, rows, CHUNK):
        total = [None] * GROUP
        for i in range(taps + GROUP - 1):
            value = read(i, r0)
            for o in range(GROUP):
                if 0 <= i - o < taps:
                    term = coef[i - o] * value
                    total[o] = term if total[o] is None else total[o] + term
        for o in range(GROUP):
            mixed[o, pl.ds(r0, CHUNK), :] = total[o]
    for pair in range(GROUP // 2):
        both = []
        for o in (2 * pair, 2 * pair + 1):
            high, low = halves(mixed[o])
            out = jnp.dot(jnp.concatenate([high, low], axis=1), matrix_x, preferred_element_type=jnp.float32)
            both.append(halves(out[:, :wide] + out[:, wide:]))
        high = jnp.concatenate([both[0][0], both[1][0]], axis=1)
        low = jnp.concatenate([both[0][1], both[1][1]], axis=1)
        out = jnp.dot(matrix_y, jnp.concatenate([high, high, low], axis=0), preferred_element_type=jnp.float32)
        finish(2 * pair, out[:, :wide])
        finish(2 * pair + 1, out[:, wide:])


def whole_kernel(
    taps, views_in, start_in, kern_in, out,
    vin, sin, kern, xf, xb, yf, yb, est1, est2, spare, views, theirs, ratio, mixed, prod, prod_in, result, hop,
    load_sem, out_sem, kern_sem, z_sem, start_sem, extra_sem, pass_sem, view_sem, est_sem, prod_sem, last_sem,
    hop_sem, onward_sem,
):
    planes, full, wide = result.shape
    rows = views.shape[2]
    half = full // 2
    radius = (taps - 1) // 2
    valid = rows - radius
    known = rows - 2 * radius
    v = lax.axis_index("view")
    g = lax.axis_index("gz")
    last = lax.axis_size("gz") - 1
    upper, core = v // 2, v % 2
    lower = 1 - upper
    seam = (last + 1) // 2
    partner = {"view": (v + 2) % 4, "gz": g}
    sibling = {"view": v + 1 - 2 * core, "gz": g}
    beside = ({"view": v, "gz": g + 1}, {"view": v, "gz": g - 1})
    opposite = ({"view": (v + 2) % 4, "gz": g + 1}, {"view": (v + 2) % 4, "gz": g - 1})
    sends = (g < last, g > 0)
    receives = (g > 0, g < last)
    at_seam = (g == seam - 1, g == seam)

    loads = []
    for q in range(planes // GROUP):
        part = pl.ds(q * GROUP, GROUP)
        loads.append(
            (
                pltpu.make_async_copy(start_in.at[part], sin.at[part], load_sem.at[0, q]),
                pltpu.make_async_copy(views_in.at[part], vin.at[part], load_sem.at[1, q]),
            )
        )
    for q in (3, 0, 2, 1):
        loads[q][0].start()

    relays = ({"view": v, "gz": last}, {"view": v, "gz": 0})
    relays_across = ({"view": (v + 2) % 4, "gz": last}, {"view": (v + 2) % 4, "gz": 0})
    at_relay = (g == last, g == 0)
    sources = ({"view": v, "gz": seam - 1}, {"view": v, "gz": seam})
    sources_across = ({"view": (v + 2) % 4, "gz": seam - 1}, {"view": (v + 2) % 4, "gz": seam})

    barrier = pltpu.get_barrier_semaphore()

    def greet(there):
        pl.semaphore_signal(barrier, inc=1, device_id=there, device_id_type=MESH)

    greet(partner)
    greet(sibling)
    count = 2
    for side in range(2):

        @pl.when(sends[side])
        def _():
            greet(beside[side])

        @pl.when(at_seam[side])
        def _():
            greet(opposite[side])
            greet(relays[side])
            greet(relays_across[side])
            greet(relays[1 - side])

        @pl.when(at_relay[side])
        def _():
            greet(sources[side])
            greet(sources_across[side])
            greet(sources[1 - side])

        count = count + jnp.where(sends[side], 1, 0) + jnp.where(at_seam[side], 4, 0) + jnp.where(at_relay[side], 3, 0)

    def remote(src, dst, sem, there):
        return pltpu.make_async_remote_copy(
            src_ref=src, dst_ref=dst, send_sem=sem.at[0], recv_sem=sem.at[1], device_id=there, device_id_type=MESH
        )

    def est_place(side, k, who):
        return 14 - 2 * who - 4 * k if side == 0 else 2 * who + 4 * k

    def est_copy(est, sem, side, k):
        high = rows if est is est1 else known
        offset = 0 if est is est1 else pl.multiple_of(upper * 2 * radius, 8)
        place = est_place(side, k, core)
        src = est.at[pl.ds(planes + place, 2), pl.ds(offset, high), :]
        dst = est.at[pl.ds(2 * planes * side + place, 2), pl.ds(offset, high), :]
        return remote(src, dst, sem.at[side, k], beside[side])

    def extra_copy(side, k):
        place = est_place(side, k, core)
        return pltpu.make_async_remote_copy(
            src_ref=spare.at[pl.ds(place, 2)],
            dst_ref=est1.at[pl.ds(2 * planes * side + place, 2)],
            send_sem=extra_sem.at[side, k],
            recv_sem=start_sem.at[side, k, 1],
            device_id=opposite[side],
            device_id_type=MESH,
        )

    def pass_copy(est, sem, side, k, who):
        high = rows if est is est1 else known
        offset = 0 if est is est1 else pl.multiple_of(upper * 2 * radius, 8)
        place = est.at[pl.ds(2 * planes * side + est_place(side, k, who), 2), pl.ds(offset, high), :]
        return remote(place, place, sem.at[side, k], sibling)

    my_rows = pl.ds(pl.multiple_of(upper * radius, 8), valid)
    other_rows = pl.ds(pl.multiple_of(lower * radius, 8), valid)
    only_next = (g == 0) | (g == seam)
    only_previous = (g == last) | (g == seam - 1)
    orders = ((12, 0, 8, 4), (12, 8, 0, 4), (0, 4, 12, 8))
    kinds = (jnp.logical_not(only_next | only_previous), only_next, only_previous)
    z_planes = [
        jnp.where(only_next, orders[1][k], jnp.where(only_previous, orders[2][k], orders[0][k])) for k in range(4)
    ]

    def z_copy(k):
        return remote(
            theirs.at[pl.ds(z_planes[k], GROUP), other_rows, :],
            views.at[1, pl.ds(radius + z_planes[k], GROUP), other_rows, :],
            z_sem.at[k],
            partner,
        )

    def z_arrival(k):
        here = views.at[1, pl.ds(radius + z_planes[k], GROUP), my_rows, :]
        return remote(here, here, z_sem.at[k], partner)

    def view_copy(which, side, k):
        src = (12 - 4 * k if side == 0 else 4 * k) + radius
        dst = 4 - 4 * k if side == 0 else planes + radius + 4 * k
        return remote(
            views.at[which, pl.ds(src, GROUP), my_rows, :],
            views.at[which, pl.ds(dst, GROUP), my_rows, :],
            view_sem.at[which, side, k],
            beside[side],
        )

    def direct_copy(side, k):
        src = 12 - 4 * k if side == 0 else 4 * k
        dst = 4 - 4 * k if side == 0 else planes + radius + 4 * k
        return remote(
            theirs.at[pl.ds(src, GROUP), other_rows, :],
            views.at[1, pl.ds(dst, GROUP), other_rows, :],
            view_sem.at[1, side, k],
            opposite[side],
        )

    def hop_copy(slot, src, high, send, there):
        return pltpu.make_async_remote_copy(
            src_ref=src,
            dst_ref=hop.at[slot, pl.ds(0, src.shape[0]), high, :],
            send_sem=hop_sem.at[0, send],
            recv_sem=hop_sem.at[1, slot],
            device_id=there,
            device_id_type=MESH,
        )

    def hop_start(side, k, across):
        place = est_place(side, k, core)
        src = spare.at[pl.ds(place, 2)] if across else est1.at[pl.ds(planes + place, 2)]
        there = relays_across[side] if across else relays[side]
        return hop_copy(k, src, pl.ds(0, rows), k + 2 * across, there)

    def hop_view(side, across):
        src = 8 if side == 0 else 4
        part = pl.ds(src, GROUP)
        if across:
            return hop_copy(1, theirs.at[part, other_rows, :], other_rows, 1, relays_across[side])
        return hop_copy(0, views.at[0, pl.ds(radius + src, GROUP), my_rows, :], my_rows, 0, relays[side])

    def onward(slot, side):
        target = sources[1 - side]
        if slot >= 2:
            src = hop.at[slot, pl.ds(0, 2)]
            dst = est1.at[pl.ds(2 * planes * side + est_place(side, slot, core), 2)]
            recv = start_sem.at[side, slot, 1]
        else:
            src = hop.at[slot, pl.ds(0, GROUP), my_rows, :]
            dst = views.at[slot, pl.ds(0 if side == 0 else planes + radius + 4, GROUP), my_rows, :]
            recv = view_sem.at[slot, side, 1, 1]
        return pltpu.make_async_remote_copy(
            src_ref=src,
            dst_ref=dst,
            send_sem=onward_sem.at[0, slot],
            recv_sem=recv,
            device_id=target,
            device_id_type=MESH,
        )

    def hop_arrival(slot):
        here = hop.at[slot, pl.ds(0, 2)] if slot >= 2 else hop.at[slot, pl.ds(0, GROUP), my_rows, :]
        return pltpu.make_async_remote_copy(
            src_ref=here,
            dst_ref=here,
            send_sem=onward_sem.at[1, slot],
            recv_sem=hop_sem.at[1, slot],
            device_id=partner,
            device_id_type=MESH,
        )

    def serve(slots):
        for side in range(2):

            @pl.when(at_relay[side])
            def _():
                for slot in slots:
                    hop_arrival(slot).wait_recv()
                    onward(slot, side).start()

    def prod_copy(i, q):
        part = pl.ds(q * GROUP, GROUP)
        return remote(prod.at[i, part], prod_in.at[i, part], prod_sem.at[i, q], sibling)

    def turn(source, p, own, other):
        @pl.when(upper == 0)
        def _():
            own[...] = source[p, :, pl.ds(0, 256)].T[:rows]
            other[...] = source[p, :, pl.ds(128, 256)].T[256 - rows :]

        @pl.when(upper == 1)
        def _():
            own[...] = source[p, :, pl.ds(128, 256)].T[256 - rows :]
            other[...] = source[p, :, pl.ds(0, 256)].T[:rows]

    plain = [jnp.logical_not(at_seam[side]) for side in range(2)]

    def turn_start(q):
        loads[q][0].wait()

        @pl.loop(q * GROUP, (q + 1) * GROUP)
        def _(p):
            turn(sin, p, est1.at[planes + p], spare.at[p])

    def send_start(k):
        for side in range(2):

            @pl.when(sends[side] & plain[side])
            def _():
                est_copy(est1, start_sem, side, k).start()

            @pl.when(at_seam[side] & (upper == core))
            def _():
                if k < 2:
                    est_copy(est1, start_sem, side, k).start()
                    extra_copy(side, k).start()
                else:
                    hop_start(side, k, 0).start()
                    hop_start(side, k, 1).start()

    with jax.named_scope("turn_start"):
        turn_start(3)
        turn_start(0)
        for q in (3, 0, 2, 1):
            loads[q][1].start()
    with jax.named_scope("barrier"):
        pl.semaphore_wait(barrier, count)
    with jax.named_scope("turn_rest"):
        send_start(0)
        kern_copy = remote(kern_in, kern.at[1], kern_sem, partner)
        kern_copy.start()
        turn_start(2)
        turn_start(1)
        for k in range(1, 4):
            send_start(k)
    with jax.named_scope("turn_views"):
        for k in range(4):
            q = z_planes[k] // GROUP
            part = pl.ds(q * GROUP, GROUP)
            pltpu.make_async_copy(views_in.at[part], vin.at[part], load_sem.at[1, q]).wait()

            @pl.loop(q * GROUP, (q + 1) * GROUP)
            def _(p):
                turn(vin, p, views.at[0, radius + p], theirs.at[p])

            @pl.when(jnp.logical_not(at_seam[0] | at_seam[1]) | (k < 2))
            def _():
                z_copy(k).start()

        for k in range(2):
            for side in range(2):

                @pl.when(sends[side] & plain[side])
                def _():
                    view_copy(0, side, k).start()

    kern[0] = kern_in[...]
    ones = jnp.ones((8, wide), jnp.float32)
    view_pad = pl.multiple_of(lower * valid, 8)
    est_pad = pl.multiple_of(lower * known, 8)

    @pl.loop(0, views.shape[1])
    def _(f):
        for which in range(2):
            views[which, f, pl.ds(view_pad, 8), :] = ones
        est2[f + jnp.where(f >= planes, planes, 0), pl.ds(est_pad, 8), :] = ones
        est2[f + jnp.where(f >= planes, planes, 0), pl.ds(est_pad + 8, 8), :] = ones

    for side in range(2):

        @pl.when(jnp.logical_not(receives[side]))
        def _():
            zero = jnp.zeros((rows, wide), jnp.float32)

            @pl.loop(0, planes)
            def _(p):
                est1[2 * planes * side + p] = zero
                est2[2 * planes * side + p] = zero

            @pl.loop(0, radius)
            def _(p):
                for which in range(2):
                    views[which, (planes + radius) * side + p] = zero

    def bands(which):
        fill_bands(kern.at[which], taps, taps, xb.at[which], xf.at[which], wide, 1)
        fill_bands(kern.at[which], taps, 2 * taps, yf.at[which], yb.at[which], rows, 1)

    with jax.named_scope("bands"):
        bands(0)
        kern_copy.wait_recv()
        bands(1)

    def ahead_group(est, which, group, divide):
        base = group * GROUP
        coef = [kern[which, pl.ds(d, 1), :] for d in range(taps)]

        def finish(o, value):
            ratio[which, base + o] = views[which, base + o] / value if divide else value

        convolve(taps, coef, lambda i, r0: est[base + i, pl.ds(r0, CHUNK), :], xf[which], yf[which], mixed, finish)

    def back_group(i, which, group):
        base = group * GROUP
        coef = [kern[which, pl.ds(taps - 1 - d, 1), :] for d in range(taps)]

        def finish(o, value):
            prod[i, base + o] = value if which == 0 else prod[i, base + o] * value

        convolve(
            taps, coef, lambda j, r0: ratio[which, base + j, pl.ds(r0, CHUNK), :], xb[which], yb[which], mixed, finish
        )

    def hand_over(est, sem, side_sem, k):
        for side in range(2):

            @pl.when(receives[side])
            def _():
                est_copy(est, sem, side, k).wait_recv()
                pass_copy(est, side_sem, side, k, core).start()

    def arrive(est, side_sem, k):
        for side in range(2):

            @pl.when(receives[side])
            def _():
                pass_copy(est, side_sem, side, k, 1 - core).wait_recv()

    def ahead(est, k, divide, between):
        @pl.loop(0, 2)
        def _(which):
            @pl.loop(0, 2)
            def _(n):
                ahead_group(est, which, 3 - k + n * (2 * k + 1), divide)

            @pl.when(which == 0)
            def _():
                between()

    def ahead1(k, more):
        with jax.named_scope("arrive1"):
            arrive(est1, pass_sem.at[0], k)
        with jax.named_scope("ahead1"):

            def between():
                if more:
                    hand_over(est1, start_sem, pass_sem.at[0], k + 1)

                    @pl.when(k == 0)
                    def _():
                        serve((2, 3))

                    for side in range(2):

                        @pl.when(at_seam[side] & (k == 1))
                        def _():
                            hop_view(side, 0).start()
                            hop_view(side, 1).start()
                            z_copy(2).start()
                            z_copy(3).start()

            ahead(est1, k, False, between)

    with jax.named_scope("arrive1"):
        hand_over(est1, start_sem, pass_sem.at[0], 0)

    @pl.loop(0, 3)
    def _(k):
        ahead1(k, True)

    ahead1(3, False)

    for side in range(2):

        @pl.when(at_seam[side])
        def _():
            view_copy(0, side, 0).start()
            direct_copy(side, 0).start()

    def forward(k):
        with jax.named_scope("wait_z"):
            z_arrival(k).wait_recv()
        for kind, order in zip(kinds, orders):
            side = 0 if order[k] >= 8 else 1
            piece = 0 if order[k] in (0, 12) else 1

            @pl.when(kind & sends[side] & plain[side])
            def _():
                view_copy(1, side, piece).start()

    forward(0)
    forward(1)
    with jax.named_scope("serve"):
        serve((0, 1))
    ordinary = jnp.logical_not(only_next | only_previous)
    pl.when(ordinary)(functools.partial(forward, 2))

    def divide(which, first, number):
        @pl.loop(first, first + number)
        def _(f):
            ratio[which, f] = views[which, f] / ratio[which, f]

    with jax.named_scope("wait_own"):
        for k in range(2):
            for side in range(2):

                @pl.when(receives[side])
                def _():
                    view_copy(0, side, k).wait_recv()

    with jax.named_scope("back1own"):
        divide(0, 0, planes + 2 * radius)

        @pl.loop(0, planes // GROUP)
        def _(group):
            back_group(0, 0, group)

    pl.when(jnp.logical_not(ordinary))(functools.partial(forward, 2))
    forward(3)

    def update(i, est, q, store):
        prod_copy(i, q).wait_recv()
        for o in range(GROUP):
            p = q * GROUP + o
            both = prod[i, p] * prod_in[i, p]
            store(p, est[planes + p] * jnp.sqrt(jnp.sqrt(both)))

    def keep(p, value):
        est2[planes + p] = value

    for k in range(2):
        with jax.named_scope("wait_other"):
            for side in range(2):

                @pl.when(receives[side])
                def _():
                    view_copy(1, side, k).wait_recv()

        with jax.named_scope("back1other"):
            if k == 0:
                divide(1, 4, planes + 2 * radius - 8)
            else:
                divide(1, 0, 4)
                divide(1, planes + 2 * radius - 4, 4)
            groups = (1, 2) if k == 0 else (0, 3)

            @pl.loop(0, 2)
            def _(n):
                q = n + 1 if k == 0 else 3 * n
                back_group(0, 1, q)
                prod_copy(0, q).start()

        with jax.named_scope("update1"):
            for q in groups:
                update(0, est1, q, keep)
        for piece in (1,) if k == 0 else (0, 2, 3):
            for side in range(2):

                @pl.when(sends[side])
                def _():
                    est_copy(est2, est_sem, side, piece).start()

    def ahead2(k, more):
        with jax.named_scope("arrive2"):
            arrive(est2, pass_sem.at[1], k)
        with jax.named_scope("ahead2"):

            def between():
                if more:
                    hand_over(est2, est_sem, pass_sem.at[1], k + 1)

            ahead(est2, k, True, between)

    with jax.named_scope("arrive2"):
        hand_over(est2, est_sem, pass_sem.at[1], 0)

    @pl.loop(0, 3)
    def _(k):
        ahead2(k, True)

    own_rows = pl.ds(pl.multiple_of(upper * half, 8), half)
    rest_rows = pl.ds(pl.multiple_of(lower * half, 8), half)
    inner = pl.multiple_of(upper * (rows - half), 8)

    def last_part(q, who, high):
        return result.at[pl.ds(q * GROUP + 2 * who, 2), high, :]

    def last_copy(q):
        part = last_part(q, core, own_rows)
        return remote(part, part, last_sem.at[0, q], partner)

    def last_arrival(q):
        part = last_part(q, core, rest_rows)
        return remote(part, part, last_sem.at[0, q], partner)

    def last_pass(q, who):
        part = last_part(q, who, rest_rows)
        return remote(part, part, last_sem.at[1, q], sibling)

    def out_copy(q):
        part = pl.ds(q * GROUP, GROUP)
        return pltpu.make_async_copy(result.at[part], out.at[part], out_sem.at[q])

    def finish_group(q):
        prod_copy(1, q).wait_recv()
        for o in range(GROUP):
            p = q * GROUP + o
            both = prod[1, p] * prod_in[1, p]
            prod_in[0, p] = est2[planes + p] * jnp.sqrt(jnp.sqrt(both))
            result[p, own_rows, :] = prod_in[0, p, pl.ds(inner, half), :]

        last_copy(q).start()

    def back2(first, step):
        @pl.loop(0, 2)
        def _(n):
            q = first + step * n
            with jax.named_scope("back2"):
                back_group(1, 0, q)
                back_group(1, 1, q)
                prod_copy(1, q).start()

            @pl.when(n > 0)
            def _():
                finish_group(first)

    back2(1, 1)
    ahead2(3, False)
    finish_group(2)
    back2(0, 3)
    finish_group(3)

    with jax.named_scope("wait_last"):
        for n, q in enumerate((1, 2, 0, 3)):
            last_arrival(q).wait_recv()
            last_pass(q, core).start()
            if n > 0:
                last_pass(before, 1 - core).wait_recv()
                out_copy(before).start()
            before = q
        last_pass(before, 1 - core).wait_recv()
        out_copy(before).start()

    kern_copy.wait_send()
    for k in range(4):
        z_copy(k).wait_send()
        prod_copy(0, k).wait_send()
        prod_copy(1, k).wait_send()
    for q in range(planes // GROUP):

        last_copy(q).wait_send()
        last_pass(q, core).wait_send()
        out_copy(q).wait()
    for side in range(2):
        for k in range(4):

            @pl.when(sends[side])
            def _():
                est_copy(est2, est_sem, side, k).wait_send()

            @pl.when(sends[side] & plain[side])
            def _():
                est_copy(est1, start_sem, side, k).wait_send()

            @pl.when(at_seam[side] & (upper == core))
            def _():
                if k < 2:
                    est_copy(est1, start_sem, side, k).wait_send()
                    extra_copy(side, k).wait_send()
                else:
                    hop_start(side, k, 0).wait_send()
                    hop_start(side, k, 1).wait_send()

            @pl.when(receives[side])
            def _():
                pass_copy(est1, pass_sem.at[0], side, k, core).wait_send()
                pass_copy(est2, pass_sem.at[1], side, k, core).wait_send()

        for k in range(2):

            @pl.when(sends[side] & plain[side])
            def _():
                view_copy(0, side, k).wait_send()
                view_copy(1, side, k).wait_send()

        @pl.when(at_seam[side])
        def _():
            view_copy(0, side, 0).wait_send()
            hop_view(side, 0).wait_send()
            direct_copy(side, 0).wait_send()
            hop_view(side, 1).wait_send()

        @pl.when(at_relay[side])
        def _():
            for slot in range(4):
                onward(slot, side).wait_send()


def turn_back(source, target):
    for p in range(source.shape[0]):
        target[p] = source[p].T


def on_device(views_data, start, psf_table, psf_index):
    planes, width_x, width_y = start.shape
    taps = psf_table.shape[2]
    radius = (taps - 1) // 2
    rows = width_y // 2 + 4 * radius
    outer = planes + 2 * radius

    picked = (jnp.arange(psf_table.shape[0]) == psf_index[0]).astype(jnp.float32)
    kern = jnp.sum(picked[:, None, None] * psf_table, axis=0)
    kern = kern / jnp.sum(kern, axis=-1, keepdims=True)
    kern = jnp.broadcast_to(jnp.pad(kern.reshape(-1), (0, -kern.size % 8))[:, None], (kern.size + -kern.size % 8, 128))

    f32, bf16 = jnp.float32, jnp.bfloat16
    plane = (rows, width_x)
    dma = pltpu.SemaphoreType.DMA
    anywhere = pl.BlockSpec(memory_space=pl.ANY)
    turned = pl.pallas_call(
        functools.partial(whole_kernel, taps),
        name="deconvolve",
        out_shape=jax.ShapeDtypeStruct((planes, width_y, width_x), f32),
        in_specs=[anywhere, anywhere, pl.BlockSpec(memory_space=pltpu.VMEM)],
        out_specs=anywhere,
        scratch_shapes=[
            pltpu.VMEM((planes, width_x, width_y), f32),
            pltpu.VMEM((planes, width_x, width_y), f32),
            pltpu.VMEM((2,) + kern.shape, f32),
            pltpu.VMEM((2, 2 * width_x, 2 * width_x), bf16),
            pltpu.VMEM((2, 2 * width_x, 2 * width_x), bf16),
            pltpu.VMEM((2, rows, 3 * rows), bf16),
            pltpu.VMEM((2, rows, 3 * rows), bf16),
            pltpu.VMEM((3 * planes,) + plane, f32),
            pltpu.VMEM((3 * planes,) + plane, f32),
            pltpu.VMEM((planes,) + plane, f32),
            pltpu.VMEM((2, outer) + plane, f32),
            pltpu.VMEM((planes,) + plane, f32),
            pltpu.VMEM((2, outer) + plane, f32),
            pltpu.VMEM((GROUP,) + plane, f32),
            pltpu.VMEM((2, planes) + plane, f32),
            pltpu.VMEM((2, planes) + plane, f32),
            pltpu.VMEM((planes, width_y, width_x), f32),
            pltpu.VMEM((4, GROUP) + plane, f32),
            dma((2, 4)),
            dma((4,)),
            dma((2,)),
            dma((4, 2)),
            dma((2, 4, 2)),
            dma((2, 2)),
            dma((2, 2, 4, 2)),
            dma((2, 2, 2, 2)),
            dma((2, 4, 2)),
            dma((2, 4, 2)),
            dma((2, 4, 2)),
            dma((2, 6)),
            dma((2, 4)),
        ],
        compiler_params=pltpu.CompilerParams(
            collective_id=0, has_side_effects=True, vmem_limit_bytes=60 * 2**20
        ),
    )(views_data[0], start, kern)
    return pl.pallas_call(
        turn_back,
        name="turn_back",
        grid=(planes // GROUP,),
        out_shape=jax.ShapeDtypeStruct(start.shape, f32),
        in_specs=[pl.BlockSpec((GROUP, width_y, width_x), lambda q: (q, 0, 0))],
        out_specs=pl.BlockSpec((GROUP, width_x, width_y), lambda q: (q, 0, 0)),
    )(turned)


def solution(mesh):
    return jax.shard_map(
        on_device,
        mesh=mesh,
        in_specs=(P("view", "gz", None, None), P("gz", None, None), P(), P("view")),
        out_specs=P("gz", None, None),
        check_vma=False,
    )
```

```python
import functools

import jax
import jax.numpy as jnp
from jax import lax
from jax.experimental import pallas as pl
from jax.experimental.pallas import tpu as pltpu
from jax.sharding import PartitionSpec as P

MESH = pl.DeviceIdType.MESH
GROUP = 4
CHUNK = 32


def halves(value):
    high = value.astype(jnp.bfloat16)
    return high, (value - high.astype(jnp.float32)).astype(jnp.bfloat16)


def fill_bands(kern, taps, first_tap, ahead, behind, period, low_block):
    rows, cols = ahead.shape
    step = 32
    radius = (taps - 1) // 2

    @pl.loop(0, rows // step)
    def _(block):
        top = pl.multiple_of(block * step, step)
        row = lax.broadcasted_iota(jnp.int32, (step, cols), 0) + top
        col = lax.broadcasted_iota(jnp.int32, (step, cols), 1)
        is_low = (col >= low_block * period) & (col < (low_block + 1) * period)
        for wrap in range(cols // period - 1):
            col = jnp.where(col >= period, col - period, col)
        for wrap in range(rows // period - 1):
            row = jnp.where(row >= period, row - period, row)
        shift = col - row
        first = jnp.zeros((step, cols), jnp.float32)
        second = first
        for tap in range(taps):
            value = jnp.broadcast_to(kern[pl.ds(first_tap + tap, 1), pl.ds(0, 1)], (step, cols))
            first = jnp.where(shift == tap - radius, value, first)
            second = jnp.where(shift == radius - tap, value, second)
        for target, matrix in ((ahead, first), (behind, second)):
            high = matrix.astype(jnp.bfloat16).astype(jnp.float32)
            target[pl.ds(top, step), :] = jnp.where(is_low, matrix - high, high).astype(jnp.bfloat16)


def convolve(taps, coef, read, matrix_x, matrix_y, mixed, finish):
    rows = mixed.shape[1]
    wide = mixed.shape[2]
    for r0 in range(0, rows, CHUNK):
        total = [None] * GROUP
        for i in range(taps + GROUP - 1):
            value = read(i, r0)
            for o in range(GROUP):
                if 0 <= i - o < taps:
                    term = coef[i - o] * value
                    total[o] = term if total[o] is None else total[o] + term
        for o in range(GROUP):
            mixed[o, pl.ds(r0, CHUNK), :] = total[o]
    for pair in range(GROUP // 2):
        both = []
        for o in (2 * pair, 2 * pair + 1):
            high, low = halves(mixed[o])
            out = jnp.dot(jnp.concatenate([high, low], axis=1), matrix_x, preferred_element_type=jnp.float32)
            both.append(halves(out[:, :wide] + out[:, wide:]))
        high = jnp.concatenate([both[0][0], both[1][0]], axis=1)
        low = jnp.concatenate([both[0][1], both[1][1]], axis=1)
        out = jnp.dot(matrix_y, jnp.concatenate([high, high, low], axis=0), preferred_element_type=jnp.float32)
        finish(2 * pair, out[:, :wide])
        finish(2 * pair + 1, out[:, wide:])


def whole_kernel(
    taps, views_in, start_in, kern_in, out,
    vin, sin, kern, xf, xb, yf, yb, est1, est2, spare, views, theirs, ratio, mixed, prod, prod_in, result, hop, detour,
    load_sem, out_sem, kern_sem, z_sem, start_sem, extra_sem, pass_sem, view_sem, est_sem, prod_sem, last_sem,
    hop_sem, onward_sem, detour_sem,
):
    planes, full, wide = result.shape
    rows = views.shape[2]
    half = full // 2
    radius = (taps - 1) // 2
    valid = rows - radius
    known = rows - 2 * radius
    v = lax.axis_index("view")
    g = lax.axis_index("gz")
    last = lax.axis_size("gz") - 1
    upper, core = v // 2, v % 2
    lower = 1 - upper
    seam = (last + 1) // 2
    partner = {"view": (v + 2) % 4, "gz": g}
    sibling = {"view": v + 1 - 2 * core, "gz": g}
    beside = ({"view": v, "gz": g + 1}, {"view": v, "gz": g - 1})
    opposite = ({"view": (v + 2) % 4, "gz": g + 1}, {"view": (v + 2) % 4, "gz": g - 1})
    sends = (g < last, g > 0)
    receives = (g > 0, g < last)
    at_seam = (g == seam - 1, g == seam)

    loads = []
    for q in range(planes // GROUP):
        part = pl.ds(q * GROUP, GROUP)
        loads.append(
            (
                pltpu.make_async_copy(start_in.at[part], sin.at[part], load_sem.at[0, q]),
                pltpu.make_async_copy(views_in.at[part], vin.at[part], load_sem.at[1, q]),
            )
        )
    for q in (3, 0, 2, 1):
        loads[q][0].start()

    relays = ({"view": v, "gz": last}, {"view": v, "gz": 0})
    relays_across = ({"view": (v + 2) % 4, "gz": last}, {"view": (v + 2) % 4, "gz": 0})
    at_relay = (g == last, g == 0)
    sources = ({"view": v, "gz": seam - 1}, {"view": v, "gz": seam})
    sources_across = ({"view": (v + 2) % 4, "gz": seam - 1}, {"view": (v + 2) % 4, "gz": seam})

    only_next = (g == 0) | (g == seam)
    only_previous = (g == last) | (g == seam - 1)
    ordinary = jnp.logical_not(only_next | only_previous)
    orders = ((12, 0, 8, 4), (12, 8, 0, 4), (0, 4, 12, 8))
    kinds = (ordinary, only_next, only_previous)
    away = 3 * seam // 4
    helper = jnp.where(only_next, g + away, g - away)
    helps_next = (g == away) | (g == seam + away)
    helps_previous = (g == seam - 1 - away) | (g == last - away)
    helped = jnp.where(helps_next, g - away, g + away)
    helpers = ({"view": v, "gz": helper}, {"view": (v + 2) % 4, "gz": helper})
    helped_ends = ({"view": v, "gz": helped}, {"view": (v + 2) % 4, "gz": helped})

    barrier = pltpu.get_barrier_semaphore()

    def greet(there):
        pl.semaphore_signal(barrier, inc=1, device_id=there, device_id_type=MESH)

    greet(partner)
    greet(sibling)

    @pl.when(jnp.logical_not(ordinary))
    def _():
        greet(helpers[0])
        greet(helpers[1])

    @pl.when(helps_next | helps_previous)
    def _():
        greet(helped_ends[0])
        greet(helped_ends[1])

    count = 2 + jnp.where(ordinary, 0, 2) + jnp.where(helps_next | helps_previous, 2, 0)
    for side in range(2):

        @pl.when(sends[side])
        def _():
            greet(beside[side])

        @pl.when(at_seam[side])
        def _():
            greet(opposite[side])
            greet(relays[side])
            greet(relays_across[side])
            greet(relays[1 - side])

        @pl.when(at_relay[side])
        def _():
            greet(sources[side])
            greet(sources_across[side])
            greet(sources[1 - side])

        count = count + jnp.where(sends[side], 1, 0) + jnp.where(at_seam[side], 4, 0) + jnp.where(at_relay[side], 3, 0)

    def remote(src, dst, sem, there):
        return pltpu.make_async_remote_copy(
            src_ref=src, dst_ref=dst, send_sem=sem.at[0], recv_sem=sem.at[1], device_id=there, device_id_type=MESH
        )

    def est_place(side, k, who):
        return 14 - 2 * who - 4 * k if side == 0 else 2 * who + 4 * k

    def est_copy(est, sem, side, k):
        high = rows if est is est1 else known
        offset = 0 if est is est1 else pl.multiple_of(upper * 2 * radius, 8)
        place = est_place(side, k, core)
        src = est.at[pl.ds(planes + place, 2), pl.ds(offset, high), :]
        dst = est.at[pl.ds(2 * planes * side + place, 2), pl.ds(offset, high), :]
        return remote(src, dst, sem.at[side, k], beside[side])

    def extra_copy(side, k):
        place = est_place(side, k, core)
        return pltpu.make_async_remote_copy(
            src_ref=spare.at[pl.ds(place, 2)],
            dst_ref=est1.at[pl.ds(2 * planes * side + place, 2)],
            send_sem=extra_sem.at[side, k],
            recv_sem=start_sem.at[side, k, 1],
            device_id=opposite[side],
            device_id_type=MESH,
        )

    def pass_copy(est, sem, side, k, who):
        high = rows if est is est1 else known
        offset = 0 if est is est1 else pl.multiple_of(upper * 2 * radius, 8)
        place = est.at[pl.ds(2 * planes * side + est_place(side, k, who), 2), pl.ds(offset, high), :]
        return remote(place, place, sem.at[side, k], sibling)

    my_rows = pl.ds(pl.multiple_of(upper * radius, 8), valid)
    other_rows = pl.ds(pl.multiple_of(lower * radius, 8), valid)
    z_planes = [
        jnp.where(only_next, orders[1][k], jnp.where(only_previous, orders[2][k], orders[0][k])) for k in range(4)
    ]

    def z_copy(k):
        return remote(
            theirs.at[pl.ds(z_planes[k], GROUP), other_rows, :],
            views.at[1, pl.ds(radius + z_planes[k], GROUP), other_rows, :],
            z_sem.at[k],
            partner,
        )

    def detour_copy():
        return pltpu.make_async_remote_copy(
            src_ref=theirs.at[pl.ds(z_planes[3], GROUP), other_rows, :],
            dst_ref=detour.at[:, other_rows, :],
            send_sem=detour_sem.at[0],
            recv_sem=detour_sem.at[1],
            device_id=helpers[1],
            device_id_type=MESH,
        )

    def detour_arrival():
        here = detour.at[:, my_rows, :]
        return pltpu.make_async_remote_copy(
            src_ref=here,
            dst_ref=here,
            send_sem=detour_sem.at[0],
            recv_sem=detour_sem.at[1],
            device_id=partner,
            device_id_type=MESH,
        )

    def detour_onward():
        place = radius + jnp.where(helps_next, orders[1][3], orders[2][3])
        return pltpu.make_async_remote_copy(
            src_ref=detour.at[:, my_rows, :],
            dst_ref=views.at[1, pl.ds(place, GROUP), my_rows, :],
            send_sem=detour_sem.at[2],
            recv_sem=z_sem.at[3, 1],
            device_id=helped_ends[0],
            device_id_type=MESH,
        )

    def z_arrival(k):
        here = views.at[1, pl.ds(radius + z_planes[k], GROUP), my_rows, :]
        return remote(here, here, z_sem.at[k], partner)

    def view_copy(which, side, k):
        src = (12 - 4 * k if side == 0 else 4 * k) + radius
        dst = 4 - 4 * k if side == 0 else planes + radius + 4 * k
        return remote(
            views.at[which, pl.ds(src, GROUP), my_rows, :],
            views.at[which, pl.ds(dst, GROUP), my_rows, :],
            view_sem.at[which, side, k],
            beside[side],
        )

    def direct_copy(side, k):
        src = 12 - 4 * k if side == 0 else 4 * k
        dst = 4 - 4 * k if side == 0 else planes + radius + 4 * k
        return remote(
            theirs.at[pl.ds(src, GROUP), other_rows, :],
            views.at[1, pl.ds(dst, GROUP), other_rows, :],
            view_sem.at[1, side, k],
            opposite[side],
        )

    def hop_copy(slot, src, high, send, there):
        return pltpu.make_async_remote_copy(
            src_ref=src,
            dst_ref=hop.at[slot, pl.ds(0, src.shape[0]), high, :],
            send_sem=hop_sem.at[0, send],
            recv_sem=hop_sem.at[1, slot],
            device_id=there,
            device_id_type=MESH,
        )

    def hop_start(side, k, across):
        place = est_place(side, k, core)
        src = spare.at[pl.ds(place, 2)] if across else est1.at[pl.ds(planes + place, 2)]
        there = relays_across[side] if across else relays[side]
        return hop_copy(k, src, pl.ds(0, rows), k + 2 * across, there)

    def hop_view(side, across):
        src = 8 if side == 0 else 4
        part = pl.ds(src, GROUP)
        if across:
            return hop_copy(1, theirs.at[part, other_rows, :], other_rows, 1, relays_across[side])
        return hop_copy(0, views.at[0, pl.ds(radius + src, GROUP), my_rows, :], my_rows, 0, relays[side])

    def onward(slot, side):
        target = sources[1 - side]
        if slot >= 2:
            src = hop.at[slot, pl.ds(0, 2)]
            dst = est1.at[pl.ds(2 * planes * side + est_place(side, slot, core), 2)]
            recv = start_sem.at[side, slot, 1]
        else:
            src = hop.at[slot, pl.ds(0, GROUP), my_rows, :]
            dst = views.at[slot, pl.ds(0 if side == 0 else planes + radius + 4, GROUP), my_rows, :]
            recv = view_sem.at[slot, side, 1, 1]
        return pltpu.make_async_remote_copy(
            src_ref=src,
            dst_ref=dst,
            send_sem=onward_sem.at[0, slot],
            recv_sem=recv,
            device_id=target,
            device_id_type=MESH,
        )

    def hop_arrival(slot):
        here = hop.at[slot, pl.ds(0, 2)] if slot >= 2 else hop.at[slot, pl.ds(0, GROUP), my_rows, :]
        return pltpu.make_async_remote_copy(
            src_ref=here,
            dst_ref=here,
            send_sem=onward_sem.at[1, slot],
            recv_sem=hop_sem.at[1, slot],
            device_id=partner,
            device_id_type=MESH,
        )

    def serve(slots):
        for side in range(2):

            @pl.when(at_relay[side])
            def _():
                for slot in slots:
                    hop_arrival(slot).wait_recv()
                    onward(slot, side).start()

    def prod_copy(i, q):
        part = pl.ds(q * GROUP, GROUP)
        return remote(prod.at[i, part], prod_in.at[i, part], prod_sem.at[i, q], sibling)

    def turn(source, p, own, other):
        @pl.when(upper == 0)
        def _():
            own[...] = source[p, :, pl.ds(0, 256)].T[:rows]
            other[...] = source[p, :, pl.ds(128, 256)].T[256 - rows :]

        @pl.when(upper == 1)
        def _():
            own[...] = source[p, :, pl.ds(128, 256)].T[256 - rows :]
            other[...] = source[p, :, pl.ds(0, 256)].T[:rows]

    plain = [jnp.logical_not(at_seam[side]) for side in range(2)]

    def turn_start(q):
        loads[q][0].wait()

        @pl.loop(q * GROUP, (q + 1) * GROUP)
        def _(p):
            turn(sin, p, est1.at[planes + p], spare.at[p])

    def send_start(k):
        for side in range(2):

            @pl.when(sends[side] & plain[side])
            def _():
                est_copy(est1, start_sem, side, k).start()

            @pl.when(at_seam[side] & (upper == core))
            def _():
                if k < 2:
                    est_copy(est1, start_sem, side, k).start()
                    extra_copy(side, k).start()
                else:
                    hop_start(side, k, 0).start()
                    hop_start(side, k, 1).start()

    with jax.named_scope("turn_start"):
        turn_start(3)
        turn_start(0)
        for q in (3, 0, 2, 1):
            loads[q][1].start()
    with jax.named_scope("barrier"):
        pl.semaphore_wait(barrier, count)
    with jax.named_scope("turn_rest"):
        send_start(0)
        kern_copy = remote(kern_in, kern.at[1], kern_sem, partner)
        kern_copy.start()
        turn_start(2)
        turn_start(1)
        for k in range(1, 4):
            send_start(k)
    with jax.named_scope("turn_views"):
        for k in range(4):
            q = z_planes[k] // GROUP
            part = pl.ds(q * GROUP, GROUP)
            pltpu.make_async_copy(views_in.at[part], vin.at[part], load_sem.at[1, q]).wait()

            @pl.loop(q * GROUP, (q + 1) * GROUP)
            def _(p):
                turn(vin, p, views.at[0, radius + p], theirs.at[p])

            if k == 3:

                @pl.when(ordinary)
                def _():
                    z_copy(3).start()

                @pl.when(jnp.logical_not(ordinary))
                def _():
                    detour_copy().start()
            else:

                @pl.when(jnp.logical_not(at_seam[0] | at_seam[1]) | (k < 2))
                def _():
                    z_copy(k).start()

        for k in range(2):
            for side in range(2):

                @pl.when(sends[side] & plain[side])
                def _():
                    view_copy(0, side, k).start()

    kern[0] = kern_in[...]
    ones = jnp.ones((8, wide), jnp.float32)
    view_pad = pl.multiple_of(lower * valid, 8)
    est_pad = pl.multiple_of(lower * known, 8)

    @pl.loop(0, views.shape[1])
    def _(f):
        for which in range(2):
            views[which, f, pl.ds(view_pad, 8), :] = ones
        est2[f + jnp.where(f >= planes, planes, 0), pl.ds(est_pad, 8), :] = ones
        est2[f + jnp.where(f >= planes, planes, 0), pl.ds(est_pad + 8, 8), :] = ones

    for side in range(2):

        @pl.when(jnp.logical_not(receives[side]))
        def _():
            zero = jnp.zeros((rows, wide), jnp.float32)

            @pl.loop(0, planes)
            def _(p):
                est1[2 * planes * side + p] = zero
                est2[2 * planes * side + p] = zero

            @pl.loop(0, radius)
            def _(p):
                for which in range(2):
                    views[which, (planes + radius) * side + p] = zero

    def bands(which):
        fill_bands(kern.at[which], taps, taps, xb.at[which], xf.at[which], wide, 1)
        fill_bands(kern.at[which], taps, 2 * taps, yf.at[which], yb.at[which], rows, 1)

    with jax.named_scope("bands"):
        bands(0)
        kern_copy.wait_recv()
        bands(1)

    def ahead_group(est, which, group, divide):
        base = group * GROUP
        coef = [kern[which, pl.ds(d, 1), :] for d in range(taps)]

        def finish(o, value):
            ratio[which, base + o] = views[which, base + o] / value if divide else value

        convolve(taps, coef, lambda i, r0: est[base + i, pl.ds(r0, CHUNK), :], xf[which], yf[which], mixed, finish)

    def back_group(i, which, group):
        base = group * GROUP
        coef = [kern[which, pl.ds(taps - 1 - d, 1), :] for d in range(taps)]

        def finish(o, value):
            prod[i, base + o] = value if which == 0 else prod[i, base + o] * value

        convolve(
            taps, coef, lambda j, r0: ratio[which, base + j, pl.ds(r0, CHUNK), :], xb[which], yb[which], mixed, finish
        )

    def hand_over(est, sem, side_sem, k):
        for side in range(2):

            @pl.when(receives[side])
            def _():
                est_copy(est, sem, side, k).wait_recv()
                pass_copy(est, side_sem, side, k, core).start()

    def arrive(est, side_sem, k):
        for side in range(2):

            @pl.when(receives[side])
            def _():
                pass_copy(est, side_sem, side, k, 1 - core).wait_recv()

    def ahead(est, k, divide, between):
        @pl.loop(0, 2)
        def _(which):
            @pl.loop(0, 2)
            def _(n):
                ahead_group(est, which, 3 - k + n * (2 * k + 1), divide)

            @pl.when(which == 0)
            def _():
                between()

    def ahead1(k, more):
        with jax.named_scope("arrive1"):
            arrive(est1, pass_sem.at[0], k)
        with jax.named_scope("ahead1"):

            def between():
                if more:
                    hand_over(est1, start_sem, pass_sem.at[0], k + 1)

                    @pl.when(k == 0)
                    def _():
                        serve((2, 3))

                    for side in range(2):

                        @pl.when(at_seam[side] & (k == 1))
                        def _():
                            hop_view(side, 0).start()
                            hop_view(side, 1).start()
                            z_copy(2).start()

            ahead(est1, k, False, between)

    with jax.named_scope("arrive1"):
        hand_over(est1, start_sem, pass_sem.at[0], 0)

    @pl.loop(0, 3)
    def _(k):
        ahead1(k, True)

    ahead1(3, False)

    for side in range(2):

        @pl.when(at_seam[side])
        def _():
            view_copy(0, side, 0).start()
            direct_copy(side, 0).start()

    def forward(k):
        with jax.named_scope("wait_z"):
            z_arrival(k).wait_recv()
        for kind, order in zip(kinds, orders):
            side = 0 if order[k] >= 8 else 1
            piece = 0 if order[k] in (0, 12) else 1

            @pl.when(kind & sends[side] & plain[side])
            def _():
                view_copy(1, side, piece).start()

    with jax.named_scope("help"):

        @pl.when(helps_next | helps_previous)
        def _():
            detour_arrival().wait_recv()
            detour_onward().start()

    forward(0)
    forward(1)
    with jax.named_scope("serve"):
        serve((0, 1))
    pl.when(ordinary)(functools.partial(forward, 2))


    def divide(which, first, number):
        @pl.loop(first, first + number)
        def _(f):
            ratio[which, f] = views[which, f] / ratio[which, f]

    with jax.named_scope("wait_own"):
        for k in range(2):
            for side in range(2):

                @pl.when(receives[side])
                def _():
                    view_copy(0, side, k).wait_recv()

    with jax.named_scope("back1own"):
        divide(0, 0, planes + 2 * radius)

        @pl.loop(0, planes // GROUP)
        def _(group):
            back_group(0, 0, group)

    pl.when(jnp.logical_not(ordinary))(functools.partial(forward, 2))
    forward(3)

    def update(i, est, q, store):
        prod_copy(i, q).wait_recv()
        for o in range(GROUP):
            p = q * GROUP + o
            both = prod[i, p] * prod_in[i, p]
            store(p, est[planes + p] * jnp.sqrt(jnp.sqrt(both)))

    def keep(p, value):
        est2[planes + p] = value

    for k in range(2):
        with jax.named_scope("wait_other"):
            for side in range(2):

                @pl.when(receives[side])
                def _():
                    view_copy(1, side, k).wait_recv()

        with jax.named_scope("back1other"):
            if k == 0:
                divide(1, 4, planes + 2 * radius - 8)
            else:
                divide(1, 0, 4)
                divide(1, planes + 2 * radius - 4, 4)
            groups = (1, 2) if k == 0 else (0, 3)

            @pl.loop(0, 2)
            def _(n):
                q = n + 1 if k == 0 else 3 * n
                back_group(0, 1, q)
                prod_copy(0, q).start()

        with jax.named_scope("update1"):
            for q in groups:
                update(0, est1, q, keep)
        for piece in (1,) if k == 0 else (0, 2, 3):
            for side in range(2):

                @pl.when(sends[side])
                def _():
                    est_copy(est2, est_sem, side, piece).start()

    def ahead2(k, more):
        with jax.named_scope("arrive2"):
            arrive(est2, pass_sem.at[1], k)
        with jax.named_scope("ahead2"):

            def between():
                if more:
                    hand_over(est2, est_sem, pass_sem.at[1], k + 1)

            ahead(est2, k, True, between)

    with jax.named_scope("arrive2"):
        hand_over(est2, est_sem, pass_sem.at[1], 0)

    @pl.loop(0, 3)
    def _(k):
        ahead2(k, True)

    own_rows = pl.ds(pl.multiple_of(upper * half, 8), half)
    rest_rows = pl.ds(pl.multiple_of(lower * half, 8), half)
    inner = pl.multiple_of(upper * (rows - half), 8)

    def last_part(q, who, high):
        return result.at[pl.ds(q * GROUP + 2 * who, 2), high, :]

    def last_copy(q):
        part = last_part(q, core, own_rows)
        return remote(part, part, last_sem.at[0, q], partner)

    def last_arrival(q):
        part = last_part(q, core, rest_rows)
        return remote(part, part, last_sem.at[0, q], partner)

    def last_pass(q, who):
        part = last_part(q, who, rest_rows)
        return remote(part, part, last_sem.at[1, q], sibling)

    def out_copy(q):
        part = pl.ds(q * GROUP, GROUP)
        return pltpu.make_async_copy(result.at[part], out.at[part], out_sem.at[q])

    def finish_group(q):
        prod_copy(1, q).wait_recv()
        for o in range(GROUP):
            p = q * GROUP + o
            both = prod[1, p] * prod_in[1, p]
            prod_in[0, p] = est2[planes + p] * jnp.sqrt(jnp.sqrt(both))
            result[p, own_rows, :] = prod_in[0, p, pl.ds(inner, half), :]

        last_copy(q).start()

    def back2(first, step):
        @pl.loop(0, 2)
        def _(n):
            q = first + step * n
            with jax.named_scope("back2"):
                back_group(1, 0, q)
                back_group(1, 1, q)
                prod_copy(1, q).start()

            @pl.when(n > 0)
            def _():
                finish_group(first)

    back2(1, 1)
    ahead2(3, False)
    finish_group(2)
    back2(0, 3)
    finish_group(3)

    with jax.named_scope("wait_last"):
        for n, q in enumerate((1, 2, 0, 3)):
            last_arrival(q).wait_recv()
            last_pass(q, core).start()
            if n > 0:
                last_pass(before, 1 - core).wait_recv()
                out_copy(before).start()
            before = q
        last_pass(before, 1 - core).wait_recv()
        out_copy(before).start()

    kern_copy.wait_send()
    @pl.when(ordinary)
    def _():
        z_copy(3).wait_send()

    @pl.when(jnp.logical_not(ordinary))
    def _():
        detour_copy().wait_send()

    @pl.when(helps_next | helps_previous)
    def _():
        detour_onward().wait_send()

    for k in range(4):
        if k < 3:
            z_copy(k).wait_send()
        prod_copy(0, k).wait_send()
        prod_copy(1, k).wait_send()
    for q in range(planes // GROUP):

        last_copy(q).wait_send()
        last_pass(q, core).wait_send()
        out_copy(q).wait()
    for side in range(2):
        for k in range(4):

            @pl.when(sends[side])
            def _():
                est_copy(est2, est_sem, side, k).wait_send()

            @pl.when(sends[side] & plain[side])
            def _():
                est_copy(est1, start_sem, side, k).wait_send()

            @pl.when(at_seam[side] & (upper == core))
            def _():
                if k < 2:
                    est_copy(est1, start_sem, side, k).wait_send()
                    extra_copy(side, k).wait_send()
                else:
                    hop_start(side, k, 0).wait_send()
                    hop_start(side, k, 1).wait_send()

            @pl.when(receives[side])
            def _():
                pass_copy(est1, pass_sem.at[0], side, k, core).wait_send()
                pass_copy(est2, pass_sem.at[1], side, k, core).wait_send()

        for k in range(2):

            @pl.when(sends[side] & plain[side])
            def _():
                view_copy(0, side, k).wait_send()
                view_copy(1, side, k).wait_send()

        @pl.when(at_seam[side])
        def _():
            view_copy(0, side, 0).wait_send()
            hop_view(side, 0).wait_send()
            direct_copy(side, 0).wait_send()
            hop_view(side, 1).wait_send()

        @pl.when(at_relay[side])
        def _():
            for slot in range(4):
                onward(slot, side).wait_send()


def turn_back(source, target):
    for p in range(source.shape[0]):
        target[p] = source[p].T


def on_device(views_data, start, psf_table, psf_index):
    planes, width_x, width_y = start.shape
    taps = psf_table.shape[2]
    radius = (taps - 1) // 2
    rows = width_y // 2 + 4 * radius
    outer = planes + 2 * radius

    picked = (jnp.arange(psf_table.shape[0]) == psf_index[0]).astype(jnp.float32)
    kern = jnp.sum(picked[:, None, None] * psf_table, axis=0)
    kern = kern / jnp.sum(kern, axis=-1, keepdims=True)
    kern = jnp.broadcast_to(jnp.pad(kern.reshape(-1), (0, -kern.size % 8))[:, None], (kern.size + -kern.size % 8, 128))

    f32, bf16 = jnp.float32, jnp.bfloat16
    plane = (rows, width_x)
    dma = pltpu.SemaphoreType.DMA
    anywhere = pl.BlockSpec(memory_space=pl.ANY)
    turned = pl.pallas_call(
        functools.partial(whole_kernel, taps),
        name="deconvolve",
        out_shape=jax.ShapeDtypeStruct((planes, width_y, width_x), f32),
        in_specs=[anywhere, anywhere, pl.BlockSpec(memory_space=pltpu.VMEM)],
        out_specs=anywhere,
        scratch_shapes=[
            pltpu.VMEM((planes, width_x, width_y), f32),
            pltpu.VMEM((planes, width_x, width_y), f32),
            pltpu.VMEM((2,) + kern.shape, f32),
            pltpu.VMEM((2, 2 * width_x, 2 * width_x), bf16),
            pltpu.VMEM((2, 2 * width_x, 2 * width_x), bf16),
            pltpu.VMEM((2, rows, 3 * rows), bf16),
            pltpu.VMEM((2, rows, 3 * rows), bf16),
            pltpu.VMEM((3 * planes,) + plane, f32),
            pltpu.VMEM((3 * planes,) + plane, f32),
            pltpu.VMEM((planes,) + plane, f32),
            pltpu.VMEM((2, outer) + plane, f32),
            pltpu.VMEM((planes,) + plane, f32),
            pltpu.VMEM((2, outer) + plane, f32),
            pltpu.VMEM((GROUP,) + plane, f32),
            pltpu.VMEM((2, planes) + plane, f32),
            pltpu.VMEM((2, planes) + plane, f32),
            pltpu.VMEM((planes, width_y, width_x), f32),
            pltpu.VMEM((4, GROUP) + plane, f32),
            pltpu.VMEM((GROUP,) + plane, f32),
            dma((2, 4)),
            dma((4,)),
            dma((2,)),
            dma((4, 2)),
            dma((2, 4, 2)),
            dma((2, 2)),
            dma((2, 2, 4, 2)),
            dma((2, 2, 2, 2)),
            dma((2, 4, 2)),
            dma((2, 4, 2)),
            dma((2, 4, 2)),
            dma((2, 6)),
            dma((2, 4)),
            dma((3,)),
        ],
        compiler_params=pltpu.CompilerParams(
            collective_id=0, has_side_effects=True, vmem_limit_bytes=60 * 2**20
        ),
    )(views_data[0], start, kern)
    return pl.pallas_call(
        turn_back,
        name="turn_back",
        grid=(planes // GROUP,),
        out_shape=jax.ShapeDtypeStruct(start.shape, f32),
        in_specs=[pl.BlockSpec((GROUP, width_y, width_x), lambda q: (q, 0, 0))],
        out_specs=pl.BlockSpec((GROUP, width_x, width_y), lambda q: (q, 0, 0)),
    )(turned)


def solution(mesh):
    return jax.shard_map(
        on_device,
        mesh=mesh,
        in_specs=(P("view", "gz", None, None), P("gz", None, None), P(), P("view")),
        out_specs=P("gz", None, None),
        check_vma=False,
    )
```

```python
import functools

import jax
import jax.numpy as jnp
from jax import lax
from jax.experimental import pallas as pl
from jax.experimental.pallas import tpu as pltpu
from jax.sharding import PartitionSpec as P

MESH = pl.DeviceIdType.MESH
GROUP = 4
CHUNK = 32


def halves(value):
    high = value.astype(jnp.bfloat16)
    return high, (value - high.astype(jnp.float32)).astype(jnp.bfloat16)


def fill_bands(kern, taps, first_tap, ahead, behind, period, low_block):
    rows, cols = ahead.shape
    step = 32
    radius = (taps - 1) // 2

    @pl.loop(0, rows // step)
    def _(block):
        top = pl.multiple_of(block * step, step)
        row = lax.broadcasted_iota(jnp.int32, (step, cols), 0) + top
        col = lax.broadcasted_iota(jnp.int32, (step, cols), 1)
        is_low = (col >= low_block * period) & (col < (low_block + 1) * period)
        for wrap in range(cols // period - 1):
            col = jnp.where(col >= period, col - period, col)
        for wrap in range(rows // period - 1):
            row = jnp.where(row >= period, row - period, row)
        shift = col - row
        first = jnp.zeros((step, cols), jnp.float32)
        second = first
        for tap in range(taps):
            value = jnp.broadcast_to(kern[pl.ds(first_tap + tap, 1), pl.ds(0, 1)], (step, cols))
            first = jnp.where(shift == tap - radius, value, first)
            second = jnp.where(shift == radius - tap, value, second)
        for target, matrix in ((ahead, first), (behind, second)):
            high = matrix.astype(jnp.bfloat16).astype(jnp.float32)
            target[pl.ds(top, step), :] = jnp.where(is_low, matrix - high, high).astype(jnp.bfloat16)


def convolve(taps, coef, read, matrix_x, matrix_y, mixed, finish):
    rows = mixed.shape[1]
    wide = mixed.shape[2]
    for r0 in range(0, rows, CHUNK):
        total = [None] * GROUP
        for i in range(taps + GROUP - 1):
            value = read(i, r0)
            for o in range(GROUP):
                if 0 <= i - o < taps:
                    term = coef[i - o] * value
                    total[o] = term if total[o] is None else total[o] + term
        for o in range(GROUP):
            mixed[o, pl.ds(r0, CHUNK), :] = total[o]
    for pair in range(GROUP // 2):
        both = []
        for o in (2 * pair, 2 * pair + 1):
            high, low = halves(mixed[o])
            out = jnp.dot(jnp.concatenate([high, low], axis=1), matrix_x, preferred_element_type=jnp.float32)
            both.append(halves(out[:, :wide] + out[:, wide:]))
        high = jnp.concatenate([both[0][0], both[1][0]], axis=1)
        low = jnp.concatenate([both[0][1], both[1][1]], axis=1)
        out = jnp.dot(matrix_y, jnp.concatenate([high, high, low], axis=0), preferred_element_type=jnp.float32)
        finish(2 * pair, out[:, :wide])
        finish(2 * pair + 1, out[:, wide:])


def whole_kernel(
    taps, views_in, start_in, table_in, index, out,
    table, vin, sin, kern, xf, xb, yf, yb, est1, est2, spare, views, theirs, ratio, mixed, prod, prod_in, result, hop, detour,
    load_sem, out_sem, kern_sem, z_sem, start_sem, extra_sem, pass_sem, view_sem, est_sem, prod_sem, last_sem,
    hop_sem, onward_sem, detour_sem,
):
    planes, full, wide = result.shape
    rows = views.shape[2]
    half = full // 2
    radius = (taps - 1) // 2
    valid = rows - radius
    known = rows - 2 * radius
    v = lax.axis_index("view")
    g = lax.axis_index("gz")
    last = lax.axis_size("gz") - 1
    upper, core = v // 2, v % 2
    lower = 1 - upper
    seam = (last + 1) // 2
    partner = {"view": (v + 2) % 4, "gz": g}
    sibling = {"view": v + 1 - 2 * core, "gz": g}
    beside = ({"view": v, "gz": g + 1}, {"view": v, "gz": g - 1})
    opposite = ({"view": (v + 2) % 4, "gz": g + 1}, {"view": (v + 2) % 4, "gz": g - 1})
    sends = (g < last, g > 0)
    receives = (g > 0, g < last)
    at_seam = (g == seam - 1, g == seam)

    loads = []
    for q in range(planes // GROUP):
        part = pl.ds(q * GROUP, GROUP)
        loads.append(
            (
                pltpu.make_async_copy(start_in.at[part], sin.at[part], load_sem.at[0, q]),
                pltpu.make_async_copy(views_in.at[part], vin.at[part], load_sem.at[1, q]),
            )
        )
    table_copy = pltpu.make_async_copy(table_in, table, out_sem.at[0])
    table_copy.start()
    for q in (3, 0, 2, 1):
        loads[q][0].start()

    relays = ({"view": v, "gz": last}, {"view": v, "gz": 0})
    relays_across = ({"view": (v + 2) % 4, "gz": last}, {"view": (v + 2) % 4, "gz": 0})
    at_relay = (g == last, g == 0)
    sources = ({"view": v, "gz": seam - 1}, {"view": v, "gz": seam})
    sources_across = ({"view": (v + 2) % 4, "gz": seam - 1}, {"view": (v + 2) % 4, "gz": seam})

    only_next = (g == 0) | (g == seam)
    only_previous = (g == last) | (g == seam - 1)
    ordinary = jnp.logical_not(only_next | only_previous)
    orders = ((12, 0, 8, 4), (12, 8, 0, 4), (0, 4, 12, 8))
    kinds = (ordinary, only_next, only_previous)
    away = 3 * seam // 4
    helper = jnp.where(only_next, g + away, g - away)
    helps_next = (g == away) | (g == seam + away)
    helps_previous = (g == seam - 1 - away) | (g == last - away)
    helped = jnp.where(helps_next, g - away, g + away)
    helpers = ({"view": v, "gz": helper}, {"view": (v + 2) % 4, "gz": helper})
    helped_ends = ({"view": v, "gz": helped}, {"view": (v + 2) % 4, "gz": helped})

    barrier = pltpu.get_barrier_semaphore()

    def greet(there):
        pl.semaphore_signal(barrier, inc=1, device_id=there, device_id_type=MESH)

    greet(partner)
    greet(sibling)

    @pl.when(jnp.logical_not(ordinary))
    def _():
        greet(helpers[0])
        greet(helpers[1])

    @pl.when(helps_next | helps_previous)
    def _():
        greet(helped_ends[0])
        greet(helped_ends[1])

    count = 2 + jnp.where(ordinary, 0, 2) + jnp.where(helps_next | helps_previous, 2, 0)
    for side in range(2):

        @pl.when(sends[side])
        def _():
            greet(beside[side])

        @pl.when(at_seam[side])
        def _():
            greet(opposite[side])
            greet(relays[side])
            greet(relays_across[side])
            greet(relays[1 - side])

        @pl.when(at_relay[side])
        def _():
            greet(sources[side])
            greet(sources_across[side])
            greet(sources[1 - side])

        count = count + jnp.where(sends[side], 1, 0) + jnp.where(at_seam[side], 4, 0) + jnp.where(at_relay[side], 3, 0)

    def remote(src, dst, sem, there):
        return pltpu.make_async_remote_copy(
            src_ref=src, dst_ref=dst, send_sem=sem.at[0], recv_sem=sem.at[1], device_id=there, device_id_type=MESH
        )

    def est_place(side, k, who):
        return 14 - 2 * who - 4 * k if side == 0 else 2 * who + 4 * k

    def est_copy(est, sem, side, k):
        high = rows if est is est1 else known
        offset = 0 if est is est1 else pl.multiple_of(upper * 2 * radius, 8)
        place = est_place(side, k, core)
        src = est.at[pl.ds(planes + place, 2), pl.ds(offset, high), :]
        dst = est.at[pl.ds(2 * planes * side + place, 2), pl.ds(offset, high), :]
        return remote(src, dst, sem.at[side, k], beside[side])

    def extra_copy(side, k):
        place = est_place(side, k, core)
        return pltpu.make_async_remote_copy(
            src_ref=spare.at[pl.ds(place, 2)],
            dst_ref=est1.at[pl.ds(2 * planes * side + place, 2)],
            send_sem=extra_sem.at[side, k],
            recv_sem=start_sem.at[side, k, 1],
            device_id=opposite[side],
            device_id_type=MESH,
        )

    def pass_copy(est, sem, side, k, who):
        high = rows if est is est1 else known
        offset = 0 if est is est1 else pl.multiple_of(upper * 2 * radius, 8)
        place = est.at[pl.ds(2 * planes * side + est_place(side, k, who), 2), pl.ds(offset, high), :]
        return remote(place, place, sem.at[side, k], sibling)

    my_rows = pl.ds(pl.multiple_of(upper * radius, 8), valid)
    other_rows = pl.ds(pl.multiple_of(lower * radius, 8), valid)
    z_planes = [
        jnp.where(only_next, orders[1][k], jnp.where(only_previous, orders[2][k], orders[0][k])) for k in range(4)
    ]

    def z_copy(k):
        return remote(
            theirs.at[pl.ds(z_planes[k], GROUP), other_rows, :],
            views.at[1, pl.ds(radius + z_planes[k], GROUP), other_rows, :],
            z_sem.at[k],
            partner,
        )

    def detour_copy():
        return pltpu.make_async_remote_copy(
            src_ref=theirs.at[pl.ds(z_planes[3], GROUP), other_rows, :],
            dst_ref=detour.at[:, other_rows, :],
            send_sem=detour_sem.at[0],
            recv_sem=detour_sem.at[1],
            device_id=helpers[1],
            device_id_type=MESH,
        )

    def detour_arrival():
        here = detour.at[:, my_rows, :]
        return pltpu.make_async_remote_copy(
            src_ref=here,
            dst_ref=here,
            send_sem=detour_sem.at[0],
            recv_sem=detour_sem.at[1],
            device_id=partner,
            device_id_type=MESH,
        )

    def detour_onward():
        place = radius + jnp.where(helps_next, orders[1][3], orders[2][3])
        return pltpu.make_async_remote_copy(
            src_ref=detour.at[:, my_rows, :],
            dst_ref=views.at[1, pl.ds(place, GROUP), my_rows, :],
            send_sem=detour_sem.at[2],
            recv_sem=z_sem.at[3, 1],
            device_id=helped_ends[0],
            device_id_type=MESH,
        )

    def z_arrival(k):
        here = views.at[1, pl.ds(radius + z_planes[k], GROUP), my_rows, :]
        return remote(here, here, z_sem.at[k], partner)

    def view_copy(which, side, k):
        src = (12 - 4 * k if side == 0 else 4 * k) + radius
        dst = 4 - 4 * k if side == 0 else planes + radius + 4 * k
        return remote(
            views.at[which, pl.ds(src, GROUP), my_rows, :],
            views.at[which, pl.ds(dst, GROUP), my_rows, :],
            view_sem.at[which, side, k],
            beside[side],
        )

    def direct_copy(side, k):
        src = 12 - 4 * k if side == 0 else 4 * k
        dst = 4 - 4 * k if side == 0 else planes + radius + 4 * k
        return remote(
            theirs.at[pl.ds(src, GROUP), other_rows, :],
            views.at[1, pl.ds(dst, GROUP), other_rows, :],
            view_sem.at[1, side, k],
            opposite[side],
        )

    def hop_copy(slot, src, high, send, there):
        return pltpu.make_async_remote_copy(
            src_ref=src,
            dst_ref=hop.at[slot, pl.ds(0, src.shape[0]), high, :],
            send_sem=hop_sem.at[0, send],
            recv_sem=hop_sem.at[1, slot],
            device_id=there,
            device_id_type=MESH,
        )

    def hop_start(side, k, across):
        place = est_place(side, k, core)
        src = spare.at[pl.ds(place, 2)] if across else est1.at[pl.ds(planes + place, 2)]
        there = relays_across[side] if across else relays[side]
        return hop_copy(k, src, pl.ds(0, rows), k + 2 * across, there)

    def hop_view(side, across):
        src = 8 if side == 0 else 4
        part = pl.ds(src, GROUP)
        if across:
            return hop_copy(1, theirs.at[part, other_rows, :], other_rows, 1, relays_across[side])
        return hop_copy(0, views.at[0, pl.ds(radius + src, GROUP), my_rows, :], my_rows, 0, relays[side])

    def onward(slot, side):
        target = sources[1 - side]
        if slot >= 2:
            src = hop.at[slot, pl.ds(0, 2)]
            dst = est1.at[pl.ds(2 * planes * side + est_place(side, slot, core), 2)]
            recv = start_sem.at[side, slot, 1]
        else:
            src = hop.at[slot, pl.ds(0, GROUP), my_rows, :]
            dst = views.at[slot, pl.ds(0 if side == 0 else planes + radius + 4, GROUP), my_rows, :]
            recv = view_sem.at[slot, side, 1, 1]
        return pltpu.make_async_remote_copy(
            src_ref=src,
            dst_ref=dst,
            send_sem=onward_sem.at[0, slot],
            recv_sem=recv,
            device_id=target,
            device_id_type=MESH,
        )

    def hop_arrival(slot):
        here = hop.at[slot, pl.ds(0, 2)] if slot >= 2 else hop.at[slot, pl.ds(0, GROUP), my_rows, :]
        return pltpu.make_async_remote_copy(
            src_ref=here,
            dst_ref=here,
            send_sem=onward_sem.at[1, slot],
            recv_sem=hop_sem.at[1, slot],
            device_id=partner,
            device_id_type=MESH,
        )

    def serve(slots):
        for side in range(2):

            @pl.when(at_relay[side])
            def _():
                for slot in slots:
                    hop_arrival(slot).wait_recv()
                    onward(slot, side).start()

    def prod_copy(i, q):
        part = pl.ds(q * GROUP, GROUP)
        return remote(prod.at[i, part], prod_in.at[i, part], prod_sem.at[i, q], sibling)

    def turn(source, p, own, other):
        @pl.when(upper == 0)
        def _():
            own[...] = source[p, :, pl.ds(0, 256)].T[:rows]
            other[...] = source[p, :, pl.ds(128, 256)].T[256 - rows :]

        @pl.when(upper == 1)
        def _():
            own[...] = source[p, :, pl.ds(128, 256)].T[256 - rows :]
            other[...] = source[p, :, pl.ds(0, 256)].T[:rows]

    plain = [jnp.logical_not(at_seam[side]) for side in range(2)]

    def turn_start(q):
        loads[q][0].wait()

        @pl.loop(q * GROUP, (q + 1) * GROUP)
        def _(p):
            turn(sin, p, est1.at[planes + p], spare.at[p])

    def send_start(k):
        for side in range(2):

            @pl.when(sends[side] & plain[side])
            def _():
                est_copy(est1, start_sem, side, k).start()

            @pl.when(at_seam[side] & (upper == core))
            def _():
                if k < 2:
                    est_copy(est1, start_sem, side, k).start()
                    extra_copy(side, k).start()
                else:
                    hop_start(side, k, 0).start()
                    hop_start(side, k, 1).start()

    kern[0] = jnp.zeros(kern.shape[1:], jnp.float32)
    table_copy.wait()
    rows_of = table[index[0]]
    rows_of = rows_of / jnp.sum(rows_of, axis=-1, keepdims=True)
    same = lax.broadcasted_iota(jnp.int32, (taps, taps), 0) == lax.broadcasted_iota(jnp.int32, (taps, taps), 1)
    for axis in range(3):
        spread = jnp.broadcast_to(rows_of[axis : axis + 1], (taps, taps))
        column = jnp.sum(jnp.where(same, spread, 0.0), axis=1, keepdims=True)
        kern[0, pl.ds(axis * taps, taps), :] = jnp.broadcast_to(column, (taps, wide))

    with jax.named_scope("turn_start"):
        turn_start(3)
        turn_start(0)
        for q in (3, 0, 2, 1):
            loads[q][1].start()
    with jax.named_scope("barrier"):
        pl.semaphore_wait(barrier, count)
    with jax.named_scope("turn_rest"):
        send_start(0)
        kern_copy = remote(kern.at[0], kern.at[1], kern_sem, partner)
        kern_copy.start()
        turn_start(2)
        turn_start(1)
        for k in range(1, 4):
            send_start(k)
    with jax.named_scope("turn_views"):
        for k in range(4):
            q = z_planes[k] // GROUP
            part = pl.ds(q * GROUP, GROUP)
            pltpu.make_async_copy(views_in.at[part], vin.at[part], load_sem.at[1, q]).wait()

            @pl.loop(q * GROUP, (q + 1) * GROUP)
            def _(p):
                turn(vin, p, views.at[0, radius + p], theirs.at[p])

            if k == 3:

                @pl.when(ordinary)
                def _():
                    z_copy(3).start()

                @pl.when(jnp.logical_not(ordinary))
                def _():
                    detour_copy().start()
            else:

                @pl.when(jnp.logical_not(at_seam[0] | at_seam[1]) | (k < 2))
                def _():
                    z_copy(k).start()

        for k in range(2):
            for side in range(2):

                @pl.when(sends[side] & plain[side])
                def _():
                    view_copy(0, side, k).start()

    ones = jnp.ones((8, wide), jnp.float32)
    view_pad = pl.multiple_of(lower * valid, 8)
    est_pad = pl.multiple_of(lower * known, 8)

    @pl.loop(0, views.shape[1])
    def _(f):
        for which in range(2):
            views[which, f, pl.ds(view_pad, 8), :] = ones
        est2[f + jnp.where(f >= planes, planes, 0), pl.ds(est_pad, 8), :] = ones
        est2[f + jnp.where(f >= planes, planes, 0), pl.ds(est_pad + 8, 8), :] = ones

    for side in range(2):

        @pl.when(jnp.logical_not(receives[side]))
        def _():
            zero = jnp.zeros((rows, wide), jnp.float32)

            @pl.loop(0, planes)
            def _(p):
                est1[2 * planes * side + p] = zero
                est2[2 * planes * side + p] = zero

            @pl.loop(0, radius)
            def _(p):
                for which in range(2):
                    views[which, (planes + radius) * side + p] = zero

    def bands(which):
        fill_bands(kern.at[which], taps, taps, xb.at[which], xf.at[which], wide, 1)
        fill_bands(kern.at[which], taps, 2 * taps, yf.at[which], yb.at[which], rows, 1)

    with jax.named_scope("bands"):
        bands(0)
        kern_copy.wait_recv()
        bands(1)

    def ahead_group(est, which, group, divide):
        base = group * GROUP
        coef = [kern[which, pl.ds(d, 1), :] for d in range(taps)]

        def finish(o, value):
            ratio[which, base + o] = views[which, base + o] / value if divide else value

        convolve(taps, coef, lambda i, r0: est[base + i, pl.ds(r0, CHUNK), :], xf[which], yf[which], mixed, finish)

    def back_group(i, which, group):
        base = group * GROUP
        coef = [kern[which, pl.ds(taps - 1 - d, 1), :] for d in range(taps)]

        def finish(o, value):
            prod[i, base + o] = value if which == 0 else prod[i, base + o] * value

        convolve(
            taps, coef, lambda j, r0: ratio[which, base + j, pl.ds(r0, CHUNK), :], xb[which], yb[which], mixed, finish
        )

    def hand_over(est, sem, side_sem, k):
        for side in range(2):

            @pl.when(receives[side])
            def _():
                est_copy(est, sem, side, k).wait_recv()
                pass_copy(est, side_sem, side, k, core).start()

    def arrive(est, side_sem, k):
        for side in range(2):

            @pl.when(receives[side])
            def _():
                pass_copy(est, side_sem, side, k, 1 - core).wait_recv()

    def ahead(est, k, divide, between):
        @pl.loop(0, 2)
        def _(which):
            @pl.loop(0, 2)
            def _(n):
                ahead_group(est, which, 3 - k + n * (2 * k + 1), divide)

            @pl.when(which == 0)
            def _():
                between()

    def ahead1(k, more):
        with jax.named_scope("arrive1"):
            arrive(est1, pass_sem.at[0], k)
        with jax.named_scope("ahead1"):

            def between():
                if more:
                    hand_over(est1, start_sem, pass_sem.at[0], k + 1)

                    @pl.when(k == 0)
                    def _():
                        serve((2, 3))

                    for side in range(2):

                        @pl.when(at_seam[side] & (k == 1))
                        def _():
                            hop_view(side, 0).start()
                            hop_view(side, 1).start()
                            z_copy(2).start()

            ahead(est1, k, False, between)

    with jax.named_scope("arrive1"):
        hand_over(est1, start_sem, pass_sem.at[0], 0)

    @pl.loop(0, 3)
    def _(k):
        ahead1(k, True)

    ahead1(3, False)

    for side in range(2):

        @pl.when(at_seam[side])
        def _():
            view_copy(0, side, 0).start()
            direct_copy(side, 0).start()

    def forward(k):
        with jax.named_scope("wait_z"):
            z_arrival(k).wait_recv()
        for kind, order in zip(kinds, orders):
            side = 0 if order[k] >= 8 else 1
            piece = 0 if order[k] in (0, 12) else 1

            @pl.when(kind & sends[side] & plain[side])
            def _():
                view_copy(1, side, piece).start()

    with jax.named_scope("help"):

        @pl.when(helps_next | helps_previous)
        def _():
            detour_arrival().wait_recv()
            detour_onward().start()

    forward(0)
    forward(1)
    with jax.named_scope("serve"):
        serve((0, 1))
    pl.when(ordinary)(functools.partial(forward, 2))


    def divide(which, first, number):
        @pl.loop(first, first + number)
        def _(f):
            ratio[which, f] = views[which, f] / ratio[which, f]

    with jax.named_scope("wait_own"):
        for k in range(2):
            for side in range(2):

                @pl.when(receives[side])
                def _():
                    view_copy(0, side, k).wait_recv()

    with jax.named_scope("back1own"):
        divide(0, 0, planes + 2 * radius)

        @pl.loop(0, planes // GROUP)
        def _(group):
            back_group(0, 0, group)

    pl.when(jnp.logical_not(ordinary))(functools.partial(forward, 2))
    forward(3)

    def update(i, est, q, store):
        prod_copy(i, q).wait_recv()
        for o in range(GROUP):
            p = q * GROUP + o
            both = prod[i, p] * prod_in[i, p]
            store(p, est[planes + p] * jnp.sqrt(jnp.sqrt(both)))

    def keep(p, value):
        est2[planes + p] = value

    for k in range(2):
        with jax.named_scope("wait_other"):
            for side in range(2):

                @pl.when(receives[side])
                def _():
                    view_copy(1, side, k).wait_recv()

        with jax.named_scope("back1other"):
            if k == 0:
                divide(1, 4, planes + 2 * radius - 8)
            else:
                divide(1, 0, 4)
                divide(1, planes + 2 * radius - 4, 4)
            groups = (1, 2) if k == 0 else (0, 3)

            @pl.loop(0, 2)
            def _(n):
                q = n + 1 if k == 0 else 3 * n
                back_group(0, 1, q)
                prod_copy(0, q).start()

        with jax.named_scope("update1"):
            for q in groups:
                update(0, est1, q, keep)
        for piece in (1,) if k == 0 else (0, 2, 3):
            for side in range(2):

                @pl.when(sends[side])
                def _():
                    est_copy(est2, est_sem, side, piece).start()

    def ahead2(k, more):
        with jax.named_scope("arrive2"):
            arrive(est2, pass_sem.at[1], k)
        with jax.named_scope("ahead2"):

            def between():
                if more:
                    hand_over(est2, est_sem, pass_sem.at[1], k + 1)

            ahead(est2, k, True, between)

    with jax.named_scope("arrive2"):
        hand_over(est2, est_sem, pass_sem.at[1], 0)

    @pl.loop(0, 3)
    def _(k):
        ahead2(k, True)

    own_rows = pl.ds(pl.multiple_of(upper * half, 8), half)
    rest_rows = pl.ds(pl.multiple_of(lower * half, 8), half)
    inner = pl.multiple_of(upper * (rows - half), 8)

    def last_part(q, who, high):
        return result.at[pl.ds(q * GROUP + 2 * who, 2), high, :]

    def last_copy(q):
        part = last_part(q, core, own_rows)
        return remote(part, part, last_sem.at[0, q], partner)

    def last_arrival(q):
        part = last_part(q, core, rest_rows)
        return remote(part, part, last_sem.at[0, q], partner)

    def last_pass(q, who):
        part = last_part(q, who, rest_rows)
        return remote(part, part, last_sem.at[1, q], sibling)

    def out_copy(q):
        part = pl.ds(q * GROUP, GROUP)
        return pltpu.make_async_copy(result.at[part], out.at[part], out_sem.at[q])

    def finish_group(q):
        prod_copy(1, q).wait_recv()
        for o in range(GROUP):
            p = q * GROUP + o
            both = prod[1, p] * prod_in[1, p]
            prod_in[0, p] = est2[planes + p] * jnp.sqrt(jnp.sqrt(both))
            result[p, own_rows, :] = prod_in[0, p, pl.ds(inner, half), :]

        last_copy(q).start()

    def back2(first, step):
        @pl.loop(0, 2)
        def _(n):
            q = first + step * n
            with jax.named_scope("back2"):
                back_group(1, 0, q)
                back_group(1, 1, q)
                prod_copy(1, q).start()

            @pl.when(n > 0)
            def _():
                finish_group(first)

    back2(1, 1)
    ahead2(3, False)
    finish_group(2)
    back2(0, 3)
    finish_group(3)

    with jax.named_scope("wait_last"):
        for n, q in enumerate((1, 2, 0, 3)):
            last_arrival(q).wait_recv()
            last_pass(q, core).start()
            if n > 0:
                last_pass(before, 1 - core).wait_recv()
                out_copy(before).start()
            before = q
        last_pass(before, 1 - core).wait_recv()
        out_copy(before).start()

    kern_copy.wait_send()
    @pl.when(ordinary)
    def _():
        z_copy(3).wait_send()

    @pl.when(jnp.logical_not(ordinary))
    def _():
        detour_copy().wait_send()

    @pl.when(helps_next | helps_previous)
    def _():
        detour_onward().wait_send()

    for k in range(4):
        if k < 3:
            z_copy(k).wait_send()
        prod_copy(0, k).wait_send()
        prod_copy(1, k).wait_send()
    for q in range(planes // GROUP):

        last_copy(q).wait_send()
        last_pass(q, core).wait_send()
        out_copy(q).wait()
    for side in range(2):
        for k in range(4):

            @pl.when(sends[side])
            def _():
                est_copy(est2, est_sem, side, k).wait_send()

            @pl.when(sends[side] & plain[side])
            def _():
                est_copy(est1, start_sem, side, k).wait_send()

            @pl.when(at_seam[side] & (upper == core))
            def _():
                if k < 2:
                    est_copy(est1, start_sem, side, k).wait_send()
                    extra_copy(side, k).wait_send()
                else:
                    hop_start(side, k, 0).wait_send()
                    hop_start(side, k, 1).wait_send()

            @pl.when(receives[side])
            def _():
                pass_copy(est1, pass_sem.at[0], side, k, core).wait_send()
                pass_copy(est2, pass_sem.at[1], side, k, core).wait_send()

        for k in range(2):

            @pl.when(sends[side] & plain[side])
            def _():
                view_copy(0, side, k).wait_send()
                view_copy(1, side, k).wait_send()

        @pl.when(at_seam[side])
        def _():
            view_copy(0, side, 0).wait_send()
            hop_view(side, 0).wait_send()
            direct_copy(side, 0).wait_send()
            hop_view(side, 1).wait_send()

        @pl.when(at_relay[side])
        def _():
            for slot in range(4):
                onward(slot, side).wait_send()


def turn_back(source, target, held, turned, in_sem, out_sem):
    pieces = source.shape[0] // 2

    def bring(q):
        part = pl.ds(2 * q, 2)
        return pltpu.make_async_copy(source.at[part], held.at[part], in_sem.at[q])

    def store(q):
        part = pl.ds(2 * q, 2)
        return pltpu.make_async_copy(turned.at[part], target.at[part], out_sem.at[q])

    for q in range(pieces):
        bring(q).start()

    @pl.loop(0, pieces)
    def _(q):
        bring(q).wait()
        for o in range(2):
            turned[2 * q + o] = held[2 * q + o].T
        store(q).start()

    for q in range(pieces):
        store(q).wait()


def on_device(views_data, start, psf_table, psf_index):
    planes, width_x, width_y = start.shape
    taps = psf_table.shape[2]
    radius = (taps - 1) // 2
    rows = width_y // 2 + 4 * radius
    outer = planes + 2 * radius

    f32, bf16 = jnp.float32, jnp.bfloat16
    plane = (rows, width_x)
    dma = pltpu.SemaphoreType.DMA
    anywhere = pl.BlockSpec(memory_space=pl.ANY)
    turned = pl.pallas_call(
        functools.partial(whole_kernel, taps),
        name="deconvolve",
        out_shape=jax.ShapeDtypeStruct((planes, width_y, width_x), f32),
        in_specs=[
            anywhere,
            anywhere,
            anywhere,
            pl.BlockSpec(memory_space=pltpu.SMEM),
        ],
        out_specs=anywhere,
        scratch_shapes=[
            pltpu.VMEM(psf_table.shape, f32),
            pltpu.VMEM((planes, width_x, width_y), f32),
            pltpu.VMEM((planes, width_x, width_y), f32),
            pltpu.VMEM((2, 3 * taps + -3 * taps % 8, width_x), f32),
            pltpu.VMEM((2, 2 * width_x, 2 * width_x), bf16),
            pltpu.VMEM((2, 2 * width_x, 2 * width_x), bf16),
            pltpu.VMEM((2, rows, 3 * rows), bf16),
            pltpu.VMEM((2, rows, 3 * rows), bf16),
            pltpu.VMEM((3 * planes,) + plane, f32),
            pltpu.VMEM((3 * planes,) + plane, f32),
            pltpu.VMEM((planes,) + plane, f32),
            pltpu.VMEM((2, outer) + plane, f32),
            pltpu.VMEM((planes,) + plane, f32),
            pltpu.VMEM((2, outer) + plane, f32),
            pltpu.VMEM((GROUP,) + plane, f32),
            pltpu.VMEM((2, planes) + plane, f32),
            pltpu.VMEM((2, planes) + plane, f32),
            pltpu.VMEM((planes, width_y, width_x), f32),
            pltpu.VMEM((4, GROUP) + plane, f32),
            pltpu.VMEM((GROUP,) + plane, f32),
            dma((2, 4)),
            dma((4,)),
            dma((2,)),
            dma((4, 2)),
            dma((2, 4, 2)),
            dma((2, 2)),
            dma((2, 2, 4, 2)),
            dma((2, 2, 2, 2)),
            dma((2, 4, 2)),
            dma((2, 4, 2)),
            dma((2, 4, 2)),
            dma((2, 6)),
            dma((2, 4)),
            dma((3,)),
        ],
        compiler_params=pltpu.CompilerParams(
            collective_id=0, has_side_effects=True, vmem_limit_bytes=60 * 2**20
        ),
    )(views_data[0], start, psf_table, psf_index)
    return pl.pallas_call(
        turn_back,
        name="turn_back",
        out_shape=jax.ShapeDtypeStruct(start.shape, f32),
        in_specs=[anywhere],
        out_specs=anywhere,
        scratch_shapes=[
            pltpu.VMEM((planes, width_y, width_x), f32),
            pltpu.VMEM(start.shape, f32),
            dma((planes // 2,)),
            dma((planes // 2,)),
        ],
    )(turned)


def solution(mesh):
    return jax.shard_map(
        on_device,
        mesh=mesh,
        in_specs=(P("view", "gz", None, None), P("gz", None, None), P(), P("view")),
        out_specs=P("gz", None, None),
        check_vma=False,
    )
```

```python
import functools

import jax
import jax.numpy as jnp
from jax import lax
from jax.experimental import pallas as pl
from jax.experimental.pallas import tpu as pltpu
from jax.sharding import PartitionSpec as P

MESH = pl.DeviceIdType.MESH
GROUP = 4
CHUNK = 32


def halves(value):
    high = value.astype(jnp.bfloat16)
    return high, (value - high.astype(jnp.float32)).astype(jnp.bfloat16)


def fill_bands(kern, taps, first_tap, ahead, behind, period, low_block):
    rows, cols = ahead.shape
    step = 32
    radius = (taps - 1) // 2

    @pl.loop(0, rows // step)
    def _(block):
        top = pl.multiple_of(block * step, step)
        row = lax.broadcasted_iota(jnp.int32, (step, cols), 0) + top
        col = lax.broadcasted_iota(jnp.int32, (step, cols), 1)
        is_low = (col >= low_block * period) & (col < (low_block + 1) * period)
        for wrap in range(cols // period - 1):
            col = jnp.where(col >= period, col - period, col)
        for wrap in range(rows // period - 1):
            row = jnp.where(row >= period, row - period, row)
        shift = col - row
        first = jnp.zeros((step, cols), jnp.float32)
        second = first
        for tap in range(taps):
            value = jnp.broadcast_to(kern[pl.ds(first_tap + tap, 1), pl.ds(0, 1)], (step, cols))
            first = jnp.where(shift == tap - radius, value, first)
            second = jnp.where(shift == radius - tap, value, second)
        for target, matrix in ((ahead, first), (behind, second)):
            high = matrix.astype(jnp.bfloat16).astype(jnp.float32)
            target[pl.ds(top, step), :] = jnp.where(is_low, matrix - high, high).astype(jnp.bfloat16)


def convolve(taps, coef, read, matrix_x, matrix_y, mixed, finish):
    rows = mixed.shape[1]
    wide = mixed.shape[2]
    for r0 in range(0, rows, CHUNK):
        total = [None] * GROUP
        for i in range(taps + GROUP - 1):
            value = read(i, r0)
            for o in range(GROUP):
                if 0 <= i - o < taps:
                    term = coef[i - o] * value
                    total[o] = term if total[o] is None else total[o] + term
        for o in range(GROUP):
            mixed[o, pl.ds(r0, CHUNK), :] = total[o]
    for pair in range(GROUP // 2):
        both = []
        for o in (2 * pair, 2 * pair + 1):
            high, low = halves(mixed[o])
            out = jnp.dot(jnp.concatenate([high, low], axis=1), matrix_x, preferred_element_type=jnp.float32)
            both.append(halves(out[:, :wide] + out[:, wide:]))
        high = jnp.concatenate([both[0][0], both[1][0]], axis=1)
        low = jnp.concatenate([both[0][1], both[1][1]], axis=1)
        out = jnp.dot(matrix_y, jnp.concatenate([high, high, low], axis=0), preferred_element_type=jnp.float32)
        finish(2 * pair, out[:, :wide])
        finish(2 * pair + 1, out[:, wide:])


def whole_kernel(
    taps, views_in, start_in, table_in, index, out,
    table, vin, sin, kern, xf, xb, yf, yb, est1, est2, spare, views, theirs, ratio, mixed, prod, prod_in, result, hop, detour,
    load_sem, out_sem, kern_sem, z_sem, start_sem, extra_sem, pass_sem, view_sem, est_sem, prod_sem, last_sem,
    hop_sem, onward_sem, detour_sem,
):
    planes, full, wide = result.shape
    rows = views.shape[2]
    half = full // 2
    radius = (taps - 1) // 2
    valid = rows - radius
    known = rows - 2 * radius
    v = lax.axis_index("view")
    g = lax.axis_index("gz")
    last = lax.axis_size("gz") - 1
    upper, core = v // 2, v % 2
    lower = 1 - upper
    seam = (last + 1) // 2
    partner = {"view": (v + 2) % 4, "gz": g}
    sibling = {"view": v + 1 - 2 * core, "gz": g}
    beside = ({"view": v, "gz": g + 1}, {"view": v, "gz": g - 1})
    opposite = ({"view": (v + 2) % 4, "gz": g + 1}, {"view": (v + 2) % 4, "gz": g - 1})
    sends = (g < last, g > 0)
    receives = (g > 0, g < last)
    at_seam = (g == seam - 1, g == seam)

    loads = []
    for q in range(planes // GROUP):
        part = pl.ds(q * GROUP, GROUP)
        loads.append(
            (
                pltpu.make_async_copy(start_in.at[part], sin.at[part], load_sem.at[0, q]),
                pltpu.make_async_copy(views_in.at[part], vin.at[part], load_sem.at[1, q]),
            )
        )
    table_copy = pltpu.make_async_copy(table_in, table, out_sem.at[0])
    table_copy.start()
    for q in (3, 0, 2, 1):
        loads[q][0].start()

    relays = ({"view": v, "gz": last}, {"view": v, "gz": 0})
    relays_across = ({"view": (v + 2) % 4, "gz": last}, {"view": (v + 2) % 4, "gz": 0})
    at_relay = (g == last, g == 0)
    sources = ({"view": v, "gz": seam - 1}, {"view": v, "gz": seam})
    sources_across = ({"view": (v + 2) % 4, "gz": seam - 1}, {"view": (v + 2) % 4, "gz": seam})

    only_next = (g == 0) | (g == seam)
    only_previous = (g == last) | (g == seam - 1)
    ordinary = jnp.logical_not(only_next | only_previous)
    orders = ((12, 0, 8, 4), (12, 8, 0, 4), (0, 4, 12, 8))
    kinds = (ordinary, only_next, only_previous)
    away = 3 * seam // 4
    helper = jnp.where(only_next, g + away, g - away)
    straight = jnp.logical_not(at_seam[0] | at_seam[1])
    helps_next = g == seam + away
    helps_previous = g == seam - 1 - away
    helped = jnp.where(helps_next, g - away, g + away)
    helpers = ({"view": v, "gz": helper}, {"view": (v + 2) % 4, "gz": helper})
    helped_ends = ({"view": v, "gz": helped}, {"view": (v + 2) % 4, "gz": helped})

    barrier = pltpu.get_barrier_semaphore()

    def greet(there):
        pl.semaphore_signal(barrier, inc=1, device_id=there, device_id_type=MESH)

    greet(partner)
    greet(sibling)

    @pl.when(jnp.logical_not(straight))
    def _():
        greet(helpers[0])
        greet(helpers[1])

    @pl.when(helps_next | helps_previous)
    def _():
        greet(helped_ends[0])
        greet(helped_ends[1])

    count = 2 + jnp.where(straight, 0, 2) + jnp.where(helps_next | helps_previous, 2, 0)
    for side in range(2):

        @pl.when(sends[side])
        def _():
            greet(beside[side])

        @pl.when(at_seam[side])
        def _():
            greet(opposite[side])
            greet(relays[side])
            greet(relays_across[side])
            greet(relays[1 - side])

        @pl.when(at_relay[side])
        def _():
            greet(sources[side])
            greet(sources_across[side])
            greet(sources[1 - side])

        count = count + jnp.where(sends[side], 1, 0) + jnp.where(at_seam[side], 4, 0) + jnp.where(at_relay[side], 3, 0)

    def remote(src, dst, sem, there):
        return pltpu.make_async_remote_copy(
            src_ref=src, dst_ref=dst, send_sem=sem.at[0], recv_sem=sem.at[1], device_id=there, device_id_type=MESH
        )

    def est_place(side, k, who):
        return 14 - 2 * who - 4 * k if side == 0 else 2 * who + 4 * k

    def est_copy(est, sem, side, k):
        high = rows if est is est1 else known
        offset = 0 if est is est1 else pl.multiple_of(upper * 2 * radius, 8)
        place = est_place(side, k, core)
        src = est.at[pl.ds(planes + place, 2), pl.ds(offset, high), :]
        dst = est.at[pl.ds(2 * planes * side + place, 2), pl.ds(offset, high), :]
        return remote(src, dst, sem.at[side, k], beside[side])

    def extra_copy(side, k):
        place = est_place(side, k, core)
        return pltpu.make_async_remote_copy(
            src_ref=spare.at[pl.ds(place, 2)],
            dst_ref=est1.at[pl.ds(2 * planes * side + place, 2)],
            send_sem=extra_sem.at[side, k],
            recv_sem=start_sem.at[side, k, 1],
            device_id=opposite[side],
            device_id_type=MESH,
        )

    def pass_copy(est, sem, side, k, who):
        high = rows if est is est1 else known
        offset = 0 if est is est1 else pl.multiple_of(upper * 2 * radius, 8)
        place = est.at[pl.ds(2 * planes * side + est_place(side, k, who), 2), pl.ds(offset, high), :]
        return remote(place, place, sem.at[side, k], sibling)

    my_rows = pl.ds(pl.multiple_of(upper * radius, 8), valid)
    other_rows = pl.ds(pl.multiple_of(lower * radius, 8), valid)
    z_planes = [
        jnp.where(only_next, orders[1][k], jnp.where(only_previous, orders[2][k], orders[0][k])) for k in range(4)
    ]

    def z_copy(k):
        return remote(
            theirs.at[pl.ds(z_planes[k], GROUP), other_rows, :],
            views.at[1, pl.ds(radius + z_planes[k], GROUP), other_rows, :],
            z_sem.at[k],
            partner,
        )

    def detour_copy():
        return pltpu.make_async_remote_copy(
            src_ref=theirs.at[pl.ds(z_planes[3], GROUP), other_rows, :],
            dst_ref=detour.at[:, other_rows, :],
            send_sem=detour_sem.at[0],
            recv_sem=detour_sem.at[1],
            device_id=helpers[1],
            device_id_type=MESH,
        )

    def detour_arrival():
        here = detour.at[:, my_rows, :]
        return pltpu.make_async_remote_copy(
            src_ref=here,
            dst_ref=here,
            send_sem=detour_sem.at[0],
            recv_sem=detour_sem.at[1],
            device_id=partner,
            device_id_type=MESH,
        )

    def detour_onward():
        place = radius + jnp.where(helps_next, orders[1][3], orders[2][3])
        return pltpu.make_async_remote_copy(
            src_ref=detour.at[:, my_rows, :],
            dst_ref=views.at[1, pl.ds(place, GROUP), my_rows, :],
            send_sem=detour_sem.at[2],
            recv_sem=z_sem.at[3, 1],
            device_id=helped_ends[0],
            device_id_type=MESH,
        )

    def z_arrival(k):
        here = views.at[1, pl.ds(radius + z_planes[k], GROUP), my_rows, :]
        return remote(here, here, z_sem.at[k], partner)

    def view_copy(which, side, k):
        src = (12 - 4 * k if side == 0 else 4 * k) + radius
        dst = 4 - 4 * k if side == 0 else planes + radius + 4 * k
        return remote(
            views.at[which, pl.ds(src, GROUP), my_rows, :],
            views.at[which, pl.ds(dst, GROUP), my_rows, :],
            view_sem.at[which, side, k],
            beside[side],
        )

    def direct_copy(side, k):
        src = 12 - 4 * k if side == 0 else 4 * k
        dst = 4 - 4 * k if side == 0 else planes + radius + 4 * k
        return remote(
            theirs.at[pl.ds(src, GROUP), other_rows, :],
            views.at[1, pl.ds(dst, GROUP), other_rows, :],
            view_sem.at[1, side, k],
            opposite[side],
        )

    def hop_copy(slot, src, high, send, there):
        return pltpu.make_async_remote_copy(
            src_ref=src,
            dst_ref=hop.at[slot, pl.ds(0, src.shape[0]), high, :],
            send_sem=hop_sem.at[0, send],
            recv_sem=hop_sem.at[1, slot],
            device_id=there,
            device_id_type=MESH,
        )

    def hop_start(side, k, across):
        place = est_place(side, k, core)
        src = spare.at[pl.ds(place, 2)] if across else est1.at[pl.ds(planes + place, 2)]
        there = relays_across[side] if across else relays[side]
        return hop_copy(k, src, pl.ds(0, rows), k + 2 * across, there)

    def hop_view(side, across):
        src = 8 if side == 0 else 4
        part = pl.ds(src, GROUP)
        if across:
            return hop_copy(1, theirs.at[part, other_rows, :], other_rows, 1, relays_across[side])
        return hop_copy(0, views.at[0, pl.ds(radius + src, GROUP), my_rows, :], my_rows, 0, relays[side])

    def onward(slot, side):
        target = sources[1 - side]
        if slot >= 2:
            src = hop.at[slot, pl.ds(0, 2)]
            dst = est1.at[pl.ds(2 * planes * side + est_place(side, slot, core), 2)]
            recv = start_sem.at[side, slot, 1]
        else:
            src = hop.at[slot, pl.ds(0, GROUP), my_rows, :]
            dst = views.at[slot, pl.ds(0 if side == 0 else planes + radius + 4, GROUP), my_rows, :]
            recv = view_sem.at[slot, side, 1, 1]
        return pltpu.make_async_remote_copy(
            src_ref=src,
            dst_ref=dst,
            send_sem=onward_sem.at[0, slot],
            recv_sem=recv,
            device_id=target,
            device_id_type=MESH,
        )

    def hop_arrival(slot):
        here = hop.at[slot, pl.ds(0, 2)] if slot >= 2 else hop.at[slot, pl.ds(0, GROUP), my_rows, :]
        return pltpu.make_async_remote_copy(
            src_ref=here,
            dst_ref=here,
            send_sem=onward_sem.at[1, slot],
            recv_sem=hop_sem.at[1, slot],
            device_id=partner,
            device_id_type=MESH,
        )

    def serve(slots):
        for side in range(2):

            @pl.when(at_relay[side])
            def _():
                for slot in slots:
                    hop_arrival(slot).wait_recv()
                    onward(slot, side).start()

    def prod_copy(i, q):
        part = pl.ds(q * GROUP, GROUP)
        return remote(prod.at[i, part], prod_in.at[i, part], prod_sem.at[i, q], sibling)

    def turn(source, p, own, other):
        @pl.when(upper == 0)
        def _():
            own[...] = source[p, :, pl.ds(0, 256)].T[:rows]
            other[...] = source[p, :, pl.ds(128, 256)].T[256 - rows :]

        @pl.when(upper == 1)
        def _():
            own[...] = source[p, :, pl.ds(128, 256)].T[256 - rows :]
            other[...] = source[p, :, pl.ds(0, 256)].T[:rows]

    plain = [jnp.logical_not(at_seam[side]) for side in range(2)]

    def turn_start(q):
        loads[q][0].wait()

        @pl.loop(q * GROUP, (q + 1) * GROUP)
        def _(p):
            turn(sin, p, est1.at[planes + p], spare.at[p])

    def send_start(k):
        for side in range(2):

            @pl.when(sends[side] & plain[side])
            def _():
                est_copy(est1, start_sem, side, k).start()

            @pl.when(at_seam[side] & (upper == core))
            def _():
                if k < 2:
                    est_copy(est1, start_sem, side, k).start()
                    extra_copy(side, k).start()
                else:
                    hop_start(side, k, 0).start()
                    hop_start(side, k, 1).start()

    kern[0] = jnp.zeros(kern.shape[1:], jnp.float32)
    table_copy.wait()
    rows_of = table[index[0]]
    rows_of = rows_of / jnp.sum(rows_of, axis=-1, keepdims=True)
    same = lax.broadcasted_iota(jnp.int32, (taps, taps), 0) == lax.broadcasted_iota(jnp.int32, (taps, taps), 1)
    for axis in range(3):
        spread = jnp.broadcast_to(rows_of[axis : axis + 1], (taps, taps))
        column = jnp.sum(jnp.where(same, spread, 0.0), axis=1, keepdims=True)
        kern[0, pl.ds(axis * taps, taps), :] = jnp.broadcast_to(column, (taps, wide))

    with jax.named_scope("turn_start"):
        turn_start(3)
        turn_start(0)
        for q in (3, 0, 2, 1):
            loads[q][1].start()
    with jax.named_scope("barrier"):
        pl.semaphore_wait(barrier, count)
    with jax.named_scope("turn_rest"):
        send_start(0)
        kern_copy = remote(kern.at[0], kern.at[1], kern_sem, partner)
        kern_copy.start()
        turn_start(2)
        turn_start(1)
        for k in range(1, 4):
            send_start(k)
    with jax.named_scope("turn_views"):
        for k in range(4):
            q = z_planes[k] // GROUP
            part = pl.ds(q * GROUP, GROUP)
            pltpu.make_async_copy(views_in.at[part], vin.at[part], load_sem.at[1, q]).wait()

            @pl.loop(q * GROUP, (q + 1) * GROUP)
            def _(p):
                turn(vin, p, views.at[0, radius + p], theirs.at[p])

            if k == 3:

                @pl.when(straight)
                def _():
                    z_copy(3).start()

                @pl.when(jnp.logical_not(straight))
                def _():
                    detour_copy().start()
            else:

                @pl.when(jnp.logical_not(at_seam[0] | at_seam[1]) | (k < 2))
                def _():
                    z_copy(k).start()

        for k in range(2):
            for side in range(2):

                @pl.when(sends[side] & plain[side])
                def _():
                    view_copy(0, side, k).start()

    ones = jnp.ones((8, wide), jnp.float32)
    view_pad = pl.multiple_of(lower * valid, 8)
    est_pad = pl.multiple_of(lower * known, 8)

    @pl.loop(0, views.shape[1])
    def _(f):
        for which in range(2):
            views[which, f, pl.ds(view_pad, 8), :] = ones
        est2[f + jnp.where(f >= planes, planes, 0), pl.ds(est_pad, 8), :] = ones
        est2[f + jnp.where(f >= planes, planes, 0), pl.ds(est_pad + 8, 8), :] = ones

    for side in range(2):

        @pl.when(jnp.logical_not(receives[side]))
        def _():
            zero = jnp.zeros((rows, wide), jnp.float32)

            @pl.loop(0, planes)
            def _(p):
                est1[2 * planes * side + p] = zero
                est2[2 * planes * side + p] = zero

            @pl.loop(0, radius)
            def _(p):
                for which in range(2):
                    views[which, (planes + radius) * side + p] = zero

    def bands(which):
        fill_bands(kern.at[which], taps, taps, xb.at[which], xf.at[which], wide, 1)
        fill_bands(kern.at[which], taps, 2 * taps, yf.at[which], yb.at[which], rows, 1)

    with jax.named_scope("bands"):
        bands(0)
        kern_copy.wait_recv()
        bands(1)

    def ahead_group(est, which, group, divide):
        base = group * GROUP
        coef = [kern[which, pl.ds(d, 1), :] for d in range(taps)]

        def finish(o, value):
            ratio[which, base + o] = views[which, base + o] / value if divide else value

        convolve(taps, coef, lambda i, r0: est[base + i, pl.ds(r0, CHUNK), :], xf[which], yf[which], mixed, finish)

    def back_group(i, which, group):
        base = group * GROUP
        coef = [kern[which, pl.ds(taps - 1 - d, 1), :] for d in range(taps)]

        def finish(o, value):
            prod[i, base + o] = value if which == 0 else prod[i, base + o] * value

        convolve(
            taps, coef, lambda j, r0: ratio[which, base + j, pl.ds(r0, CHUNK), :], xb[which], yb[which], mixed, finish
        )

    def hand_over(est, sem, side_sem, k):
        for side in range(2):

            @pl.when(receives[side])
            def _():
                est_copy(est, sem, side, k).wait_recv()
                pass_copy(est, side_sem, side, k, core).start()

    def arrive(est, side_sem, k):
        for side in range(2):

            @pl.when(receives[side])
            def _():
                pass_copy(est, side_sem, side, k, 1 - core).wait_recv()

    def ahead(est, k, divide, between):
        @pl.loop(0, 2)
        def _(which):
            @pl.loop(0, 2)
            def _(n):
                ahead_group(est, which, 3 - k + n * (2 * k + 1), divide)

            @pl.when(which == 0)
            def _():
                between()

    def ahead1(k, more):
        with jax.named_scope("arrive1"):
            arrive(est1, pass_sem.at[0], k)
        with jax.named_scope("ahead1"):

            def between():
                if more:
                    hand_over(est1, start_sem, pass_sem.at[0], k + 1)

                    @pl.when(k == 0)
                    def _():
                        serve((2, 3))

                    for side in range(2):

                        @pl.when(at_seam[side] & (k == 1))
                        def _():
                            hop_view(side, 0).start()
                            hop_view(side, 1).start()
                            z_copy(2).start()

            ahead(est1, k, False, between)

    with jax.named_scope("arrive1"):
        hand_over(est1, start_sem, pass_sem.at[0], 0)

    @pl.loop(0, 3)
    def _(k):
        ahead1(k, True)

    ahead1(3, False)

    for side in range(2):

        @pl.when(at_seam[side])
        def _():
            view_copy(0, side, 0).start()
            direct_copy(side, 0).start()

    def forward(k):
        with jax.named_scope("wait_z"):
            z_arrival(k).wait_recv()
        for kind, order in zip(kinds, orders):
            side = 0 if order[k] >= 8 else 1
            piece = 0 if order[k] in (0, 12) else 1

            @pl.when(kind & sends[side] & plain[side])
            def _():
                view_copy(1, side, piece).start()

    with jax.named_scope("help"):

        @pl.when(helps_next | helps_previous)
        def _():
            detour_arrival().wait_recv()
            detour_onward().start()

    forward(0)
    forward(1)
    with jax.named_scope("serve"):
        serve((0, 1))
    pl.when(ordinary)(functools.partial(forward, 2))


    def divide(which, first, number):
        @pl.loop(first, first + number)
        def _(f):
            ratio[which, f] = views[which, f] / ratio[which, f]

    with jax.named_scope("wait_own"):
        for k in range(2):
            for side in range(2):

                @pl.when(receives[side])
                def _():
                    view_copy(0, side, k).wait_recv()

    with jax.named_scope("back1own"):
        divide(0, 0, planes + 2 * radius)

        @pl.loop(0, planes // GROUP)
        def _(group):
            back_group(0, 0, group)

    pl.when(jnp.logical_not(ordinary))(functools.partial(forward, 2))
    forward(3)

    def update(i, est, q, store):
        prod_copy(i, q).wait_recv()
        for o in range(GROUP):
            p = q * GROUP + o
            both = prod[i, p] * prod_in[i, p]
            store(p, est[planes + p] * jnp.sqrt(jnp.sqrt(both)))

    def keep(p, value):
        est2[planes + p] = value

    for k in range(2):
        with jax.named_scope("wait_other"):
            for side in range(2):

                @pl.when(receives[side])
                def _():
                    view_copy(1, side, k).wait_recv()

        with jax.named_scope("back1other"):
            if k == 0:
                divide(1, 4, planes + 2 * radius - 8)
            else:
                divide(1, 0, 4)
                divide(1, planes + 2 * radius - 4, 4)
            groups = (1, 2) if k == 0 else (0, 3)

            @pl.loop(0, 2)
            def _(n):
                q = n + 1 if k == 0 else 3 * n
                back_group(0, 1, q)
                prod_copy(0, q).start()

        with jax.named_scope("update1"):
            for q in groups:
                update(0, est1, q, keep)
        for piece in (1,) if k == 0 else (0, 2, 3):
            for side in range(2):

                @pl.when(sends[side])
                def _():
                    est_copy(est2, est_sem, side, piece).start()

    def ahead2(k, more):
        with jax.named_scope("arrive2"):
            arrive(est2, pass_sem.at[1], k)
        with jax.named_scope("ahead2"):

            def between():
                if more:
                    hand_over(est2, est_sem, pass_sem.at[1], k + 1)

            ahead(est2, k, True, between)

    with jax.named_scope("arrive2"):
        hand_over(est2, est_sem, pass_sem.at[1], 0)

    @pl.loop(0, 3)
    def _(k):
        ahead2(k, True)

    own_rows = pl.ds(pl.multiple_of(upper * half, 8), half)
    rest_rows = pl.ds(pl.multiple_of(lower * half, 8), half)
    inner = pl.multiple_of(upper * (rows - half), 8)

    def last_part(q, who, high):
        return result.at[pl.ds(q * GROUP + 2 * who, 2), high, :]

    def last_copy(q):
        part = last_part(q, core, own_rows)
        return remote(part, part, last_sem.at[0, q], partner)

    def last_arrival(q):
        part = last_part(q, core, rest_rows)
        return remote(part, part, last_sem.at[0, q], partner)

    def last_pass(q, who):
        part = last_part(q, who, rest_rows)
        return remote(part, part, last_sem.at[1, q], sibling)

    def out_copy(q):
        part = pl.ds(q * GROUP, GROUP)
        return pltpu.make_async_copy(result.at[part], out.at[part], out_sem.at[q])

    def finish_group(q):
        prod_copy(1, q).wait_recv()
        for o in range(GROUP):
            p = q * GROUP + o
            both = prod[1, p] * prod_in[1, p]
            prod_in[0, p] = est2[planes + p] * jnp.sqrt(jnp.sqrt(both))
            result[p, own_rows, :] = prod_in[0, p, pl.ds(inner, half), :]

        last_copy(q).start()

    def back2(first, step):
        @pl.loop(0, 2)
        def _(n):
            q = first + step * n
            with jax.named_scope("back2"):
                back_group(1, 0, q)
                back_group(1, 1, q)
                prod_copy(1, q).start()

            @pl.when(n > 0)
            def _():
                finish_group(first)

    back2(1, 1)
    ahead2(3, False)
    finish_group(2)
    back2(0, 3)
    finish_group(3)

    with jax.named_scope("wait_last"):
        for n, q in enumerate((1, 2, 0, 3)):
            last_arrival(q).wait_recv()
            last_pass(q, core).start()
            if n > 0:
                last_pass(before, 1 - core).wait_recv()
                out_copy(before).start()
            before = q
        last_pass(before, 1 - core).wait_recv()
        out_copy(before).start()

    kern_copy.wait_send()
    @pl.when(straight)
    def _():
        z_copy(3).wait_send()

    @pl.when(jnp.logical_not(straight))
    def _():
        detour_copy().wait_send()

    @pl.when(helps_next | helps_previous)
    def _():
        detour_onward().wait_send()

    for k in range(4):
        if k < 3:
            z_copy(k).wait_send()
        prod_copy(0, k).wait_send()
        prod_copy(1, k).wait_send()
    for q in range(planes // GROUP):

        last_copy(q).wait_send()
        last_pass(q, core).wait_send()
        out_copy(q).wait()
    for side in range(2):
        for k in range(4):

            @pl.when(sends[side])
            def _():
                est_copy(est2, est_sem, side, k).wait_send()

            @pl.when(sends[side] & plain[side])
            def _():
                est_copy(est1, start_sem, side, k).wait_send()

            @pl.when(at_seam[side] & (upper == core))
            def _():
                if k < 2:
                    est_copy(est1, start_sem, side, k).wait_send()
                    extra_copy(side, k).wait_send()
                else:
                    hop_start(side, k, 0).wait_send()
                    hop_start(side, k, 1).wait_send()

            @pl.when(receives[side])
            def _():
                pass_copy(est1, pass_sem.at[0], side, k, core).wait_send()
                pass_copy(est2, pass_sem.at[1], side, k, core).wait_send()

        for k in range(2):

            @pl.when(sends[side] & plain[side])
            def _():
                view_copy(0, side, k).wait_send()
                view_copy(1, side, k).wait_send()

        @pl.when(at_seam[side])
        def _():
            view_copy(0, side, 0).wait_send()
            hop_view(side, 0).wait_send()
            direct_copy(side, 0).wait_send()
            hop_view(side, 1).wait_send()

        @pl.when(at_relay[side])
        def _():
            for slot in range(4):
                onward(slot, side).wait_send()


def turn_back(source, target, held, turned, in_sem, out_sem):
    pieces = source.shape[0] // 2

    def bring(q):
        part = pl.ds(2 * q, 2)
        return pltpu.make_async_copy(source.at[part], held.at[part], in_sem.at[q])

    def store(q):
        part = pl.ds(2 * q, 2)
        return pltpu.make_async_copy(turned.at[part], target.at[part], out_sem.at[q])

    for q in range(pieces):
        bring(q).start()

    @pl.loop(0, pieces)
    def _(q):
        bring(q).wait()
        for o in range(2):
            turned[2 * q + o] = held[2 * q + o].T
        store(q).start()

    for q in range(pieces):
        store(q).wait()


def on_device(views_data, start, psf_table, psf_index):
    planes, width_x, width_y = start.shape
    taps = psf_table.shape[2]
    radius = (taps - 1) // 2
    rows = width_y // 2 + 4 * radius
    outer = planes + 2 * radius

    f32, bf16 = jnp.float32, jnp.bfloat16
    plane = (rows, width_x)
    dma = pltpu.SemaphoreType.DMA
    anywhere = pl.BlockSpec(memory_space=pl.ANY)
    turned = pl.pallas_call(
        functools.partial(whole_kernel, taps),
        name="deconvolve",
        out_shape=jax.ShapeDtypeStruct((planes, width_y, width_x), f32),
        in_specs=[
            anywhere,
            anywhere,
            anywhere,
            pl.BlockSpec(memory_space=pltpu.SMEM),
        ],
        out_specs=anywhere,
        scratch_shapes=[
            pltpu.VMEM(psf_table.shape, f32),
            pltpu.VMEM((planes, width_x, width_y), f32),
            pltpu.VMEM((planes, width_x, width_y), f32),
            pltpu.VMEM((2, 3 * taps + -3 * taps % 8, width_x), f32),
            pltpu.VMEM((2, 2 * width_x, 2 * width_x), bf16),
            pltpu.VMEM((2, 2 * width_x, 2 * width_x), bf16),
            pltpu.VMEM((2, rows, 3 * rows), bf16),
            pltpu.VMEM((2, rows, 3 * rows), bf16),
            pltpu.VMEM((3 * planes,) + plane, f32),
            pltpu.VMEM((3 * planes,) + plane, f32),
            pltpu.VMEM((planes,) + plane, f32),
            pltpu.VMEM((2, outer) + plane, f32),
            pltpu.VMEM((planes,) + plane, f32),
            pltpu.VMEM((2, outer) + plane, f32),
            pltpu.VMEM((GROUP,) + plane, f32),
            pltpu.VMEM((2, planes) + plane, f32),
            pltpu.VMEM((2, planes) + plane, f32),
            pltpu.VMEM((planes, width_y, width_x), f32),
            pltpu.VMEM((4, GROUP) + plane, f32),
            pltpu.VMEM((GROUP,) + plane, f32),
            dma((2, 4)),
            dma((4,)),
            dma((2,)),
            dma((4, 2)),
            dma((2, 4, 2)),
            dma((2, 2)),
            dma((2, 2, 4, 2)),
            dma((2, 2, 2, 2)),
            dma((2, 4, 2)),
            dma((2, 4, 2)),
            dma((2, 4, 2)),
            dma((2, 6)),
            dma((2, 4)),
            dma((3,)),
        ],
        compiler_params=pltpu.CompilerParams(
            collective_id=0, has_side_effects=True, vmem_limit_bytes=60 * 2**20
        ),
    )(views_data[0], start, psf_table, psf_index)
    return pl.pallas_call(
        turn_back,
        name="turn_back",
        out_shape=jax.ShapeDtypeStruct(start.shape, f32),
        in_specs=[anywhere],
        out_specs=anywhere,
        scratch_shapes=[
            pltpu.VMEM((planes, width_y, width_x), f32),
            pltpu.VMEM(start.shape, f32),
            dma((planes // 2,)),
            dma((planes // 2,)),
        ],
    )(turned)


def solution(mesh):
    return jax.shard_map(
        on_device,
        mesh=mesh,
        in_specs=(P("view", "gz", None, None), P("gz", None, None), P(), P("view")),
        out_specs=P("gz", None, None),
        check_vma=False,
    )
```

```python
import functools

import jax
import jax.numpy as jnp
from jax import lax
from jax.experimental import pallas as pl
from jax.experimental.pallas import tpu as pltpu
from jax.sharding import PartitionSpec as P

MESH = pl.DeviceIdType.MESH
GROUP = 4
CHUNK = 32


def halves(value):
    high = value.astype(jnp.bfloat16)
    return high, (value - high.astype(jnp.float32)).astype(jnp.bfloat16)


def fill_bands(kern, taps, first_tap, ahead, behind, period, low_block):
    rows, cols = ahead.shape
    step = 32
    radius = (taps - 1) // 2

    @pl.loop(0, rows // step)
    def _(block):
        top = pl.multiple_of(block * step, step)
        row = lax.broadcasted_iota(jnp.int32, (step, cols), 0) + top
        col = lax.broadcasted_iota(jnp.int32, (step, cols), 1)
        is_low = (col >= low_block * period) & (col < (low_block + 1) * period)
        for wrap in range(cols // period - 1):
            col = jnp.where(col >= period, col - period, col)
        for wrap in range(rows // period - 1):
            row = jnp.where(row >= period, row - period, row)
        shift = col - row
        first = jnp.zeros((step, cols), jnp.float32)
        second = first
        for tap in range(taps):
            value = jnp.broadcast_to(kern[pl.ds(first_tap + tap, 1), pl.ds(0, 1)], (step, cols))
            first = jnp.where(shift == tap - radius, value, first)
            second = jnp.where(shift == radius - tap, value, second)
        for target, matrix in ((ahead, first), (behind, second)):
            high = matrix.astype(jnp.bfloat16).astype(jnp.float32)
            target[pl.ds(top, step), :] = jnp.where(is_low, matrix - high, high).astype(jnp.bfloat16)


def convolve(taps, coef, read, matrix_x, matrix_y, mixed, finish, size=GROUP):
    rows = mixed.shape[1]
    wide = mixed.shape[2]
    for r0 in range(0, rows, CHUNK):
        total = [None] * size
        for i in range(taps + size - 1):
            value = read(i, r0)
            for o in range(size):
                if 0 <= i - o < taps:
                    term = coef[i - o] * value
                    total[o] = term if total[o] is None else total[o] + term
        for o in range(size):
            mixed[o, pl.ds(r0, CHUNK), :] = total[o]
    for pair in range(size // 2):
        both = []
        for o in (2 * pair, 2 * pair + 1):
            high, low = halves(mixed[o])
            out = jnp.dot(jnp.concatenate([high, low], axis=1), matrix_x, preferred_element_type=jnp.float32)
            both.append(halves(out[:, :wide] + out[:, wide:]))
        high = jnp.concatenate([both[0][0], both[1][0]], axis=1)
        low = jnp.concatenate([both[0][1], both[1][1]], axis=1)
        out = jnp.dot(matrix_y, jnp.concatenate([high, high, low], axis=0), preferred_element_type=jnp.float32)
        finish(2 * pair, out[:, :wide])
        finish(2 * pair + 1, out[:, wide:])


def whole_kernel(
    taps, views_in, start_in, table_in, index, out,
    table, vin, sin, kern, xf, xb, yf, yb, est1, est2, spare, views, theirs, ratio, mixed, prod, prod_in, result, hop, detour,
    load_sem, out_sem, kern_sem, z_sem, start_sem, extra_sem, pass_sem, view_sem, est_sem, prod_sem, last_sem,
    hop_sem, onward_sem, detour_sem,
):
    planes, full, wide = result.shape
    rows = views.shape[2]
    half = full // 2
    radius = (taps - 1) // 2
    valid = rows - radius
    known = rows - 2 * radius
    v = lax.axis_index("view")
    g = lax.axis_index("gz")
    last = lax.axis_size("gz") - 1
    upper, core = v // 2, v % 2
    lower = 1 - upper
    seam = (last + 1) // 2
    partner = {"view": (v + 2) % 4, "gz": g}
    sibling = {"view": v + 1 - 2 * core, "gz": g}
    beside = ({"view": v, "gz": g + 1}, {"view": v, "gz": g - 1})
    opposite = ({"view": (v + 2) % 4, "gz": g + 1}, {"view": (v + 2) % 4, "gz": g - 1})
    sends = (g < last, g > 0)
    receives = (g > 0, g < last)
    at_seam = (g == seam - 1, g == seam)

    loads = []
    for q in range(planes // GROUP):
        part = pl.ds(q * GROUP, GROUP)
        loads.append(
            (
                pltpu.make_async_copy(start_in.at[part], sin.at[part], load_sem.at[0, q]),
                pltpu.make_async_copy(views_in.at[part], vin.at[part], load_sem.at[1, q]),
            )
        )
    table_copy = pltpu.make_async_copy(table_in, table, out_sem.at[0])
    table_copy.start()
    for q in (3, 0, 2, 1):
        loads[q][0].start()

    relays = ({"view": v, "gz": last}, {"view": v, "gz": 0})
    relays_across = ({"view": (v + 2) % 4, "gz": last}, {"view": (v + 2) % 4, "gz": 0})
    at_relay = (g == last, g == 0)
    sources = ({"view": v, "gz": seam - 1}, {"view": v, "gz": seam})
    sources_across = ({"view": (v + 2) % 4, "gz": seam - 1}, {"view": (v + 2) % 4, "gz": seam})

    only_next = (g == 0) | (g == seam)
    only_previous = (g == last) | (g == seam - 1)
    ordinary = jnp.logical_not(only_next | only_previous)
    orders = ((12, 0, 8, 4), (12, 8, 0, 4), (0, 4, 12, 8))
    kinds = (ordinary, only_next, only_previous)
    away = 3 * seam // 4
    helper = jnp.where(only_next, g + away, g - away)
    straight = jnp.logical_not(at_seam[0] | at_seam[1])
    helps_next = g == seam + away
    helps_previous = g == seam - 1 - away
    helped = jnp.where(helps_next, g - away, g + away)
    helpers = ({"view": v, "gz": helper}, {"view": (v + 2) % 4, "gz": helper})
    helped_ends = ({"view": v, "gz": helped}, {"view": (v + 2) % 4, "gz": helped})

    barrier = pltpu.get_barrier_semaphore()

    def greet(there):
        pl.semaphore_signal(barrier, inc=1, device_id=there, device_id_type=MESH)

    greet(partner)
    greet(sibling)

    @pl.when(jnp.logical_not(straight))
    def _():
        greet(helpers[0])
        greet(helpers[1])

    @pl.when(helps_next | helps_previous)
    def _():
        greet(helped_ends[0])
        greet(helped_ends[1])

    count = 2 + jnp.where(straight, 0, 2) + jnp.where(helps_next | helps_previous, 2, 0)
    for side in range(2):

        @pl.when(sends[side])
        def _():
            greet(beside[side])

        @pl.when(at_seam[side])
        def _():
            greet(opposite[side])
            greet(relays[side])
            greet(relays_across[side])
            greet(relays[1 - side])

        @pl.when(at_relay[side])
        def _():
            greet(sources[side])
            greet(sources_across[side])
            greet(sources[1 - side])

        count = count + jnp.where(sends[side], 1, 0) + jnp.where(at_seam[side], 4, 0) + jnp.where(at_relay[side], 3, 0)

    def remote(src, dst, sem, there):
        return pltpu.make_async_remote_copy(
            src_ref=src, dst_ref=dst, send_sem=sem.at[0], recv_sem=sem.at[1], device_id=there, device_id_type=MESH
        )

    def est_place(side, k, who):
        return 14 - 2 * who - 4 * k if side == 0 else 2 * who + 4 * k

    def est_copy(est, sem, side, k):
        high = rows if est is est1 else known
        offset = 0 if est is est1 else pl.multiple_of(upper * 2 * radius, 8)
        place = est_place(side, k, core)
        src = est.at[pl.ds(planes + place, 2), pl.ds(offset, high), :]
        dst = est.at[pl.ds(2 * planes * side + place, 2), pl.ds(offset, high), :]
        return remote(src, dst, sem.at[side, k], beside[side])

    def extra_copy(side, k):
        place = est_place(side, k, core)
        return pltpu.make_async_remote_copy(
            src_ref=spare.at[pl.ds(place, 2)],
            dst_ref=est1.at[pl.ds(2 * planes * side + place, 2)],
            send_sem=extra_sem.at[side, k],
            recv_sem=start_sem.at[side, k, 1],
            device_id=opposite[side],
            device_id_type=MESH,
        )

    def pass_copy(est, sem, side, k, who):
        high = rows if est is est1 else known
        offset = 0 if est is est1 else pl.multiple_of(upper * 2 * radius, 8)
        place = est.at[pl.ds(2 * planes * side + est_place(side, k, who), 2), pl.ds(offset, high), :]
        return remote(place, place, sem.at[side, k], sibling)

    my_rows = pl.ds(pl.multiple_of(upper * radius, 8), valid)
    other_rows = pl.ds(pl.multiple_of(lower * radius, 8), valid)
    z_planes = [
        jnp.where(only_next, orders[1][k], jnp.where(only_previous, orders[2][k], orders[0][k])) for k in range(4)
    ]

    def z_copy(k):
        return remote(
            theirs.at[pl.ds(z_planes[k], GROUP), other_rows, :],
            views.at[1, pl.ds(radius + z_planes[k], GROUP), other_rows, :],
            z_sem.at[k],
            partner,
        )

    def detour_copy():
        return pltpu.make_async_remote_copy(
            src_ref=theirs.at[pl.ds(z_planes[3], GROUP), other_rows, :],
            dst_ref=detour.at[:, other_rows, :],
            send_sem=detour_sem.at[0],
            recv_sem=detour_sem.at[1],
            device_id=helpers[1],
            device_id_type=MESH,
        )

    def detour_arrival():
        here = detour.at[:, my_rows, :]
        return pltpu.make_async_remote_copy(
            src_ref=here,
            dst_ref=here,
            send_sem=detour_sem.at[0],
            recv_sem=detour_sem.at[1],
            device_id=partner,
            device_id_type=MESH,
        )

    def detour_onward():
        place = radius + jnp.where(helps_next, orders[1][3], orders[2][3])
        return pltpu.make_async_remote_copy(
            src_ref=detour.at[:, my_rows, :],
            dst_ref=views.at[1, pl.ds(place, GROUP), my_rows, :],
            send_sem=detour_sem.at[2],
            recv_sem=z_sem.at[3, 1],
            device_id=helped_ends[0],
            device_id_type=MESH,
        )

    def z_arrival(k):
        here = views.at[1, pl.ds(radius + z_planes[k], GROUP), my_rows, :]
        return remote(here, here, z_sem.at[k], partner)

    def view_copy(which, side, k):
        src = (12 - 4 * k if side == 0 else 4 * k) + radius
        dst = 4 - 4 * k if side == 0 else planes + radius + 4 * k
        return remote(
            views.at[which, pl.ds(src, GROUP), my_rows, :],
            views.at[which, pl.ds(dst, GROUP), my_rows, :],
            view_sem.at[which, side, k],
            beside[side],
        )

    def direct_copy(side, k):
        src = 12 - 4 * k if side == 0 else 4 * k
        dst = 4 - 4 * k if side == 0 else planes + radius + 4 * k
        return remote(
            theirs.at[pl.ds(src, GROUP), other_rows, :],
            views.at[1, pl.ds(dst, GROUP), other_rows, :],
            view_sem.at[1, side, k],
            opposite[side],
        )

    def hop_copy(slot, src, high, send, there):
        return pltpu.make_async_remote_copy(
            src_ref=src,
            dst_ref=hop.at[slot, pl.ds(0, src.shape[0]), high, :],
            send_sem=hop_sem.at[0, send],
            recv_sem=hop_sem.at[1, slot],
            device_id=there,
            device_id_type=MESH,
        )

    def hop_start(side, k, across):
        place = est_place(side, k, core)
        src = spare.at[pl.ds(place, 2)] if across else est1.at[pl.ds(planes + place, 2)]
        there = relays_across[side] if across else relays[side]
        return hop_copy(k, src, pl.ds(0, rows), k + 2 * across, there)

    def hop_view(side, across):
        src = 8 if side == 0 else 4
        part = pl.ds(src, GROUP)
        if across:
            return hop_copy(1, theirs.at[part, other_rows, :], other_rows, 1, relays_across[side])
        return hop_copy(0, views.at[0, pl.ds(radius + src, GROUP), my_rows, :], my_rows, 0, relays[side])

    def onward(slot, side):
        target = sources[1 - side]
        if slot >= 2:
            src = hop.at[slot, pl.ds(0, 2)]
            dst = est1.at[pl.ds(2 * planes * side + est_place(side, slot, core), 2)]
            recv = start_sem.at[side, slot, 1]
        else:
            src = hop.at[slot, pl.ds(0, GROUP), my_rows, :]
            dst = views.at[slot, pl.ds(0 if side == 0 else planes + radius + 4, GROUP), my_rows, :]
            recv = view_sem.at[slot, side, 1, 1]
        return pltpu.make_async_remote_copy(
            src_ref=src,
            dst_ref=dst,
            send_sem=onward_sem.at[0, slot],
            recv_sem=recv,
            device_id=target,
            device_id_type=MESH,
        )

    def hop_arrival(slot):
        here = hop.at[slot, pl.ds(0, 2)] if slot >= 2 else hop.at[slot, pl.ds(0, GROUP), my_rows, :]
        return pltpu.make_async_remote_copy(
            src_ref=here,
            dst_ref=here,
            send_sem=onward_sem.at[1, slot],
            recv_sem=hop_sem.at[1, slot],
            device_id=partner,
            device_id_type=MESH,
        )

    def serve(slots):
        for side in range(2):

            @pl.when(at_relay[side])
            def _():
                for slot in slots:
                    hop_arrival(slot).wait_recv()
                    onward(slot, side).start()

    def prod_copy(i, q):
        part = pl.ds(q * GROUP, GROUP)
        return remote(prod.at[i, part], prod_in.at[i, part], prod_sem.at[i, q], sibling)

    def turn(source, p, own, other):
        @pl.when(upper == 0)
        def _():
            own[...] = source[p, :, pl.ds(0, 256)].T[:rows]
            other[...] = source[p, :, pl.ds(128, 256)].T[256 - rows :]

        @pl.when(upper == 1)
        def _():
            own[...] = source[p, :, pl.ds(128, 256)].T[256 - rows :]
            other[...] = source[p, :, pl.ds(0, 256)].T[:rows]

    plain = [jnp.logical_not(at_seam[side]) for side in range(2)]

    def turn_start(q):
        loads[q][0].wait()

        @pl.loop(q * GROUP, (q + 1) * GROUP)
        def _(p):
            turn(sin, p, est1.at[planes + p], spare.at[p])

    def send_start(k):
        for side in range(2):

            @pl.when(sends[side] & plain[side])
            def _():
                est_copy(est1, start_sem, side, k).start()

            @pl.when(at_seam[side] & (upper == core))
            def _():
                if k < 2:
                    est_copy(est1, start_sem, side, k).start()
                    extra_copy(side, k).start()
                else:
                    hop_start(side, k, 0).start()
                    hop_start(side, k, 1).start()

    kern[0] = jnp.zeros(kern.shape[1:], jnp.float32)
    table_copy.wait()
    rows_of = table[index[0]]
    rows_of = rows_of / jnp.sum(rows_of, axis=-1, keepdims=True)
    same = lax.broadcasted_iota(jnp.int32, (taps, taps), 0) == lax.broadcasted_iota(jnp.int32, (taps, taps), 1)
    for axis in range(3):
        spread = jnp.broadcast_to(rows_of[axis : axis + 1], (taps, taps))
        column = jnp.sum(jnp.where(same, spread, 0.0), axis=1, keepdims=True)
        kern[0, pl.ds(axis * taps, taps), :] = jnp.broadcast_to(column, (taps, wide))

    with jax.named_scope("turn_start"):
        turn_start(3)
        turn_start(0)
        for q in (3, 0, 2, 1):
            loads[q][1].start()
    with jax.named_scope("barrier"):
        pl.semaphore_wait(barrier, count)
    with jax.named_scope("turn_rest"):
        send_start(0)
        kern_copy = remote(kern.at[0], kern.at[1], kern_sem, partner)
        kern_copy.start()
        turn_start(2)
        turn_start(1)
        for k in range(1, 4):
            send_start(k)
    with jax.named_scope("turn_views"):
        for k in range(4):
            q = z_planes[k] // GROUP
            part = pl.ds(q * GROUP, GROUP)
            pltpu.make_async_copy(views_in.at[part], vin.at[part], load_sem.at[1, q]).wait()

            @pl.loop(q * GROUP, (q + 1) * GROUP)
            def _(p):
                turn(vin, p, views.at[0, radius + p], theirs.at[p])

            if k == 3:

                @pl.when(straight)
                def _():
                    z_copy(3).start()

                @pl.when(jnp.logical_not(straight))
                def _():
                    detour_copy().start()
            else:

                @pl.when(jnp.logical_not(at_seam[0] | at_seam[1]) | (k < 2))
                def _():
                    z_copy(k).start()

        for k in range(2):
            for side in range(2):

                @pl.when(sends[side] & plain[side])
                def _():
                    view_copy(0, side, k).start()

    ones = jnp.ones((8, wide), jnp.float32)
    view_pad = pl.multiple_of(lower * valid, 8)
    est_pad = pl.multiple_of(lower * known, 8)

    @pl.loop(0, views.shape[1])
    def _(f):
        for which in range(2):
            views[which, f, pl.ds(view_pad, 8), :] = ones
        est2[f + jnp.where(f >= planes, planes, 0), pl.ds(est_pad, 8), :] = ones
        est2[f + jnp.where(f >= planes, planes, 0), pl.ds(est_pad + 8, 8), :] = ones

    for side in range(2):

        @pl.when(jnp.logical_not(receives[side]))
        def _():
            zero = jnp.zeros((rows, wide), jnp.float32)

            @pl.loop(0, planes)
            def _(p):
                est1[2 * planes * side + p] = zero
                est2[2 * planes * side + p] = zero

            @pl.loop(0, radius)
            def _(p):
                for which in range(2):
                    views[which, (planes + radius) * side + p] = zero

    def bands(which):
        fill_bands(kern.at[which], taps, taps, xb.at[which], xf.at[which], wide, 1)
        fill_bands(kern.at[which], taps, 2 * taps, yf.at[which], yb.at[which], rows, 1)

    with jax.named_scope("bands"):
        bands(0)
        kern_copy.wait_recv()
        bands(1)

    def ahead_group(est, which, group, divide):
        base = group * GROUP
        coef = [kern[which, pl.ds(d, 1), :] for d in range(taps)]

        def finish(o, value):
            ratio[which, base + o] = views[which, base + o] / value if divide else value

        convolve(taps, coef, lambda i, r0: est[base + i, pl.ds(r0, CHUNK), :], xf[which], yf[which], mixed, finish)

    def back_group(i, which, group):
        back_planes(i, which, group * GROUP, GROUP)

    def back_planes(i, which, base, size):
        coef = [kern[which, pl.ds(taps - 1 - d, 1), :] for d in range(taps)]

        def finish(o, value):
            prod[i, base + o] = value if which == 0 else prod[i, base + o] * value

        convolve(
            taps,
            coef,
            lambda j, r0: ratio[which, base + j, pl.ds(r0, CHUNK), :],
            xb[which],
            yb[which],
            mixed,
            finish,
            size,
        )

    def hand_over(est, sem, side_sem, k):
        for side in range(2):

            @pl.when(receives[side])
            def _():
                est_copy(est, sem, side, k).wait_recv()
                pass_copy(est, side_sem, side, k, core).start()

    def arrive(est, side_sem, k):
        for side in range(2):

            @pl.when(receives[side])
            def _():
                pass_copy(est, side_sem, side, k, 1 - core).wait_recv()

    def ahead(est, k, divide, between):
        @pl.loop(0, 2)
        def _(which):
            @pl.loop(0, 2)
            def _(n):
                ahead_group(est, which, 3 - k + n * (2 * k + 1), divide)

            @pl.when(which == 0)
            def _():
                between()

    def ahead1(k, more):
        with jax.named_scope("arrive1"):
            arrive(est1, pass_sem.at[0], k)
        with jax.named_scope("ahead1"):

            def between():
                if more:
                    hand_over(est1, start_sem, pass_sem.at[0], k + 1)

                    @pl.when(k == 0)
                    def _():
                        serve((2, 3))

                    for side in range(2):

                        @pl.when(at_seam[side] & (k == 1))
                        def _():
                            hop_view(side, 0).start()
                            hop_view(side, 1).start()
                            z_copy(2).start()

            ahead(est1, k, False, between)

    with jax.named_scope("arrive1"):
        hand_over(est1, start_sem, pass_sem.at[0], 0)

    @pl.loop(0, 3)
    def _(k):
        ahead1(k, True)

    ahead1(3, False)

    for side in range(2):

        @pl.when(at_seam[side])
        def _():
            view_copy(0, side, 0).start()
            direct_copy(side, 0).start()

    def forward(k):
        with jax.named_scope("wait_z"):
            z_arrival(k).wait_recv()
        for kind, order in zip(kinds, orders):
            side = 0 if order[k] >= 8 else 1
            piece = 0 if order[k] in (0, 12) else 1

            @pl.when(kind & sends[side] & plain[side])
            def _():
                view_copy(1, side, piece).start()

    with jax.named_scope("help"):

        @pl.when(helps_next | helps_previous)
        def _():
            detour_arrival().wait_recv()
            detour_onward().start()

    forward(0)
    forward(1)
    with jax.named_scope("serve"):
        serve((0, 1))
    pl.when(ordinary)(functools.partial(forward, 2))


    def divide(which, first, number):
        @pl.loop(first, first + number)
        def _(f):
            ratio[which, f] = views[which, f] / ratio[which, f]

    with jax.named_scope("wait_own"):
        for k in range(2):
            for side in range(2):

                @pl.when(receives[side])
                def _():
                    view_copy(0, side, k).wait_recv()

    with jax.named_scope("back1own"):
        divide(0, 0, planes + 2 * radius)

        @pl.loop(0, planes // GROUP)
        def _(group):
            back_group(0, 0, group)

    pl.when(jnp.logical_not(ordinary))(functools.partial(forward, 2))
    forward(3)

    def update(i, est, q, store):
        prod_copy(i, q).wait_recv()
        for o in range(GROUP):
            p = q * GROUP + o
            both = prod[i, p] * prod_in[i, p]
            store(p, est[planes + p] * jnp.sqrt(jnp.sqrt(both)))

    def keep(p, value):
        est2[planes + p] = value

    for k in range(2):
        with jax.named_scope("wait_other"):
            for side in range(2):

                @pl.when(receives[side])
                def _():
                    view_copy(1, side, k).wait_recv()

        with jax.named_scope("back1other"):
            if k == 0:
                divide(1, 4, planes + 2 * radius - 8)
            else:
                divide(1, 0, 4)
                divide(1, planes + 2 * radius - 4, 4)
            groups = (1, 2) if k == 0 else (0, 3)

            @pl.loop(0, 2)
            def _(n):
                q = n + 1 if k == 0 else 3 * n
                back_group(0, 1, q)
                prod_copy(0, q).start()

        with jax.named_scope("update1"):
            for q in groups:
                update(0, est1, q, keep)
        for piece in (1,) if k == 0 else (0, 2, 3):
            for side in range(2):

                @pl.when(sends[side])
                def _():
                    est_copy(est2, est_sem, side, piece).start()

    def ahead2(k, more):
        with jax.named_scope("arrive2"):
            arrive(est2, pass_sem.at[1], k)
        with jax.named_scope("ahead2"):

            def between():
                if more:
                    hand_over(est2, est_sem, pass_sem.at[1], k + 1)

            ahead(est2, k, True, between)

    with jax.named_scope("arrive2"):
        hand_over(est2, est_sem, pass_sem.at[1], 0)

    @pl.loop(0, 3)
    def _(k):
        ahead2(k, True)

    own_rows = pl.ds(pl.multiple_of(upper * half, 8), half)
    rest_rows = pl.ds(pl.multiple_of(lower * half, 8), half)
    inner = pl.multiple_of(upper * (rows - half), 8)

    def extent(q):
        return (q * GROUP, GROUP) if q < 3 else (12 + 2 * (q - 3), 2)

    def prod_piece(q, place):
        part = pl.ds(*place)
        return remote(prod.at[1, part], prod_in.at[1, part], prod_sem.at[1, q], sibling)

    def last_part(place, who, high):
        start, size = place
        return result.at[pl.ds(start + size // 2 * who, size // 2), high, :]

    def last_copy(q, place):
        part = last_part(place, core, own_rows)
        return remote(part, part, last_sem.at[0, q], partner)

    def last_arrival(q):
        part = last_part(extent(q), core, rest_rows)
        return remote(part, part, last_sem.at[0, q], partner)

    def last_pass(q, who):
        part = last_part(extent(q), who, rest_rows)
        return remote(part, part, last_sem.at[1, q], sibling)

    def out_copy(q):
        part = pl.ds(*extent(q))
        return pltpu.make_async_copy(result.at[part], out.at[part], out_sem.at[q])

    def finish_piece(q, place):
        prod_piece(q, place).wait_recv()
        for o in range(place[1]):
            p = place[0] + o
            both = prod[1, p] * prod_in[1, p]
            prod_in[0, p] = est2[planes + p] * jnp.sqrt(jnp.sqrt(both))
            result[p, own_rows, :] = prod_in[0, p, pl.ds(inner, half), :]

        last_copy(q, place).start()

    def back_piece(q, place):
        with jax.named_scope("back2"):
            back_planes(1, 0, *place)
            back_planes(1, 1, *place)
            prod_piece(q, place).start()

    @pl.loop(0, 2)
    def _(n):
        back_piece(1 + n, (GROUP * (1 + n), GROUP))

        @pl.when(n > 0)
        def _():
            finish_piece(1, extent(1))

    ahead2(3, False)
    finish_piece(2, extent(2))
    back_piece(0, extent(0))

    @pl.loop(0, 2)
    def _(n):
        back_piece(3 + n, (12 + 2 * n, 2))

        @pl.when(n == 0)
        def _():
            finish_piece(0, extent(0))

        @pl.when(n > 0)
        def _():
            finish_piece(3, extent(3))

    finish_piece(4, extent(4))

    with jax.named_scope("wait_last"):
        for n, q in enumerate((1, 2, 0, 3, 4)):
            last_arrival(q).wait_recv()
            last_pass(q, core).start()
            if n > 0:
                last_pass(before, 1 - core).wait_recv()
                out_copy(before).start()
            before = q
        last_pass(before, 1 - core).wait_recv()
        out_copy(before).start()

    kern_copy.wait_send()
    @pl.when(straight)
    def _():
        z_copy(3).wait_send()

    @pl.when(jnp.logical_not(straight))
    def _():
        detour_copy().wait_send()

    @pl.when(helps_next | helps_previous)
    def _():
        detour_onward().wait_send()

    for k in range(4):
        if k < 3:
            z_copy(k).wait_send()
        prod_copy(0, k).wait_send()
    for q in range(5):
        prod_piece(q, extent(q)).wait_send()
        last_copy(q, extent(q)).wait_send()
        last_pass(q, core).wait_send()
        out_copy(q).wait()
    for side in range(2):
        for k in range(4):

            @pl.when(sends[side])
            def _():
                est_copy(est2, est_sem, side, k).wait_send()

            @pl.when(sends[side] & plain[side])
            def _():
                est_copy(est1, start_sem, side, k).wait_send()

            @pl.when(at_seam[side] & (upper == core))
            def _():
                if k < 2:
                    est_copy(est1, start_sem, side, k).wait_send()
                    extra_copy(side, k).wait_send()
                else:
                    hop_start(side, k, 0).wait_send()
                    hop_start(side, k, 1).wait_send()

            @pl.when(receives[side])
            def _():
                pass_copy(est1, pass_sem.at[0], side, k, core).wait_send()
                pass_copy(est2, pass_sem.at[1], side, k, core).wait_send()

        for k in range(2):

            @pl.when(sends[side] & plain[side])
            def _():
                view_copy(0, side, k).wait_send()
                view_copy(1, side, k).wait_send()

        @pl.when(at_seam[side])
        def _():
            view_copy(0, side, 0).wait_send()
            hop_view(side, 0).wait_send()
            direct_copy(side, 0).wait_send()
            hop_view(side, 1).wait_send()

        @pl.when(at_relay[side])
        def _():
            for slot in range(4):
                onward(slot, side).wait_send()


def turn_back(source, target, held, turned, in_sem, out_sem):
    pieces = source.shape[0] // 2

    def bring(q):
        part = pl.ds(2 * q, 2)
        return pltpu.make_async_copy(source.at[part], held.at[part], in_sem.at[q])

    def store(q):
        part = pl.ds(2 * q, 2)
        return pltpu.make_async_copy(turned.at[part], target.at[part], out_sem.at[q])

    for q in range(pieces):
        bring(q).start()

    @pl.loop(0, pieces)
    def _(q):
        bring(q).wait()
        for o in range(2):
            turned[2 * q + o] = held[2 * q + o].T
        store(q).start()

    for q in range(pieces):
        store(q).wait()


def on_device(views_data, start, psf_table, psf_index):
    planes, width_x, width_y = start.shape
    taps = psf_table.shape[2]
    radius = (taps - 1) // 2
    rows = width_y // 2 + 4 * radius
    outer = planes + 2 * radius

    f32, bf16 = jnp.float32, jnp.bfloat16
    plane = (rows, width_x)
    dma = pltpu.SemaphoreType.DMA
    anywhere = pl.BlockSpec(memory_space=pl.ANY)
    turned = pl.pallas_call(
        functools.partial(whole_kernel, taps),
        name="deconvolve",
        out_shape=jax.ShapeDtypeStruct((planes, width_y, width_x), f32),
        in_specs=[
            anywhere,
            anywhere,
            anywhere,
            pl.BlockSpec(memory_space=pltpu.SMEM),
        ],
        out_specs=anywhere,
        scratch_shapes=[
            pltpu.VMEM(psf_table.shape, f32),
            pltpu.VMEM((planes, width_x, width_y), f32),
            pltpu.VMEM((planes, width_x, width_y), f32),
            pltpu.VMEM((2, 3 * taps + -3 * taps % 8, width_x), f32),
            pltpu.VMEM((2, 2 * width_x, 2 * width_x), bf16),
            pltpu.VMEM((2, 2 * width_x, 2 * width_x), bf16),
            pltpu.VMEM((2, rows, 3 * rows), bf16),
            pltpu.VMEM((2, rows, 3 * rows), bf16),
            pltpu.VMEM((3 * planes,) + plane, f32),
            pltpu.VMEM((3 * planes,) + plane, f32),
            pltpu.VMEM((planes,) + plane, f32),
            pltpu.VMEM((2, outer) + plane, f32),
            pltpu.VMEM((planes,) + plane, f32),
            pltpu.VMEM((2, outer) + plane, f32),
            pltpu.VMEM((GROUP,) + plane, f32),
            pltpu.VMEM((2, planes) + plane, f32),
            pltpu.VMEM((2, planes) + plane, f32),
            pltpu.VMEM((planes, width_y, width_x), f32),
            pltpu.VMEM((4, GROUP) + plane, f32),
            pltpu.VMEM((GROUP,) + plane, f32),
            dma((2, 4)),
            dma((5,)),
            dma((2,)),
            dma((4, 2)),
            dma((2, 4, 2)),
            dma((2, 2)),
            dma((2, 2, 4, 2)),
            dma((2, 2, 2, 2)),
            dma((2, 4, 2)),
            dma((2, 5, 2)),
            dma((2, 5, 2)),
            dma((2, 6)),
            dma((2, 4)),
            dma((3,)),
        ],
        compiler_params=pltpu.CompilerParams(
            collective_id=0, has_side_effects=True, vmem_limit_bytes=60 * 2**20
        ),
    )(views_data[0], start, psf_table, psf_index)
    return pl.pallas_call(
        turn_back,
        name="turn_back",
        out_shape=jax.ShapeDtypeStruct(start.shape, f32),
        in_specs=[anywhere],
        out_specs=anywhere,
        scratch_shapes=[
            pltpu.VMEM((planes, width_y, width_x), f32),
            pltpu.VMEM(start.shape, f32),
            dma((planes // 2,)),
            dma((planes // 2,)),
        ],
    )(turned)


def solution(mesh):
    return jax.shard_map(
        on_device,
        mesh=mesh,
        in_specs=(P("view", "gz", None, None), P("gz", None, None), P(), P("view")),
        out_specs=P("gz", None, None),
        check_vma=False,
    )
```
